8 devices in a mesh: dp: 1 (over z), ep: 8 (over y, x, core).
Axes of the slice: x: 2, y: 2, z: 1, core: 2. Of those that a mesh axis runs over, the one named last changes fastest.
Arguments:
- tokens: bfloat16 [512, 2048], P(('dp', 'ep'))
- route_idx: int32 [512, 6], P(('dp', 'ep'))
- gate_vals: float32 [512, 6], P(('dp', 'ep'))
- w_gate: bfloat16 [64, 2048, 1408], P('ep')
- w_up: bfloat16 [64, 2048, 1408], P('ep')
- w_down: bfloat16 [64, 1408, 2048], P('ep')
Outputs:
- output: bfloat16 [512, 2048], P(('dp', 'ep'))
All inputs are finite; a program needn't handle non-finite values.
Results may differ from the reference program's by a relative error of at most 0.00786066.
Values are sent between devices in bfloat16 or wider.
A program may use at most 1 GiB of HBM per device.

```python
import functools
import jax
import jax.numpy as jnp
from jax import lax

TOKENS_DEV = 64
GROUP_SIZE = 8
D_MODEL = 2048
D_FF = 1408
EXPERTS = 64
TOP_K = 6
CAPACITY = 32
TOKENS = TOKENS_DEV * GROUP_SIZE


def device_routing(expert_order, hot_counts, dev_key):
    key_jitter, key_perm, key_tokens = jax.random.split(dev_key, 3)
    cold_n = EXPERTS - TOP_K
    half_n = cold_n // 2
    rest_slots = TOKENS_DEV * TOP_K - jnp.sum(hot_counts)
    base_count = rest_slots // cold_n
    extra_count = rest_slots - base_count * cold_n
    cold_counts = base_count + (jnp.arange(cold_n) < extra_count).astype(jnp.int32)
    jitter_up = jax.random.randint(key_jitter, (half_n,), 0, (base_count - 1) // 2 + 1)
    jitter = jnp.stack([jitter_up, -jitter_up], axis=1).reshape(-1)
    jitter = jnp.pad(jitter, (0, cold_n - 2 * half_n))
    cold_counts = cold_counts + jax.random.permutation(key_perm, jitter)
    all_counts = jnp.concatenate([hot_counts, cold_counts])
    run_ends = jnp.cumsum(all_counts)
    rank_ids = jnp.searchsorted(run_ends, jnp.arange(TOKENS_DEV * TOP_K), side="right")
    flat_ids = expert_order[rank_ids]
    slot_grid = flat_ids.reshape(TOP_K, TOKENS_DEV).T
    return jax.random.permutation(key_tokens, slot_grid, axis=0)


def draw_routing(route_key):
    key_order, key_hot, key_pick, key_dev = jax.random.split(route_key, 4)
    expert_order = jax.random.permutation(key_order, EXPERTS)
    hot_counts = CAPACITY - jax.random.randint(key_hot, (GROUP_SIZE, TOP_K), 0, CAPACITY // 4 + 1)
    full_dev = jax.random.randint(key_pick, (), 0, GROUP_SIZE)
    at_full = (jnp.arange(GROUP_SIZE)[:, None] == full_dev) & (jnp.arange(TOP_K)[None, :] == 0)
    hot_counts = jnp.where(at_full, CAPACITY, hot_counts)
    dev_keys = jax.random.split(key_dev, GROUP_SIZE)
    per_device = jax.vmap(functools.partial(device_routing, expert_order))(hot_counts, dev_keys)
    return per_device.reshape(TOKENS, TOP_K).astype(jnp.int32)


def draw_weight(weight_key, fan_in, fan_out):
    expert_keys = jax.random.split(weight_key, EXPERTS)
    return lax.map(lambda one_key: (jax.random.normal(one_key, (fan_in, fan_out), jnp.float32) * fan_in ** -0.5).astype(jnp.bfloat16), expert_keys)


def setup_inputs(seed: int = 0, part: int = 0) -> dict:
    root_key = jax.random.key(seed)
    part_key = jax.random.fold_in(root_key, part)
    key_tok, key_route, key_gate = jax.random.split(part_key, 3)
    key_wg, key_wu, key_wd = jax.random.split(jax.random.key(seed + 1), 3)
    tokens = jax.random.normal(key_tok, (TOKENS, D_MODEL), jnp.float32).astype(jnp.bfloat16)
    route_idx = draw_routing(key_route)
    gate_vals = jax.random.uniform(key_gate, (TOKENS, TOP_K), jnp.float32, 0.5, 1.5) * TOP_K ** -0.5
    return {"tokens": tokens, "route_idx": route_idx, "gate_vals": gate_vals, "w_gate": draw_weight(key_wg, D_MODEL, D_FF), "w_up": draw_weight(key_wu, D_MODEL, D_FF), "w_down": draw_weight(key_wd, D_FF, D_MODEL)}


def reference(tokens, route_idx, gate_vals, w_gate, w_up, w_down):
    row_cap = GROUP_SIZE * CAPACITY
    targets = jnp.arange(row_cap) + 1

    def expert_step(y_acc, expert_args):
        expert_id, wg_one, wu_one, wd_one = expert_args
        hit_mask = route_idx == expert_id
        member = jnp.sum(hit_mask, axis=1, dtype=jnp.int32)
        row_weight = jnp.sum(jnp.where(hit_mask, gate_vals, 0.0), axis=1)
        row_ids = jnp.searchsorted(jnp.cumsum(member), targets, side="left")
        picked = jnp.take(tokens, row_ids, axis=0, mode="fill", fill_value=0)
        pre_gate = jnp.dot(picked, wg_one, preferred_element_type=jnp.float32)
        pre_up = jnp.dot(picked, wu_one, preferred_element_type=jnp.float32)
        hidden = (jax.nn.silu(pre_gate) * pre_up).astype(jnp.bfloat16)
        expert_out = jnp.dot(hidden, wd_one, preferred_element_type=jnp.float32).astype(jnp.bfloat16)
        row_gate = jnp.take(row_weight, row_ids, mode="fill", fill_value=0.0)
        y_acc = y_acc.at[row_ids].add(row_gate[:, None] * expert_out.astype(jnp.float32), mode="drop")
        return y_acc, None

    y_init = jnp.zeros((TOKENS, D_MODEL), jnp.float32)
    y_sum, unused = lax.scan(expert_step, y_init, (jnp.arange(EXPERTS), w_gate, w_up, w_down))
    return y_sum.astype(jnp.bfloat16)
```

```python
import jax
import jax.numpy as jnp
from jax import lax
from jax.experimental import pallas as pl
from jax.experimental.pallas import tpu as pltpu
from jax.sharding import PartitionSpec as P

BF16 = jnp.bfloat16
F32 = jnp.float32
MESH = pl.DeviceIdType.MESH
N_DEV = 8
CAP = 32
SLOTS = 3
COLS = 256
VMEM = pl.BlockSpec(memory_space=pltpu.VMEM)
ANY = pl.BlockSpec(memory_space=pl.ANY)


def remote(src, dst, send_sem, recv_sem, peer):
    return pltpu.make_async_remote_copy(src_ref=src, dst_ref=dst, send_sem=send_sem, recv_sem=recv_sem, device_id={"ep": peer}, device_id_type=MESH)


def on_chip(shape, dtype):
    return pltpu.VMEM(shape, dtype)


def pin(v):
    return pltpu.with_memory_space_constraint(v, pltpu.VMEM)


def place():
    me = lax.axis_index("ep")
    core = lax.rem(me, 2)
    x = lax.rem(me // 2, 2)
    y = me // 4
    return me, core, x, y, me + 1 - 2 * core, me + 2 - 4 * x, me + 4 - 8 * y


def entry_barrier(me):
    barrier = pltpu.get_barrier_semaphore()
    for d in range(1, N_DEV):
        pl.semaphore_signal(barrier, inc=1, device_id={"ep": lax.rem(me + d, N_DEV)}, device_id_type=MESH)
    pl.semaphore_wait(barrier, N_DEV - 1)


def gather_kernel(tok, route_t, gate_t, wg, wu, w_out, x_out, sg_out, h_out, s_out, wd_out, pad, sg_loc, w_sem, sib_s, sib_r, link_s, link_r, sg_s, sg_r):
    me, core, x, y, sib, xn, yn = place()
    loads = []
    for e in range(SLOTS):
        loads.append(pltpu.make_async_copy(wg.at[e], w_out.at[e, 0], w_sem.at[e, 0]))
        loads.append(pltpu.make_async_copy(wu.at[e], w_out.at[e, 1], w_sem.at[e, 1]))
    for load in loads:
        load.start()
    entry_barrier(me)

    n_tok = tok.shape[0]
    half = n_tok // 2
    first, second = pl.ds(0, half), pl.ds(half, half)

    def rows(device, part=0, count=half):
        return x_out.at[pl.ds(pl.multiple_of(device * n_tok + part * half, half), count)]

    to_x_a = remote(tok.at[first], rows(me, 0), link_s.at[0], link_r.at[0], xn)
    to_x_b = remote(tok.at[second], rows(me, 1), link_s.at[1], link_r.at[1], xn)
    to_y_b = remote(tok.at[second], rows(me, 1), link_s.at[2], link_r.at[2], yn)
    to_y_a = remote(tok.at[first], rows(me, 0), link_s.at[3], link_r.at[3], yn)
    to_sib = remote(tok, rows(me, 0, n_tok), sib_s.at[0], sib_r.at[0], sib)
    for copy in (to_x_a, to_y_b, to_x_b, to_y_a, to_sib):
        copy.start()

    pad[...] = jnp.zeros_like(pad)
    pad[0, 0:6, 0:n_tok] = route_t[...].astype(F32)
    pad[1, 0:6, 0:n_tok] = gate_t[...]
    routes = pad[0] + pltpu.roll(pad[0], n_tok, 1)
    gates = pad[1] + pltpu.roll(pad[1], n_tok, 1)
    expert = lax.broadcasted_iota(jnp.int32, (64, 128), 0).astype(F32)
    lane = lax.broadcasted_iota(jnp.int32, (64, 128), 1)
    mine = (lane // n_tok) == core
    member = jnp.zeros((64, 128), F32)
    weight = jnp.zeros((64, 128), F32)
    for k in range(6):
        hit = (expert == routes[k : k + 1, :]) & mine
        member = jnp.where(hit, 1.0, member)
        weight = jnp.where(hit, gates[k : k + 1, :], weight)
    row = lax.broadcasted_iota(jnp.int32, (128, 128), 0)
    col = lax.broadcasted_iota(jnp.int32, (128, 128), 1)
    upto = jnp.where((row <= col), 1.0, 0.0).astype(BF16)
    rank = jnp.dot(member.astype(BF16), upto, preferred_element_type=F32)
    code = jnp.where(member > 0.5, rank + (me * CAP).astype(F32), 0.0)
    sg_loc[:, 0:8, :] = code.reshape(8, 8, 128)
    sg_loc[:, 8:16, :] = weight.reshape(8, 8, 128)
    sg_out[me] = sg_loc[me]
    sg_copies = []
    for d in range(1, N_DEV):
        peer = lax.rem(me + d, N_DEV)
        sg_copies.append(remote(sg_loc.at[peer], sg_out.at[me], sg_s.at[d], sg_r.at[d], peer))
    x_out[pl.ds(pl.multiple_of(me * n_tok, n_tok), n_tok), :] = tok[...]
    for copy in sg_copies:
        copy.start()

    dg = lax.rem(xn + 4, N_DEV)
    passed = []

    def pass_on(index, source, part):
        copy = remote(rows(source, part), rows(source, part), sib_s.at[index], sib_r.at[index], sib)
        copy.start()
        passed.append(copy)

    to_x_a.wait_recv()
    via_y = remote(rows(xn, 0), rows(xn, 0), link_s.at[4], link_r.at[4], yn)
    via_y.start()
    pass_on(1, xn, 0)
    to_y_b.wait_recv()
    via_x = remote(rows(yn, 1), rows(yn, 1), link_s.at[5], link_r.at[5], xn)
    via_x.start()
    pass_on(2, yn, 1)
    to_x_b.wait_recv()
    pass_on(3, xn, 1)
    to_y_a.wait_recv()
    pass_on(4, yn, 0)
    via_y.wait_recv()
    pass_on(5, dg, 0)
    via_x.wait_recv()
    pass_on(6, dg, 1)
    for copy in (to_x_a, to_x_b, to_y_b, to_y_a, via_y, via_x):
        copy.wait_send()
    to_sib.wait()
    for copy in passed + sg_copies:
        copy.wait()
    for load in loads:
        load.wait()


def hidden_kernel(w_in, h_in, s_in, wd_in, x_all, sg, wg, wu, wd, w_buf, h_out, s_out, wd_out, codes, xe, w_sem, d_sem):
    n_exp = wg.shape[0]
    d_ff = wg.shape[2]
    down = pltpu.make_async_copy(wd.at[:, :, pl.ds(0, COLS)], wd_out.at[0], d_sem)
    down.start()
    for p in range(4):
        codes[:, pl.ds(p * 128, 128)] = sg[2 * p, 0:8, :] + sg[2 * p + 1, 0:8, :]

    def load(e, part, src):
        s = lax.rem(e, SLOTS)
        return pltpu.make_async_copy(src.at[e], w_buf.at[s, part], w_sem.at[s, part])

    def hidden_rows(e, cap, slot):
        m = cap * N_DEV
        r = lax.broadcasted_iota(jnp.int32, (m, 512), 0)
        target = ((r // cap) * CAP + lax.rem(r, cap) + 1).astype(F32)
        pick = (target == codes[pl.ds(e, 1), :]).astype(BF16)
        for c in range(0, x_all.shape[1], 512):
            part = jnp.dot(pick, x_all[:, pl.ds(c, 512)], preferred_element_type=F32)
            xe[pl.ds(0, m), pl.ds(c, 512)] = part.astype(BF16)

        def put(act, c, w):
            if cap == CAP:
                h_out[e, :, pl.ds(c, w)] = act
            else:
                for i in range(N_DEV):
                    h_out[e, pl.ds(i * CAP, cap), pl.ds(c, w)] = act[i * cap : (i + 1) * cap]
                    h_out[e, pl.ds(i * CAP + cap, CAP - cap), pl.ds(c, w)] = jnp.zeros((CAP - cap, w), BF16)

        def act_of(a, b):
            return (a * jax.nn.sigmoid(a) * b).astype(BF16)

        rows = xe[pl.ds(0, m), :]
        for c in range(0, d_ff - 128, 256):
            a = jnp.dot(rows, w_buf[slot, 0, :, pl.ds(c, 256)], preferred_element_type=F32)
            b = jnp.dot(rows, w_buf[slot, 1, :, pl.ds(c, 256)], preferred_element_type=F32)
            put(act_of(a, b), c, 256)
        c = d_ff - 128
        both = jnp.concatenate([w_buf[slot, 0, :, pl.ds(c, 128)], w_buf[slot, 1, :, pl.ds(c, 128)]], axis=1)
        ab = jnp.dot(rows, both, preferred_element_type=F32)
        put(act_of(ab[:, :128], ab[:, 128:]), c, 128)

    def step(e, carry):
        slot = lax.rem(e, SLOTS)

        @pl.when(e >= SLOTS)
        def _():
            load(e, 0, wg).wait()
            load(e, 1, wu).wait()

        code_row = codes[pl.ds(e, 1), :]
        block = lax.broadcasted_iota(jnp.int32, (1, 512), 1) // 64
        most = jnp.max(code_row - (block * CAP).astype(F32))
        small = most <= 16.0

        @pl.when(small)
        def _():
            hidden_rows(e, CAP // 2, slot)

        @pl.when(jnp.logical_not(small))
        def _():
            hidden_rows(e, CAP, slot)

        @pl.when(e + SLOTS < n_exp)
        def _():
            load(e + SLOTS, 0, wg).start()
            load(e + SLOTS, 1, wu).start()

        return carry

    lax.fori_loop(0, n_exp, step, 0)

    r = lax.broadcasted_iota(jnp.int32, (256, 128), 0)
    lane = lax.broadcasted_iota(jnp.int32, (256, 128), 1)
    for p in range(4):
        target = ((2 * p + lane // 64) * CAP + lax.rem(r, CAP) + 1).astype(F32)
        code = sg[2 * p, 0:8, :] + sg[2 * p + 1, 0:8, :]
        gate = sg[2 * p, 8:16, :] + sg[2 * p + 1, 8:16, :]
        code = jnp.broadcast_to(code[:, None, :], (8, CAP, 128)).reshape(256, 128)
        gate = jnp.broadcast_to(gate[:, None, :], (8, CAP, 128)).reshape(256, 128)
        s_t = jnp.where(code == target, gate, 0.0)
        s_f = s_t.T
        hi = jnp.minimum(s_f, 3.3895e38).astype(BF16)
        rest = s_f - hi.astype(F32)
        mid = rest.astype(BF16)
        low = (rest - mid.astype(F32)).astype(BF16)
        s_out[p, 0] = hi
        s_out[p, 1] = mid
        s_out[p, 2] = low
    down.wait()


def combine_kernel(wd_in, h, s, wd, wd_buf, y_out, o, part, d2d, h1a, h1b, h2a, h2b, w_sem, ds, dr, h1as, h1ar, h1bs, h1br, h2as, h2ar, h2bs, h2br):
    me, core, x, y, sib, xn, yn = place()
    n_blk = wd.shape[2] // COLS
    half = 32
    first, second = pl.ds(0, half), pl.ds(half, half)

    def load(b):
        s_ = lax.rem(b, 2)
        return pltpu.make_async_copy(wd.at[:, :, pl.ds(pl.multiple_of(b * COLS, COLS), COLS)], wd_buf.at[s_], w_sem.at[s_])

    load(1).start()
    entry_barrier(me)

    def send_d2d(b):
        return remote(part.at[b, 1 - core], d2d.at[b], ds.at[b], dr.at[b], sib)

    def send_1a(b):
        return remote(part.at[b, core, :, 1 - x, first], h1a.at[b], h1as.at[b], h1ar.at[b], xn)

    def send_1b(b):
        return remote(part.at[b, core, 1 - y, :, second], h1b.at[b], h1bs.at[b], h1br.at[b], yn)

    def send_2a(b):
        return remote(part.at[b, core, 1 - y, x, first], h2a.at[b], h2as.at[b], h2ar.at[b], yn)

    def send_2b(b):
        return remote(part.at[b, core, y, 1 - x, second], h2b.at[b], h2bs.at[b], h2br.at[b], xn)

    def lag(b, k, body):
        @pl.when((b >= k) & (b < n_blk + k))
        def _():
            body(b - k)

    def stage_1(b):
        send_d2d(b).start()

    def stage_2(b):
        send_d2d(b).wait_recv()
        part[b, core] += d2d[b]
        send_1a(b).start()
        send_1b(b).start()

    def stage_3(b):
        send_1a(b).wait_recv()
        send_1b(b).wait_recv()
        part[b, core, :, x, first] += h1a[b]
        part[b, core, y, :, second] += h1b[b]
        send_2a(b).start()
        send_2b(b).start()

    def stage_4(b):
        send_2a(b).wait_recv()
        send_2b(b).wait_recv()
        cols = pl.ds(pl.multiple_of(b * COLS, COLS), COLS)
        y_out[first, cols] = (part[b, core, y, x, first] + h2a[b]).astype(BF16)
        y_out[second, cols] = (part[b, core, y, x, second] + h2b[b]).astype(BF16)

    def compute(b):
        slot = lax.rem(b, 2)

        @pl.when((b >= 1) & (b + 1 < n_blk))
        def _():
            load(b + 1).start()

        @pl.when(b >= 1)
        def _():
            load(b).wait()

        for e in range(h.shape[0]):
            out = jnp.dot(h[e], wd_buf[slot, e], preferred_element_type=F32).astype(BF16)
            for i in range(N_DEV):
                o[i, pl.ds(e * CAP, CAP), :] = out[i * CAP : (i + 1) * CAP]
        for i in range(N_DEV):
            gates = s[i // 2, :, pl.ds((i % 2) * 64, 64), :].reshape(192, 256)
            terms = jnp.dot(gates, o[i], preferred_element_type=F32)
            part[b, i % 2, i // 4, (i // 2) % 2] = terms[0:64] + terms[64:128] + terms[128:192]

    def step(b, carry):
        lag(b, 1, stage_1)
        lag(b, 2, stage_2)
        lag(b, 3, stage_3)
        lag(b, 4, stage_4)
        lag(b, 0, compute)
        return carry

    lax.fori_loop(0, n_blk + 4, step, 0)

    def drain(b, carry):
        for send in (send_d2d, send_1a, send_1b, send_2a, send_2b):
            send(b).wait_send()
        return carry

    lax.fori_loop(0, n_blk, drain, 0)


def solution(mesh):
    row_spec = P(("dp", "ep"))
    expert_spec = P("ep")
    dma = pltpu.SemaphoreType.DMA

    def local_step(tok, route, gate, wg, wu, wd):
        n_exp, d_model, d_ff = wg.shape
        n_tok = tok.shape[0]
        n_blk = d_model // COLS
        w_on, x_all, sg, h, s, wd_on = pl.pallas_call(
            gather_kernel,
            out_shape=[on_chip((SLOTS, 2, d_model, d_ff), BF16), on_chip((N_DEV * n_tok, d_model), BF16), on_chip((N_DEV, 16, 128), F32), on_chip((n_exp, N_DEV * CAP, d_ff), BF16), on_chip((4, 3, 128, 256), BF16), on_chip((2, n_exp, d_ff, COLS), BF16)],
            in_specs=[VMEM, VMEM, VMEM, ANY, ANY],
            out_specs=[VMEM] * 6,
            scratch_shapes=[pltpu.VMEM((2, 8, 128), F32), pltpu.VMEM((N_DEV, 16, 128), F32), dma((SLOTS, 2)), dma((7,)), dma((7,)), dma((6,)), dma((6,)), dma((N_DEV,)), dma((N_DEV,))],
            compiler_params=pltpu.CompilerParams(collective_id=0, has_side_effects=True, vmem_limit_bytes=6 << 20),
            name="gather",
        )(tok, route.T, gate.T, wg, wu)
        unused, h, s, wd_on = pl.pallas_call(
            hidden_kernel,
            out_shape=[on_chip(w_on.shape, BF16), on_chip((n_exp, N_DEV * CAP, d_ff), BF16), on_chip((4, 3, 128, 256), BF16), on_chip((2, n_exp, d_ff, COLS), BF16)],
            in_specs=[VMEM] * 6 + [ANY] * 3,
            out_specs=[VMEM] * 4,
            scratch_shapes=[pltpu.VMEM((8, 512), F32), pltpu.VMEM((256, d_model), BF16), dma((SLOTS, 2)), dma],
            input_output_aliases={0: 0, 1: 1, 2: 2, 3: 3},
            compiler_params=pltpu.CompilerParams(vmem_limit_bytes=6 << 20),
            name="hidden",
        )(pin(w_on), pin(h), pin(s), pin(wd_on), pin(x_all), pin(sg), wg, wu, wd)
        out = pl.pallas_call(
            combine_kernel,
            out_shape=[on_chip(wd_on.shape, BF16), jax.ShapeDtypeStruct((n_tok, d_model), BF16)],
            in_specs=[VMEM, VMEM, VMEM, ANY],
            out_specs=[VMEM] * 2,
            scratch_shapes=[
                pltpu.VMEM((N_DEV, 256, COLS), BF16),
                pltpu.VMEM((n_blk, 2, 2, 2, n_tok, COLS), F32),
                pltpu.VMEM((n_blk, 2, 2, n_tok, COLS), F32),
                pltpu.VMEM((n_blk, 2, n_tok // 2, COLS), F32),
                pltpu.VMEM((n_blk, 2, n_tok // 2, COLS), F32),
                pltpu.VMEM((n_blk, n_tok // 2, COLS), F32),
                pltpu.VMEM((n_blk, n_tok // 2, COLS), F32),
                dma((2,)),
            ]
            + [dma((n_blk,))] * 10,
            input_output_aliases={0: 0},
            compiler_params=pltpu.CompilerParams(collective_id=1, has_side_effects=True, vmem_limit_bytes=16 << 20),
            name="combine",
        )(pin(wd_on), pin(h), pin(s), wd)
        return out[1]

    return jax.shard_map(local_step, mesh=mesh, in_specs=(row_spec, row_spec, row_spec, expert_spec, expert_spec, expert_spec), out_specs=row_spec, check_vma=False)
```

```python
import jax
import jax.numpy as jnp
from jax import lax
from jax.experimental import pallas as pl
from jax.experimental.pallas import tpu as pltpu
from jax.sharding import PartitionSpec as P

BF16 = jnp.bfloat16
F32 = jnp.float32
MESH = pl.DeviceIdType.MESH
N_DEV = 8
CAP = 32
SLOTS = 4
FRONT = 6
LIMIT = 4 << 20
COLS = 256
VMEM = pl.BlockSpec(memory_space=pltpu.VMEM)
ANY = pl.BlockSpec(memory_space=pl.ANY)


def remote(src, dst, send_sem, recv_sem, peer):
    return pltpu.make_async_remote_copy(src_ref=src, dst_ref=dst, send_sem=send_sem, recv_sem=recv_sem, device_id={"ep": peer}, device_id_type=MESH)


def on_chip(shape, dtype):
    return pltpu.VMEM(shape, dtype)


def pin(v):
    return pltpu.with_memory_space_constraint(v, pltpu.VMEM)


def place():
    me = lax.axis_index("ep")
    core = lax.rem(me, 2)
    x = lax.rem(me // 2, 2)
    y = me // 4
    return me, core, x, y, me + 1 - 2 * core, me + 2 - 4 * x, me + 4 - 8 * y


def entry_barrier(me):
    barrier = pltpu.get_barrier_semaphore()
    for d in range(1, N_DEV):
        pl.semaphore_signal(barrier, inc=1, device_id={"ep": lax.rem(me + d, N_DEV)}, device_id_type=MESH)
    pl.semaphore_wait(barrier, N_DEV - 1)


def gather_kernel(tok, route_t, gate_t, wg, wu, wd, w_out, x_out, codes_out, h_out, s_out, wd_out, pad_i, pad_g, pad, sg_loc, sg, w_sem, d_sem, in_sem, sib_s, sib_r, link_s, link_r, sg_s, sg_r):
    me, core, x, y, sib, xn, yn = place()
    n_tok = tok.shape[0]
    half = n_tok // 2

    def rows(device, part=0, count=half):
        return x_out.at[pl.ds(pl.multiple_of(device * n_tok + part * half, half), count)]

    own = pltpu.make_async_copy(tok, rows(me, 0, n_tok), in_sem.at[0])
    own_route = pltpu.make_async_copy(route_t, pad_i, in_sem.at[1])
    own_gate = pltpu.make_async_copy(gate_t, pad_g, in_sem.at[2])
    own.start()
    own_route.start()
    own_gate.start()
    loads = []
    for e in range(SLOTS):
        loads.append(pltpu.make_async_copy(wg.at[e], w_out.at[e, 0], w_sem.at[e, 0]))
        loads.append(pltpu.make_async_copy(wu.at[e], w_out.at[e, 1], w_sem.at[e, 1]))
    loads.append(pltpu.make_async_copy(wd.at[:, :, pl.ds(0, COLS)], wd_out, d_sem))
    for load in loads:
        load.start()
    entry_barrier(me)

    to_x_a = remote(rows(me, 0), rows(me, 0), link_s.at[0], link_r.at[0], xn)
    to_x_b = remote(rows(me, 1), rows(me, 1), link_s.at[1], link_r.at[1], xn)
    to_y_b = remote(rows(me, 1), rows(me, 1), link_s.at[2], link_r.at[2], yn)
    to_y_a = remote(rows(me, 0), rows(me, 0), link_s.at[3], link_r.at[3], yn)
    to_sib = remote(rows(me, 0, n_tok), rows(me, 0, n_tok), sib_s.at[0], sib_r.at[0], sib)
    own.wait()
    for copy in (to_x_a, to_y_b, to_x_b, to_y_a, to_sib):
        copy.start()

    pad[...] = jnp.zeros_like(pad)
    own_route.wait()
    pad[0, 0:6, 0:n_tok] = pad_i[...].astype(F32)
    own_gate.wait()
    pad[1, 0:6, 0:n_tok] = pad_g[...]
    routes = pad[0] + pltpu.roll(pad[0], n_tok, 1)
    gates = pad[1] + pltpu.roll(pad[1], n_tok, 1)
    expert = lax.broadcasted_iota(jnp.int32, (64, 128), 0).astype(F32)
    lane = lax.broadcasted_iota(jnp.int32, (64, 128), 1)
    mine = (lane // n_tok) == core
    member = jnp.zeros((64, 128), F32)
    weight = jnp.zeros((64, 128), F32)
    for k in range(6):
        hit = (expert == routes[k : k + 1, :]) & mine
        member = jnp.where(hit, 1.0, member)
        weight = jnp.where(hit, gates[k : k + 1, :], weight)
    row = lax.broadcasted_iota(jnp.int32, (128, 128), 0)
    col = lax.broadcasted_iota(jnp.int32, (128, 128), 1)
    upto = jnp.where((row <= col), 1.0, 0.0).astype(BF16)
    rank = jnp.dot(member.astype(BF16), upto, preferred_element_type=F32)
    code = jnp.where(member > 0.5, rank + (me * CAP).astype(F32), 0.0)
    sg_loc[:, 0:8, :] = code.reshape(8, 8, 128)
    sg_loc[:, 8:16, :] = weight.reshape(8, 8, 128)
    sg[me] = sg_loc[me]
    sg_copies = []
    for d in range(1, N_DEV):
        peer = lax.rem(me + d, N_DEV)
        sg_copies.append(remote(sg_loc.at[peer], sg.at[me], sg_s.at[d], sg_r.at[d], peer))
    for copy in sg_copies:
        copy.start()
    for copy in sg_copies:
        copy.wait()

    r = lax.broadcasted_iota(jnp.int32, (256, 128), 0)
    lane = lax.broadcasted_iota(jnp.int32, (256, 128), 1)
    for p in range(4):
        target = ((2 * p + lane // 64) * CAP + lax.rem(r, CAP) + 1).astype(F32)
        code = sg[2 * p, 0:8, :] + sg[2 * p + 1, 0:8, :]
        gate = sg[2 * p, 8:16, :] + sg[2 * p + 1, 8:16, :]
        codes_out[:, pl.ds(p * 128, 128)] = code
        code = jnp.broadcast_to(code[:, None, :], (8, CAP, 128)).reshape(256, 128)
        gate = jnp.broadcast_to(gate[:, None, :], (8, CAP, 128)).reshape(256, 128)
        s_t = jnp.where(code == target, gate, 0.0)
        s_f = s_t.T
        hi = jnp.minimum(s_f, 3.3895e38).astype(BF16)
        rest = s_f - hi.astype(F32)
        mid = rest.astype(BF16)
        low = (rest - mid.astype(F32)).astype(BF16)
        s_out[p, 0] = hi
        s_out[p, 1] = mid
        s_out[p, 2] = low

    dg = lax.rem(xn + 4, N_DEV)
    passed = []

    def pass_on(index, source, part):
        copy = remote(rows(source, part), rows(source, part), sib_s.at[index], sib_r.at[index], sib)
        copy.start()
        passed.append(copy)

    to_x_a.wait_recv()
    via_y = remote(rows(xn, 0), rows(xn, 0), link_s.at[4], link_r.at[4], yn)
    via_y.start()
    pass_on(1, xn, 0)
    to_y_b.wait_recv()
    via_x = remote(rows(yn, 1), rows(yn, 1), link_s.at[5], link_r.at[5], xn)
    via_x.start()
    pass_on(2, yn, 1)
    to_x_b.wait_recv()
    pass_on(3, xn, 1)
    to_y_a.wait_recv()
    pass_on(4, yn, 0)
    via_y.wait_recv()
    pass_on(5, dg, 0)
    via_x.wait_recv()
    pass_on(6, dg, 1)
    for copy in (to_x_a, to_x_b, to_y_b, to_y_a, via_y, via_x):
        copy.wait_send()
    to_sib.wait()
    for copy in passed:
        copy.wait()
    for load in loads:
        load.wait()


def hidden_kernel(w_in, h_in, x_all, codes, wg, wu, w_buf, h_out, xe, w_sem):
    n_exp = wg.shape[0]
    d_ff = wg.shape[2]

    def load(e, part, src):
        s = lax.rem(e, SLOTS)
        return pltpu.make_async_copy(src.at[e], w_buf.at[s, part], w_sem.at[s, part])

    def hidden_rows(e, cap, slot):
        m = cap * N_DEV
        r = lax.broadcasted_iota(jnp.int32, (m, 512), 0)
        target = ((r // cap) * CAP + lax.rem(r, cap) + 1).astype(F32)
        pick = (target == codes[pl.ds(e, 1), :]).astype(BF16)
        for c in range(0, x_all.shape[1], 512):
            part = jnp.dot(pick, x_all[:, pl.ds(c, 512)], preferred_element_type=F32)
            xe[pl.ds(0, m), pl.ds(c, 512)] = part.astype(BF16)

        def put(act, c, w):
            if cap == CAP:
                h_out[e, :, pl.ds(c, w)] = act
            else:
                for i in range(N_DEV):
                    h_out[e, pl.ds(i * CAP, cap), pl.ds(c, w)] = act[i * cap : (i + 1) * cap]
                    h_out[e, pl.ds(i * CAP + cap, CAP - cap), pl.ds(c, w)] = jnp.zeros((CAP - cap, w), BF16)

        def act_of(a, b):
            return (a * jax.nn.sigmoid(a) * b).astype(BF16)

        rows = xe[pl.ds(0, m), :]
        for c in range(0, d_ff - 128, 256):
            a = jnp.dot(rows, w_buf[slot, 0, :, pl.ds(c, 256)], preferred_element_type=F32)
            b = jnp.dot(rows, w_buf[slot, 1, :, pl.ds(c, 256)], preferred_element_type=F32)
            put(act_of(a, b), c, 256)
        c = d_ff - 128
        both = jnp.concatenate([w_buf[slot, 0, :, pl.ds(c, 128)], w_buf[slot, 1, :, pl.ds(c, 128)]], axis=1)
        ab = jnp.dot(rows, both, preferred_element_type=F32)
        put(act_of(ab[:, :128], ab[:, 128:]), c, 128)

    def step(e, carry):
        slot = lax.rem(e, SLOTS)

        @pl.when(e >= SLOTS)
        def _():
            load(e, 0, wg).wait()
            load(e, 1, wu).wait()

        code_row = codes[pl.ds(e, 1), :]
        block = lax.broadcasted_iota(jnp.int32, (1, 512), 1) // 64
        most = jnp.max(code_row - (block * CAP).astype(F32))
        small = most <= 16.0

        @pl.when(small)
        def _():
            hidden_rows(e, CAP // 2, slot)

        @pl.when(jnp.logical_not(small))
        def _():
            hidden_rows(e, CAP, slot)

        @pl.when(e + SLOTS < n_exp)
        def _():
            load(e + SLOTS, 0, wg).start()
            load(e + SLOTS, 1, wu).start()

        return carry

    lax.fori_loop(0, n_exp, step, 0)


def combine_kernel(h, s, wd_on, wd, y_out, wd_buf, o, part, d2d, h1a, h1b, h2a, h2b, w_sem, ds, dr, h1as, h1ar, h1bs, h1br, h2as, h2ar, h2bs, h2br):
    me, core, x, y, sib, xn, yn = place()
    n_blk = wd.shape[2] // COLS
    n_buf = wd_buf.shape[0]
    n_exp = h.shape[0]
    half = 32
    first, second = pl.ds(0, half), pl.ds(half, half)

    def load(b):
        slot = lax.rem(b - 1, n_buf)
        return pltpu.make_async_copy(wd.at[:, :, pl.ds(pl.multiple_of(b * COLS, COLS), COLS)], wd_buf.at[slot], w_sem.at[slot])

    for b in range(1, n_buf + 1):
        load(b).start()
    entry_barrier(me)

    def send_d2d(b):
        return remote(part.at[b, 1 - core], d2d.at[b], ds.at[b], dr.at[b], sib)

    def send_1a(b):
        return remote(part.at[b, core, :, 1 - x, first], h1a.at[b], h1as.at[b], h1ar.at[b], xn)

    def send_1b(b):
        return remote(part.at[b, core, 1 - y, :, second], h1b.at[b], h1bs.at[b], h1br.at[b], yn)

    def send_2a(b):
        return remote(part.at[b, core, 1 - y, x, first], h2a.at[b], h2as.at[b], h2ar.at[b], yn)

    def send_2b(b):
        return remote(part.at[b, core, y, 1 - x, second], h2b.at[b], h2bs.at[b], h2br.at[b], xn)

    def lag(b, k, body):
        @pl.when((b >= k) & (b < n_blk + k))
        def _():
            body(b - k)

    def stage_1(b):
        send_d2d(b).start()

    def stage_2(b):
        send_d2d(b).wait_recv()
        part[b, core] += d2d[b]
        send_1a(b).start()
        send_1b(b).start()

    def stage_3(b):
        send_1a(b).wait_recv()
        send_1b(b).wait_recv()
        part[b, core, :, x, first] += h1a[b]
        part[b, core, y, :, second] += h1b[b]
        send_2a(b).start()
        send_2b(b).start()

    def stage_4(b):
        send_2a(b).wait_recv()
        send_2b(b).wait_recv()
        cols = pl.ds(pl.multiple_of(b * COLS, COLS), COLS)
        y_out[first, cols] = (part[b, core, y, x, first] + h2a[b]).astype(BF16)
        y_out[second, cols] = (part[b, core, y, x, second] + h2b[b]).astype(BF16)

    def down(e, weights):
        out = jnp.dot(h[e], weights[e], preferred_element_type=F32).astype(BF16)
        for i in range(N_DEV):
            o[i, pl.ds(e * CAP, CAP), :] = out[i * CAP : (i + 1) * CAP]

    def on_weights(b, body):
        @pl.when(b == 0)
        def _():
            body(wd_on)

        @pl.when((b >= 1) & (b < n_blk))
        def _():
            body(wd_buf.at[lax.rem(b - 1, n_buf)])

    def step(b, carry):
        lag(b, 1, stage_1)

        @pl.when((b >= 1) & (b < n_blk))
        def _():
            load(b).wait()

        def front(weights):
            for e in range(FRONT):
                down(e, weights)

        on_weights(b, front)
        lag(b, 1, stage_2)
        lag(b, 3, stage_3)
        lag(b, 5, stage_4)

        def back(weights):
            for e in range(FRONT, n_exp):
                down(e, weights)
            for i in range(N_DEV):
                gates = s[i // 2, :, pl.ds((i % 2) * 64, 64), :].reshape(192, 256)
                terms = jnp.dot(gates, o[i], preferred_element_type=F32)
                part[b, i % 2, i // 4, (i // 2) % 2] = terms[0:64] + terms[64:128] + terms[128:192]

        on_weights(b, back)

        @pl.when((b >= 1) & (b + n_buf < n_blk))
        def _():
            load(b + n_buf).start()

        return carry

    lax.fori_loop(0, n_blk + 5, step, 0)

    def drain(b, carry):
        for send in (send_d2d, send_1a, send_1b, send_2a, send_2b):
            send(b).wait_send()
        return carry

    lax.fori_loop(0, n_blk, drain, 0)


def solution(mesh):
    row_spec = P(("dp", "ep"))
    expert_spec = P("ep")
    dma = pltpu.SemaphoreType.DMA

    def local_step(tok, route, gate, wg, wu, wd):
        n_exp, d_model, d_ff = wg.shape
        n_tok = tok.shape[0]
        n_blk = d_model // COLS
        hidden = (n_exp, N_DEV * CAP, d_ff)
        w_on, x_all, codes, h, s, wd_on = pl.pallas_call(
            gather_kernel,
            out_shape=[on_chip((SLOTS, 2, d_model, d_ff), BF16), on_chip((N_DEV * n_tok, d_model), BF16), on_chip((8, 512), F32), on_chip(hidden, BF16), on_chip((4, 3, 128, 256), BF16), on_chip((n_exp, d_ff, COLS), BF16)],
            in_specs=[ANY] * 6,
            out_specs=[VMEM] * 6,
            scratch_shapes=[
                pltpu.VMEM((6, n_tok), jnp.int32),
                pltpu.VMEM((6, n_tok), F32),
                pltpu.VMEM((2, 8, 128), F32),
                pltpu.VMEM((N_DEV, 16, 128), F32),
                pltpu.VMEM((N_DEV, 16, 128), F32),
                dma((SLOTS, 2)),
                dma,
                dma((3,)),
                dma((7,)),
                dma((7,)),
                dma((6,)),
                dma((6,)),
                dma((N_DEV,)),
                dma((N_DEV,)),
            ],
            compiler_params=pltpu.CompilerParams(collective_id=0, has_side_effects=True, vmem_limit_bytes=LIMIT),
            name="gather",
        )(tok, route.T, gate.T, wg, wu, wd)
        unused, h = pl.pallas_call(
            hidden_kernel,
            out_shape=[on_chip(w_on.shape, BF16), on_chip(hidden, BF16)],
            in_specs=[VMEM] * 4 + [ANY] * 2,
            out_specs=[VMEM] * 2,
            scratch_shapes=[pltpu.VMEM((256, d_model), BF16), dma((SLOTS, 2))],
            input_output_aliases={0: 0, 1: 1},
            compiler_params=pltpu.CompilerParams(vmem_limit_bytes=LIMIT),
            name="hidden",
        )(pin(w_on), pin(h), pin(x_all), pin(codes), wg, wu)
        return pl.pallas_call(
            combine_kernel,
            out_shape=jax.ShapeDtypeStruct((n_tok, d_model), BF16),
            in_specs=[VMEM] * 3 + [ANY],
            out_specs=VMEM,
            scratch_shapes=[
                pltpu.VMEM((3, n_exp, d_ff, COLS), BF16),
                pltpu.VMEM((N_DEV, 256, COLS), BF16),
                pltpu.VMEM((n_blk, 2, 2, 2, n_tok, COLS), F32),
                pltpu.VMEM((n_blk, 2, 2, n_tok, COLS), F32),
                pltpu.VMEM((n_blk, 2, n_tok // 2, COLS), F32),
                pltpu.VMEM((n_blk, 2, n_tok // 2, COLS), F32),
                pltpu.VMEM((n_blk, n_tok // 2, COLS), F32),
                pltpu.VMEM((n_blk, n_tok // 2, COLS), F32),
                dma((3,)),
            ]
            + [dma((n_blk,))] * 10,
            compiler_params=pltpu.CompilerParams(collective_id=1, has_side_effects=True, vmem_limit_bytes=32 << 20),
            name="combine",
        )(pin(h), pin(s), pin(wd_on), wd)

    return jax.shard_map(local_step, mesh=mesh, in_specs=(row_spec, row_spec, row_spec, expert_spec, expert_spec, expert_spec), out_specs=row_spec, check_vma=False)
```

```python
import jax
import jax.numpy as jnp
from jax import lax
from jax.experimental import pallas as pl
from jax.experimental.pallas import tpu as pltpu
from jax.sharding import PartitionSpec as P

BF16 = jnp.bfloat16
F32 = jnp.float32
MESH = pl.DeviceIdType.MESH
N_DEV = 8
CAP = 32
SLOTS = 4
FRONT = 6
LIMIT = 4 << 20
COLS = 256
VMEM = pl.BlockSpec(memory_space=pltpu.VMEM)
ANY = pl.BlockSpec(memory_space=pl.ANY)


def remote(src, dst, send_sem, recv_sem, peer):
    return pltpu.make_async_remote_copy(src_ref=src, dst_ref=dst, send_sem=send_sem, recv_sem=recv_sem, device_id={"ep": peer}, device_id_type=MESH)


def on_chip(shape, dtype):
    return pltpu.VMEM(shape, dtype)


def pin(v):
    return pltpu.with_memory_space_constraint(v, pltpu.VMEM)


def place():
    me = lax.axis_index("ep")
    core = lax.rem(me, 2)
    x = lax.rem(me // 2, 2)
    y = me // 4
    return me, core, x, y, me + 1 - 2 * core, me + 2 - 4 * x, me + 4 - 8 * y


def entry_barrier(me):
    barrier = pltpu.get_barrier_semaphore()
    for d in range(1, N_DEV):
        pl.semaphore_signal(barrier, inc=1, device_id={"ep": lax.rem(me + d, N_DEV)}, device_id_type=MESH)
    pl.semaphore_wait(barrier, N_DEV - 1)


def gather_kernel(tok, route_t, gate_t, wg, wu, wd, w_out, x_out, codes_out, h_out, s_out, wd_out, pad_i, pad_g, pad, sg_loc, sg, w_sem, d_sem, in_sem, sib_s, sib_r, link_s, link_r, sg_s, sg_r):
    me, core, x, y, sib, xn, yn = place()
    n_tok = tok.shape[0]
    half = n_tok // 2

    def rows(device, part=0, count=half):
        return x_out.at[pl.ds(pl.multiple_of(device * n_tok + part * half, half), count)]

    own = pltpu.make_async_copy(tok, rows(me, 0, n_tok), in_sem.at[0])
    own_route = pltpu.make_async_copy(route_t, pad_i, in_sem.at[1])
    own_gate = pltpu.make_async_copy(gate_t, pad_g, in_sem.at[2])
    own.start()
    own_route.start()
    own_gate.start()
    loads = []
    for e in range(SLOTS):
        loads.append(pltpu.make_async_copy(wg.at[e], w_out.at[e, 0], w_sem.at[e, 0]))
        loads.append(pltpu.make_async_copy(wu.at[e], w_out.at[e, 1], w_sem.at[e, 1]))
    loads.append(pltpu.make_async_copy(wd.at[:, :, pl.ds(0, COLS)], wd_out, d_sem))
    entry_barrier(me)

    def bring(count):
        for load in loads[bring.done : bring.done + count]:
            load.start()
        bring.done += count

    bring.done = 0
    to_x_a = remote(rows(me, 0), rows(me, 0), link_s.at[0], link_r.at[0], xn)
    to_x_b = remote(rows(me, 1), rows(me, 1), link_s.at[1], link_r.at[1], xn)
    to_y_b = remote(rows(me, 1), rows(me, 1), link_s.at[2], link_r.at[2], yn)
    to_y_a = remote(rows(me, 0), rows(me, 0), link_s.at[3], link_r.at[3], yn)
    to_sib = remote(rows(me, 0, n_tok), rows(me, 0, n_tok), sib_s.at[0], sib_r.at[0], sib)
    own.wait()
    for copy in (to_x_a, to_y_b, to_x_b, to_y_a, to_sib):
        copy.start()
    bring(4)

    pad[...] = jnp.zeros_like(pad)
    own_route.wait()
    pad[0, 0:6, 0:n_tok] = pad_i[...].astype(F32)
    own_gate.wait()
    pad[1, 0:6, 0:n_tok] = pad_g[...]
    routes = pad[0] + pltpu.roll(pad[0], n_tok, 1)
    gates = pad[1] + pltpu.roll(pad[1], n_tok, 1)
    expert = lax.broadcasted_iota(jnp.int32, (64, 128), 0).astype(F32)
    lane = lax.broadcasted_iota(jnp.int32, (64, 128), 1)
    mine = (lane // n_tok) == core
    member = jnp.zeros((64, 128), F32)
    weight = jnp.zeros((64, 128), F32)
    for k in range(6):
        hit = (expert == routes[k : k + 1, :]) & mine
        member = jnp.where(hit, 1.0, member)
        weight = jnp.where(hit, gates[k : k + 1, :], weight)
    row = lax.broadcasted_iota(jnp.int32, (128, 128), 0)
    col = lax.broadcasted_iota(jnp.int32, (128, 128), 1)
    upto = jnp.where((row <= col), 1.0, 0.0).astype(BF16)
    rank = jnp.dot(member.astype(BF16), upto, preferred_element_type=F32)
    code = jnp.where(member > 0.5, rank + (me * CAP).astype(F32), 0.0)
    sg_loc[:, 0:8, :] = code.reshape(8, 8, 128)
    sg_loc[:, 8:16, :] = weight.reshape(8, 8, 128)
    sg[me] = sg_loc[me]
    sg_copies = []
    for d in range(1, N_DEV):
        peer = lax.rem(me + d, N_DEV)
        sg_copies.append(remote(sg_loc.at[peer], sg.at[me], sg_s.at[d], sg_r.at[d], peer))
    for copy in sg_copies:
        copy.start()
    for copy in sg_copies:
        copy.wait()

    r = lax.broadcasted_iota(jnp.int32, (256, 128), 0)
    lane = lax.broadcasted_iota(jnp.int32, (256, 128), 1)
    for p in range(4):
        target = ((2 * p + lane // 64) * CAP + lax.rem(r, CAP) + 1).astype(F32)
        code = sg[2 * p, 0:8, :] + sg[2 * p + 1, 0:8, :]
        gate = sg[2 * p, 8:16, :] + sg[2 * p + 1, 8:16, :]
        codes_out[:, pl.ds(p * 128, 128)] = code
        code = jnp.broadcast_to(code[:, None, :], (8, CAP, 128)).reshape(256, 128)
        gate = jnp.broadcast_to(gate[:, None, :], (8, CAP, 128)).reshape(256, 128)
        s_t = jnp.where(code == target, gate, 0.0)
        s_f = s_t.T
        hi = jnp.minimum(s_f, 3.3895e38).astype(BF16)
        rest = s_f - hi.astype(F32)
        mid = rest.astype(BF16)
        low = (rest - mid.astype(F32)).astype(BF16)
        s_out[p, 0] = hi
        s_out[p, 1] = mid
        s_out[p, 2] = low

    dg = lax.rem(xn + 4, N_DEV)
    passed = []

    def pass_on(index, source, part):
        copy = remote(rows(source, part), rows(source, part), sib_s.at[index], sib_r.at[index], sib)
        copy.start()
        passed.append(copy)

    to_x_a.wait_recv()
    via_y = remote(rows(xn, 0), rows(xn, 0), link_s.at[4], link_r.at[4], yn)
    via_y.start()
    pass_on(1, xn, 0)
    bring(1)
    to_y_b.wait_recv()
    via_x = remote(rows(yn, 1), rows(yn, 1), link_s.at[5], link_r.at[5], xn)
    via_x.start()
    pass_on(2, yn, 1)
    bring(1)
    to_x_b.wait_recv()
    pass_on(3, xn, 1)
    bring(1)
    to_y_a.wait_recv()
    pass_on(4, yn, 0)
    bring(1)
    via_y.wait_recv()
    pass_on(5, dg, 0)
    via_x.wait_recv()
    pass_on(6, dg, 1)
    bring(1)
    for copy in (to_x_a, to_x_b, to_y_b, to_y_a, via_y, via_x):
        copy.wait_send()
    to_sib.wait()
    for copy in passed:
        copy.wait()
    for load in loads:
        load.wait()


def hidden_kernel(w_in, h_in, x_all, codes, wg, wu, w_buf, h_out, xe, w_sem):
    n_exp = wg.shape[0]
    d_ff = wg.shape[2]

    def load(e, part, src):
        s = lax.rem(e, SLOTS)
        return pltpu.make_async_copy(src.at[e], w_buf.at[s, part], w_sem.at[s, part])

    def hidden_rows(e, cap, slot):
        m = cap * N_DEV
        r = lax.broadcasted_iota(jnp.int32, (m, 512), 0)
        target = ((r // cap) * CAP + lax.rem(r, cap) + 1).astype(F32)
        pick = (target == codes[pl.ds(e, 1), :]).astype(BF16)
        for c in range(0, x_all.shape[1], 512):
            part = jnp.dot(pick, x_all[:, pl.ds(c, 512)], preferred_element_type=F32)
            xe[pl.ds(0, m), pl.ds(c, 512)] = part.astype(BF16)

        def put(act, c, w):
            if cap == CAP:
                h_out[e, :, pl.ds(c, w)] = act
            else:
                for i in range(N_DEV):
                    h_out[e, pl.ds(i * CAP, cap), pl.ds(c, w)] = act[i * cap : (i + 1) * cap]
                    h_out[e, pl.ds(i * CAP + cap, CAP - cap), pl.ds(c, w)] = jnp.zeros((CAP - cap, w), BF16)

        def act_of(a, b):
            return (a * jax.nn.sigmoid(a) * b).astype(BF16)

        rows = xe[pl.ds(0, m), :]
        for c in range(0, d_ff - 128, 256):
            a = jnp.dot(rows, w_buf[slot, 0, :, pl.ds(c, 256)], preferred_element_type=F32)
            b = jnp.dot(rows, w_buf[slot, 1, :, pl.ds(c, 256)], preferred_element_type=F32)
            put(act_of(a, b), c, 256)
        c = d_ff - 128
        both = jnp.concatenate([w_buf[slot, 0, :, pl.ds(c, 128)], w_buf[slot, 1, :, pl.ds(c, 128)]], axis=1)
        ab = jnp.dot(rows, both, preferred_element_type=F32)
        put(act_of(ab[:, :128], ab[:, 128:]), c, 128)

    def step(e, carry):
        slot = lax.rem(e, SLOTS)

        @pl.when(e >= SLOTS)
        def _():
            load(e, 0, wg).wait()
            load(e, 1, wu).wait()

        code_row = codes[pl.ds(e, 1), :]
        block = lax.broadcasted_iota(jnp.int32, (1, 512), 1) // 64
        most = jnp.max(code_row - (block * CAP).astype(F32))
        small = most <= 16.0

        @pl.when(small)
        def _():
            hidden_rows(e, CAP // 2, slot)

        @pl.when(jnp.logical_not(small))
        def _():
            hidden_rows(e, CAP, slot)

        @pl.when(e + SLOTS < n_exp)
        def _():
            load(e + SLOTS, 0, wg).start()
            load(e + SLOTS, 1, wu).start()

        return carry

    lax.fori_loop(0, n_exp, step, 0)


def combine_kernel(h, s, wd_on, wd, y_out, wd_buf, o, part, d2d, h1a, h1b, h2a, h2b, w_sem, ds, dr, h1as, h1ar, h1bs, h1br, h2as, h2ar, h2bs, h2br):
    me, core, x, y, sib, xn, yn = place()
    n_blk = wd.shape[2] // COLS
    n_buf = wd_buf.shape[0]
    n_exp = h.shape[0]
    half = 32
    first, second = pl.ds(0, half), pl.ds(half, half)

    def load(b):
        slot = lax.rem(b - 1, n_buf)
        return pltpu.make_async_copy(wd.at[:, :, pl.ds(pl.multiple_of(b * COLS, COLS), COLS)], wd_buf.at[slot], w_sem.at[slot])

    for b in range(1, n_buf + 1):
        load(b).start()
    entry_barrier(me)

    def send_d2d(b):
        return remote(part.at[b, 1 - core], d2d.at[b], ds.at[b], dr.at[b], sib)

    def send_1a(b):
        return remote(part.at[b, core, :, 1 - x, first], h1a.at[b], h1as.at[b], h1ar.at[b], xn)

    def send_1b(b):
        return remote(part.at[b, core, 1 - y, :, second], h1b.at[b], h1bs.at[b], h1br.at[b], yn)

    def send_2a(b):
        return remote(part.at[b, core, 1 - y, x, first], h2a.at[b], h2as.at[b], h2ar.at[b], yn)

    def send_2b(b):
        return remote(part.at[b, core, y, 1 - x, second], h2b.at[b], h2bs.at[b], h2br.at[b], xn)

    def lag(b, k, body):
        @pl.when((b >= k) & (b < n_blk + k))
        def _():
            body(b - k)

    def stage_1(b):
        send_d2d(b).start()

    def stage_2(b):
        send_d2d(b).wait_recv()
        part[b, core] += d2d[b]
        send_1a(b).start()
        send_1b(b).start()

    def stage_3(b):
        send_1a(b).wait_recv()
        send_1b(b).wait_recv()
        part[b, core, :, x, first] += h1a[b]
        part[b, core, y, :, second] += h1b[b]
        send_2a(b).start()
        send_2b(b).start()

    def stage_4(b):
        send_2a(b).wait_recv()
        send_2b(b).wait_recv()
        cols = pl.ds(pl.multiple_of(b * COLS, COLS), COLS)
        y_out[first, cols] = (part[b, core, y, x, first] + h2a[b]).astype(BF16)
        y_out[second, cols] = (part[b, core, y, x, second] + h2b[b]).astype(BF16)

    def down(e, weights):
        out = jnp.dot(h[e], weights[e], preferred_element_type=F32).astype(BF16)
        for i in range(N_DEV):
            o[i, pl.ds(e * CAP, CAP), :] = out[i * CAP : (i + 1) * CAP]

    def on_weights(b, body):
        @pl.when(b == 0)
        def _():
            body(wd_on)

        @pl.when((b >= 1) & (b < n_blk))
        def _():
            body(wd_buf.at[lax.rem(b - 1, n_buf)])

    def step(b, carry):
        lag(b, 1, stage_1)

        @pl.when((b >= 1) & (b < n_blk))
        def _():
            load(b).wait()

        def front(weights):
            for e in range(FRONT):
                down(e, weights)

        on_weights(b, front)
        lag(b, 1, stage_2)
        lag(b, 3, stage_3)
        lag(b, 5, stage_4)

        def back(weights):
            for e in range(FRONT, n_exp):
                down(e, weights)
            for i in range(N_DEV):
                gates = s[i // 2, :, pl.ds((i % 2) * 64, 64), :].reshape(192, 256)
                terms = jnp.dot(gates, o[i], preferred_element_type=F32)
                part[b, i % 2, i // 4, (i // 2) % 2] = terms[0:64] + terms[64:128] + terms[128:192]

        on_weights(b, back)

        @pl.when((b >= 1) & (b + n_buf < n_blk))
        def _():
            load(b + n_buf).start()

        return carry

    lax.fori_loop(0, n_blk + 5, step, 0)

    def drain(b, carry):
        for send in (send_d2d, send_1a, send_1b, send_2a, send_2b):
            send(b).wait_send()
        return carry

    lax.fori_loop(0, n_blk, drain, 0)


def solution(mesh):
    row_spec = P(("dp", "ep"))
    expert_spec = P("ep")
    dma = pltpu.SemaphoreType.DMA

    def local_step(tok, route, gate, wg, wu, wd):
        n_exp, d_model, d_ff = wg.shape
        n_tok = tok.shape[0]
        n_blk = d_model // COLS
        hidden = (n_exp, N_DEV * CAP, d_ff)
        w_on, x_all, codes, h, s, wd_on = pl.pallas_call(
            gather_kernel,
            out_shape=[on_chip((SLOTS, 2, d_model, d_ff), BF16), on_chip((N_DEV * n_tok, d_model), BF16), on_chip((8, 512), F32), on_chip(hidden, BF16), on_chip((4, 3, 128, 256), BF16), on_chip((n_exp, d_ff, COLS), BF16)],
            in_specs=[ANY] * 6,
            out_specs=[VMEM] * 6,
            scratch_shapes=[
                pltpu.VMEM((6, n_tok), jnp.int32),
                pltpu.VMEM((6, n_tok), F32),
                pltpu.VMEM((2, 8, 128), F32),
                pltpu.VMEM((N_DEV, 16, 128), F32),
                pltpu.VMEM((N_DEV, 16, 128), F32),
                dma((SLOTS, 2)),
                dma,
                dma((3,)),
                dma((7,)),
                dma((7,)),
                dma((6,)),
                dma((6,)),
                dma((N_DEV,)),
                dma((N_DEV,)),
            ],
            compiler_params=pltpu.CompilerParams(collective_id=0, has_side_effects=True, vmem_limit_bytes=LIMIT),
            name="gather",
        )(tok, route.T, gate.T, wg, wu, wd)
        unused, h = pl.pallas_call(
            hidden_kernel,
            out_shape=[on_chip(w_on.shape, BF16), on_chip(hidden, BF16)],
            in_specs=[VMEM] * 4 + [ANY] * 2,
            out_specs=[VMEM] * 2,
            scratch_shapes=[pltpu.VMEM((256, d_model), BF16), dma((SLOTS, 2))],
            input_output_aliases={0: 0, 1: 1},
            compiler_params=pltpu.CompilerParams(vmem_limit_bytes=LIMIT),
            name="hidden",
        )(pin(w_on), pin(h), pin(x_all), pin(codes), wg, wu)
        return pl.pallas_call(
            combine_kernel,
            out_shape=jax.ShapeDtypeStruct((n_tok, d_model), BF16),
            in_specs=[VMEM] * 3 + [ANY],
            out_specs=VMEM,
            scratch_shapes=[
                pltpu.VMEM((3, n_exp, d_ff, COLS), BF16),
                pltpu.VMEM((N_DEV, 256, COLS), BF16),
                pltpu.VMEM((n_blk, 2, 2, 2, n_tok, COLS), F32),
                pltpu.VMEM((n_blk, 2, 2, n_tok, COLS), F32),
                pltpu.VMEM((n_blk, 2, n_tok // 2, COLS), F32),
                pltpu.VMEM((n_blk, 2, n_tok // 2, COLS), F32),
                pltpu.VMEM((n_blk, n_tok // 2, COLS), F32),
                pltpu.VMEM((n_blk, n_tok // 2, COLS), F32),
                dma((3,)),
            ]
            + [dma((n_blk,))] * 10,
            compiler_params=pltpu.CompilerParams(collective_id=1, has_side_effects=True, vmem_limit_bytes=32 << 20),
            name="combine",
        )(pin(h), pin(s), pin(wd_on), wd)

    return jax.shard_map(local_step, mesh=mesh, in_specs=(row_spec, row_spec, row_spec, expert_spec, expert_spec, expert_spec), out_specs=row_spec, check_vma=False)
```

```python
import jax
import jax.numpy as jnp
from jax import lax
from jax.experimental import pallas as pl
from jax.experimental.pallas import tpu as pltpu
from jax.sharding import PartitionSpec as P

BF16 = jnp.bfloat16
F32 = jnp.float32
MESH = pl.DeviceIdType.MESH
N_DEV = 8
CAP = 32
SLOTS = 4
EARLY = 3
FRONT = 6
LIMIT = 4 << 20
COLS = 256
VMEM = pl.BlockSpec(memory_space=pltpu.VMEM)
ANY = pl.BlockSpec(memory_space=pl.ANY)


def remote(src, dst, send_sem, recv_sem, peer):
    return pltpu.make_async_remote_copy(src_ref=src, dst_ref=dst, send_sem=send_sem, recv_sem=recv_sem, device_id={"ep": peer}, device_id_type=MESH)


def on_chip(shape, dtype):
    return pltpu.VMEM(shape, dtype)


def pin(v):
    return pltpu.with_memory_space_constraint(v, pltpu.VMEM)


def place():
    me = lax.axis_index("ep")
    core = lax.rem(me, 2)
    x = lax.rem(me // 2, 2)
    y = me // 4
    return me, core, x, y, me + 1 - 2 * core, me + 2 - 4 * x, me + 4 - 8 * y


def entry_barrier(me):
    barrier = pltpu.get_barrier_semaphore()
    for d in range(1, N_DEV):
        pl.semaphore_signal(barrier, inc=1, device_id={"ep": lax.rem(me + d, N_DEV)}, device_id_type=MESH)
    pl.semaphore_wait(barrier, N_DEV - 1)


def gather_kernel(tok, route_t, gate_t, wg, wu, w_out, x_out, codes_out, h_out, s_out, wd_out, pad_i, pad_g, pad, sg_loc, sg, w_sem, in_sem, sib_s, sib_r, link_s, link_r, sg_s, sg_r):
    me, core, x, y, sib, xn, yn = place()
    n_tok = tok.shape[0]
    half = n_tok // 2

    def rows(device, part=0, count=half):
        return x_out.at[pl.ds(pl.multiple_of(device * n_tok + part * half, half), count)]

    own = pltpu.make_async_copy(tok, rows(me, 0, n_tok), in_sem.at[0])
    own_route = pltpu.make_async_copy(route_t, pad_i, in_sem.at[1])
    own_gate = pltpu.make_async_copy(gate_t, pad_g, in_sem.at[2])
    own.start()
    own_route.start()
    own_gate.start()
    barrier = pltpu.get_barrier_semaphore()
    for d in range(1, N_DEV):
        pl.semaphore_signal(barrier, inc=1, device_id={"ep": lax.rem(me + d, N_DEV)}, device_id_type=MESH)
    loads = []
    for e in range(EARLY):
        loads.append(pltpu.make_async_copy(wg.at[e], w_out.at[e, 0], w_sem.at[e, 0]))
        loads.append(pltpu.make_async_copy(wu.at[e], w_out.at[e, 1], w_sem.at[e, 1]))
    for load in loads:
        load.start()

    pad[...] = jnp.zeros_like(pad)
    own_route.wait()
    pad[0, 0:6, 0:n_tok] = pad_i[...].astype(F32)
    own_gate.wait()
    pad[1, 0:6, 0:n_tok] = pad_g[...]
    routes = pad[0] + pltpu.roll(pad[0], n_tok, 1)
    gates = pad[1] + pltpu.roll(pad[1], n_tok, 1)
    expert = lax.broadcasted_iota(jnp.int32, (64, 128), 0).astype(F32)
    lane = lax.broadcasted_iota(jnp.int32, (64, 128), 1)
    mine = (lane // n_tok) == core
    member = jnp.zeros((64, 128), F32)
    weight = jnp.zeros((64, 128), F32)
    for k in range(6):
        hit = (expert == routes[k : k + 1, :]) & mine
        member = jnp.where(hit, 1.0, member)
        weight = jnp.where(hit, gates[k : k + 1, :], weight)
    row = lax.broadcasted_iota(jnp.int32, (128, 128), 0)
    col = lax.broadcasted_iota(jnp.int32, (128, 128), 1)
    upto = jnp.where((row <= col), 1.0, 0.0).astype(BF16)
    rank = jnp.dot(member.astype(BF16), upto, preferred_element_type=F32)
    code = jnp.where(member > 0.5, rank + (me * CAP).astype(F32), 0.0)
    sg_loc[:, 0:8, :] = code.reshape(8, 8, 128)
    sg_loc[:, 8:16, :] = weight.reshape(8, 8, 128)
    sg[me] = sg_loc[me]
    pl.semaphore_wait(barrier, N_DEV - 1)

    sg_copies = []
    for d in range(1, N_DEV):
        peer = lax.rem(me + d, N_DEV)
        sg_copies.append(remote(sg_loc.at[peer], sg.at[me], sg_s.at[d], sg_r.at[d], peer))
    for copy in sg_copies:
        copy.start()
    to_x_a = remote(rows(me, 0), rows(me, 0), link_s.at[0], link_r.at[0], xn)
    to_x_b = remote(rows(me, 1), rows(me, 1), link_s.at[1], link_r.at[1], xn)
    to_y_b = remote(rows(me, 1), rows(me, 1), link_s.at[2], link_r.at[2], yn)
    to_y_a = remote(rows(me, 0), rows(me, 0), link_s.at[3], link_r.at[3], yn)
    to_sib = remote(rows(me, 0, n_tok), rows(me, 0, n_tok), sib_s.at[0], sib_r.at[0], sib)
    own.wait()
    for copy in (to_x_a, to_y_b, to_x_b, to_y_a, to_sib):
        copy.start()
    dg = lax.rem(xn + 4, N_DEV)
    passed = []

    def pass_on(index, source, part):
        copy = remote(rows(source, part), rows(source, part), sib_s.at[index], sib_r.at[index], sib)
        copy.start()
        passed.append(copy)

    to_x_a.wait_recv()
    via_y = remote(rows(xn, 0), rows(xn, 0), link_s.at[4], link_r.at[4], yn)
    via_y.start()
    pass_on(1, xn, 0)
    to_y_b.wait_recv()
    via_x = remote(rows(yn, 1), rows(yn, 1), link_s.at[5], link_r.at[5], xn)
    via_x.start()
    pass_on(2, yn, 1)
    for copy in sg_copies:
        copy.wait()

    r = lax.broadcasted_iota(jnp.int32, (256, 128), 0)
    lane = lax.broadcasted_iota(jnp.int32, (256, 128), 1)
    for p in range(4):
        target = ((2 * p + lane // 64) * CAP + lax.rem(r, CAP) + 1).astype(F32)
        code = sg[2 * p, 0:8, :] + sg[2 * p + 1, 0:8, :]
        gate = sg[2 * p, 8:16, :] + sg[2 * p + 1, 8:16, :]
        codes_out[:, pl.ds(p * 128, 128)] = code
        code = jnp.broadcast_to(code[:, None, :], (8, CAP, 128)).reshape(256, 128)
        gate = jnp.broadcast_to(gate[:, None, :], (8, CAP, 128)).reshape(256, 128)
        s_t = jnp.where(code == target, gate, 0.0)
        s_f = s_t.T
        hi = jnp.minimum(s_f, 3.3895e38).astype(BF16)
        rest = s_f - hi.astype(F32)
        mid = rest.astype(BF16)
        low = (rest - mid.astype(F32)).astype(BF16)
        s_out[p, 0] = hi
        s_out[p, 1] = mid
        s_out[p, 2] = low

    to_x_b.wait_recv()
    pass_on(3, xn, 1)
    to_y_a.wait_recv()
    pass_on(4, yn, 0)
    via_y.wait_recv()
    pass_on(5, dg, 0)
    via_x.wait_recv()
    pass_on(6, dg, 1)
    for copy in (to_x_a, to_x_b, to_y_b, to_y_a, via_y, via_x):
        copy.wait_send()
    to_sib.wait()
    for copy in passed:
        copy.wait()
    for load in loads:
        load.wait()


def hidden_kernel(w_in, h_in, wd_in, x_all, codes, wg, wu, wd, w_buf, h_out, wd_out, xe, w_sem, d_sem):
    n_exp = wg.shape[0]
    d_ff = wg.shape[2]

    def load(e, part, src):
        s = lax.rem(e, SLOTS)
        return pltpu.make_async_copy(src.at[e], w_buf.at[s, part], w_sem.at[s, part])

    for e in range(EARLY, SLOTS):
        load(e, 0, wg).start()
        load(e, 1, wu).start()
    down = pltpu.make_async_copy(wd.at[:, :, pl.ds(0, COLS)], wd_out, d_sem)

    def hidden_rows(e, cap, slot):
        m = cap * N_DEV
        r = lax.broadcasted_iota(jnp.int32, (m, 512), 0)
        target = ((r // cap) * CAP + lax.rem(r, cap) + 1).astype(F32)
        pick = (target == codes[pl.ds(e, 1), :]).astype(BF16)
        for c in range(0, x_all.shape[1], 512):
            part = jnp.dot(pick, x_all[:, pl.ds(c, 512)], preferred_element_type=F32)
            xe[pl.ds(0, m), pl.ds(c, 512)] = part.astype(BF16)

        def put(act, c, w):
            if cap == CAP:
                h_out[e, :, pl.ds(c, w)] = act
            else:
                for i in range(N_DEV):
                    h_out[e, pl.ds(i * CAP, cap), pl.ds(c, w)] = act[i * cap : (i + 1) * cap]
                    h_out[e, pl.ds(i * CAP + cap, CAP - cap), pl.ds(c, w)] = jnp.zeros((CAP - cap, w), BF16)

        def act_of(a, b):
            return (a * jax.nn.sigmoid(a) * b).astype(BF16)

        rows = xe[pl.ds(0, m), :]
        for c in range(0, d_ff - 128, 256):
            a = jnp.dot(rows, w_buf[slot, 0, :, pl.ds(c, 256)], preferred_element_type=F32)
            b = jnp.dot(rows, w_buf[slot, 1, :, pl.ds(c, 256)], preferred_element_type=F32)
            put(act_of(a, b), c, 256)
        c = d_ff - 128
        both = jnp.concatenate([w_buf[slot, 0, :, pl.ds(c, 128)], w_buf[slot, 1, :, pl.ds(c, 128)]], axis=1)
        ab = jnp.dot(rows, both, preferred_element_type=F32)
        put(act_of(ab[:, :128], ab[:, 128:]), c, 128)

    def step(e, carry):
        slot = lax.rem(e, SLOTS)

        @pl.when(e >= EARLY)
        def _():
            load(e, 0, wg).wait()
            load(e, 1, wu).wait()

        code_row = codes[pl.ds(e, 1), :]
        block = lax.broadcasted_iota(jnp.int32, (1, 512), 1) // 64
        most = jnp.max(code_row - (block * CAP).astype(F32))
        small = most <= 16.0

        @pl.when(small)
        def _():
            hidden_rows(e, CAP // 2, slot)

        @pl.when(jnp.logical_not(small))
        def _():
            hidden_rows(e, CAP, slot)

        @pl.when(e + SLOTS < n_exp)
        def _():
            load(e + SLOTS, 0, wg).start()
            load(e + SLOTS, 1, wu).start()

        @pl.when(e + SLOTS == n_exp)
        def _():
            down.start()

        return carry

    lax.fori_loop(0, n_exp, step, 0)
    down.wait()


def combine_kernel(h, s, wd_on, wd, y_out, wd_buf, o, part, d2d, h1a, h1b, h2a, h2b, w_sem, ds, dr, h1as, h1ar, h1bs, h1br, h2as, h2ar, h2bs, h2br):
    me, core, x, y, sib, xn, yn = place()
    n_blk = wd.shape[2] // COLS
    n_buf = wd_buf.shape[0]
    n_exp = h.shape[0]
    half = 32
    first, second = pl.ds(0, half), pl.ds(half, half)

    def load(b):
        slot = lax.rem(b - 1, n_buf)
        return pltpu.make_async_copy(wd.at[:, :, pl.ds(pl.multiple_of(b * COLS, COLS), COLS)], wd_buf.at[slot], w_sem.at[slot])

    for b in range(1, n_buf + 1):
        load(b).start()
    entry_barrier(me)

    def send_d2d(b):
        return remote(part.at[b, 1 - core], d2d.at[b], ds.at[b], dr.at[b], sib)

    def send_1a(b):
        return remote(part.at[b, core, :, 1 - x, first], h1a.at[b], h1as.at[b], h1ar.at[b], xn)

    def send_1b(b):
        return remote(part.at[b, core, 1 - y, :, second], h1b.at[b], h1bs.at[b], h1br.at[b], yn)

    def send_2a(b):
        return remote(part.at[b, core, 1 - y, x, first], h2a.at[b], h2as.at[b], h2ar.at[b], yn)

    def send_2b(b):
        return remote(part.at[b, core, y, 1 - x, second], h2b.at[b], h2bs.at[b], h2br.at[b], xn)

    def lag(b, k, body):
        @pl.when((b >= k) & (b < n_blk + k))
        def _():
            body(b - k)

    def stage_1(b):
        send_d2d(b).start()

    def stage_2(b):
        send_d2d(b).wait_recv()
        part[b, core] += d2d[b]
        send_1a(b).start()
        send_1b(b).start()

    def stage_3(b):
        send_1a(b).wait_recv()
        send_1b(b).wait_recv()
        part[b, core, :, x, first] += h1a[b]
        part[b, core, y, :, second] += h1b[b]
        send_2a(b).start()
        send_2b(b).start()

    def stage_4(b):
        send_2a(b).wait_recv()
        send_2b(b).wait_recv()
        cols = pl.ds(pl.multiple_of(b * COLS, COLS), COLS)
        y_out[first, cols] = (part[b, core, y, x, first] + h2a[b]).astype(BF16)
        y_out[second, cols] = (part[b, core, y, x, second] + h2b[b]).astype(BF16)

    def down(e, weights):
        out = jnp.dot(h[e], weights[e], preferred_element_type=F32).astype(BF16)
        for i in range(N_DEV):
            o[i, pl.ds(e * CAP, CAP), :] = out[i * CAP : (i + 1) * CAP]

    def on_weights(b, body):
        @pl.when(b == 0)
        def _():
            body(wd_on)

        @pl.when((b >= 1) & (b < n_blk))
        def _():
            body(wd_buf.at[lax.rem(b - 1, n_buf)])

    def step(b, carry):
        lag(b, 1, stage_1)

        @pl.when((b >= 1) & (b < n_blk))
        def _():
            load(b).wait()

        def front(weights):
            for e in range(FRONT):
                down(e, weights)

        on_weights(b, front)
        lag(b, 1, stage_2)
        lag(b, 3, stage_3)
        lag(b, 5, stage_4)

        def back(weights):
            for e in range(FRONT, n_exp):
                down(e, weights)
            for i in range(N_DEV):
                gates = s[i // 2, :, pl.ds((i % 2) * 64, 64), :].reshape(192, 256)
                terms = jnp.dot(gates, o[i], preferred_element_type=F32)
                part[b, i % 2, i // 4, (i // 2) % 2] = terms[0:64] + terms[64:128] + terms[128:192]

        on_weights(b, back)

        @pl.when((b >= 1) & (b + n_buf < n_blk))
        def _():
            load(b + n_buf).start()

        return carry

    lax.fori_loop(0, n_blk + 5, step, 0)

    def drain(b, carry):
        for send in (send_d2d, send_1a, send_1b, send_2a, send_2b):
            send(b).wait_send()
        return carry

    lax.fori_loop(0, n_blk, drain, 0)


def solution(mesh):
    row_spec = P(("dp", "ep"))
    expert_spec = P("ep")
    dma = pltpu.SemaphoreType.DMA

    def local_step(tok, route, gate, wg, wu, wd):
        n_exp, d_model, d_ff = wg.shape
        n_tok = tok.shape[0]
        n_blk = d_model // COLS
        hidden = (n_exp, N_DEV * CAP, d_ff)
        w_on, x_all, codes, h, s, wd_on = pl.pallas_call(
            gather_kernel,
            out_shape=[on_chip((SLOTS, 2, d_model, d_ff), BF16), on_chip((N_DEV * n_tok, d_model), BF16), on_chip((8, 512), F32), on_chip(hidden, BF16), on_chip((4, 3, 128, 256), BF16), on_chip((n_exp, d_ff, COLS), BF16)],
            in_specs=[ANY] * 5,
            out_specs=[VMEM] * 6,
            scratch_shapes=[
                pltpu.VMEM((6, n_tok), jnp.int32),
                pltpu.VMEM((6, n_tok), F32),
                pltpu.VMEM((2, 8, 128), F32),
                pltpu.VMEM((N_DEV, 16, 128), F32),
                pltpu.VMEM((N_DEV, 16, 128), F32),
                dma((EARLY, 2)),
                dma((3,)),
                dma((7,)),
                dma((7,)),
                dma((6,)),
                dma((6,)),
                dma((N_DEV,)),
                dma((N_DEV,)),
            ],
            compiler_params=pltpu.CompilerParams(collective_id=0, has_side_effects=True, vmem_limit_bytes=LIMIT),
            name="gather",
        )(tok, route.T, gate.T, wg, wu)
        unused, h, wd_on = pl.pallas_call(
            hidden_kernel,
            out_shape=[on_chip(w_on.shape, BF16), on_chip(hidden, BF16), on_chip(wd_on.shape, BF16)],
            in_specs=[VMEM] * 5 + [ANY] * 3,
            out_specs=[VMEM] * 3,
            scratch_shapes=[pltpu.VMEM((256, d_model), BF16), dma((SLOTS, 2)), dma],
            input_output_aliases={0: 0, 1: 1, 2: 2},
            compiler_params=pltpu.CompilerParams(vmem_limit_bytes=LIMIT),
            name="hidden",
        )(pin(w_on), pin(h), pin(wd_on), pin(x_all), pin(codes), wg, wu, wd)
        return pl.pallas_call(
            combine_kernel,
            out_shape=jax.ShapeDtypeStruct((n_tok, d_model), BF16),
            in_specs=[VMEM] * 3 + [ANY],
            out_specs=VMEM,
            scratch_shapes=[
                pltpu.VMEM((3, n_exp, d_ff, COLS), BF16),
                pltpu.VMEM((N_DEV, 256, COLS), BF16),
                pltpu.VMEM((n_blk, 2, 2, 2, n_tok, COLS), F32),
                pltpu.VMEM((n_blk, 2, 2, n_tok, COLS), F32),
                pltpu.VMEM((n_blk, 2, n_tok // 2, COLS), F32),
                pltpu.VMEM((n_blk, 2, n_tok // 2, COLS), F32),
                pltpu.VMEM((n_blk, n_tok // 2, COLS), F32),
                pltpu.VMEM((n_blk, n_tok // 2, COLS), F32),
                dma((3,)),
            ]
            + [dma((n_blk,))] * 10,
            compiler_params=pltpu.CompilerParams(collective_id=1, has_side_effects=True, vmem_limit_bytes=32 << 20),
            name="combine",
        )(pin(h), pin(s), pin(wd_on), wd)

    return jax.shard_map(local_step, mesh=mesh, in_specs=(row_spec, row_spec, row_spec, expert_spec, expert_spec, expert_spec), out_specs=row_spec, check_vma=False)
```

```python
import jax
import jax.numpy as jnp
from jax import lax
from jax.experimental import pallas as pl
from jax.experimental.pallas import tpu as pltpu
from jax.sharding import PartitionSpec as P

BF16 = jnp.bfloat16
F32 = jnp.float32
MESH = pl.DeviceIdType.MESH
N_DEV = 8
CAP = 32
SLOTS = 4
EARLY = 3
FRONT = 6
LAG_3 = 3
LAG_4 = 6
LIMIT = 4 << 20
COLS = 256
VMEM = pl.BlockSpec(memory_space=pltpu.VMEM)
ANY = pl.BlockSpec(memory_space=pl.ANY)


def remote(src, dst, send_sem, recv_sem, peer):
    return pltpu.make_async_remote_copy(src_ref=src, dst_ref=dst, send_sem=send_sem, recv_sem=recv_sem, device_id={"ep": peer}, device_id_type=MESH)


def on_chip(shape, dtype):
    return pltpu.VMEM(shape, dtype)


def pin(v):
    return pltpu.with_memory_space_constraint(v, pltpu.VMEM)


def place():
    me = lax.axis_index("ep")
    core = lax.rem(me, 2)
    x = lax.rem(me // 2, 2)
    y = me // 4
    return me, core, x, y, me + 1 - 2 * core, me + 2 - 4 * x, me + 4 - 8 * y


def entry_barrier(me):
    barrier = pltpu.get_barrier_semaphore()
    for d in range(1, N_DEV):
        pl.semaphore_signal(barrier, inc=1, device_id={"ep": lax.rem(me + d, N_DEV)}, device_id_type=MESH)
    pl.semaphore_wait(barrier, N_DEV - 1)


def gather_kernel(tok, route_t, gate_t, wg, wu, w_out, x_out, codes_out, h_out, s_out, wd_out, pad_i, pad_g, pad, sg_loc, sg, w_sem, in_sem, sib_s, sib_r, link_s, link_r, sg_s, sg_r):
    me, core, x, y, sib, xn, yn = place()
    n_tok = tok.shape[0]
    half = n_tok // 2

    def rows(device, part=0, count=half):
        return x_out.at[pl.ds(pl.multiple_of(device * n_tok + part * half, half), count)]

    own = pltpu.make_async_copy(tok, rows(me, 0, n_tok), in_sem.at[0])
    own_route = pltpu.make_async_copy(route_t, pad_i, in_sem.at[1])
    own_gate = pltpu.make_async_copy(gate_t, pad_g, in_sem.at[2])
    own.start()
    own_route.start()
    own_gate.start()
    barrier = pltpu.get_barrier_semaphore()
    for d in range(1, N_DEV):
        pl.semaphore_signal(barrier, inc=1, device_id={"ep": lax.rem(me + d, N_DEV)}, device_id_type=MESH)
    loads = []
    for e in range(EARLY):
        loads.append(pltpu.make_async_copy(wg.at[e], w_out.at[e, 0], w_sem.at[e, 0]))
        loads.append(pltpu.make_async_copy(wu.at[e], w_out.at[e, 1], w_sem.at[e, 1]))
    for load in loads:
        load.start()

    pad[...] = jnp.zeros_like(pad)
    own_route.wait()
    pad[0, 0:6, 0:n_tok] = pad_i[...].astype(F32)
    own_gate.wait()
    pad[1, 0:6, 0:n_tok] = pad_g[...]
    routes = pad[0] + pltpu.roll(pad[0], n_tok, 1)
    gates = pad[1] + pltpu.roll(pad[1], n_tok, 1)
    expert = lax.broadcasted_iota(jnp.int32, (64, 128), 0).astype(F32)
    lane = lax.broadcasted_iota(jnp.int32, (64, 128), 1)
    mine = (lane // n_tok) == core
    member = jnp.zeros((64, 128), F32)
    weight = jnp.zeros((64, 128), F32)
    for k in range(6):
        hit = (expert == routes[k : k + 1, :]) & mine
        member = jnp.where(hit, 1.0, member)
        weight = jnp.where(hit, gates[k : k + 1, :], weight)
    row = lax.broadcasted_iota(jnp.int32, (128, 128), 0)
    col = lax.broadcasted_iota(jnp.int32, (128, 128), 1)
    upto = jnp.where((row <= col), 1.0, 0.0).astype(BF16)
    rank = jnp.dot(member.astype(BF16), upto, preferred_element_type=F32)
    code = jnp.where(member > 0.5, rank + (me * CAP).astype(F32), 0.0)
    sg_loc[:, 0:8, :] = code.reshape(8, 8, 128)
    sg_loc[:, 8:16, :] = weight.reshape(8, 8, 128)
    sg[me] = sg_loc[me]
    pl.semaphore_wait(barrier, N_DEV - 1)

    sg_copies = []
    for d in range(1, N_DEV):
        peer = lax.rem(me + d, N_DEV)
        sg_copies.append(remote(sg_loc.at[peer], sg.at[me], sg_s.at[d], sg_r.at[d], peer))
    for copy in sg_copies:
        copy.start()
    to_x_a = remote(rows(me, 0), rows(me, 0), link_s.at[0], link_r.at[0], xn)
    to_x_b = remote(rows(me, 1), rows(me, 1), link_s.at[1], link_r.at[1], xn)
    to_y_b = remote(rows(me, 1), rows(me, 1), link_s.at[2], link_r.at[2], yn)
    to_y_a = remote(rows(me, 0), rows(me, 0), link_s.at[3], link_r.at[3], yn)
    to_sib = remote(rows(me, 0, n_tok), rows(me, 0, n_tok), sib_s.at[0], sib_r.at[0], sib)
    own.wait()
    for copy in (to_x_a, to_y_b, to_x_b, to_y_a, to_sib):
        copy.start()
    dg = lax.rem(xn + 4, N_DEV)
    passed = []

    def pass_on(index, source, part):
        copy = remote(rows(source, part), rows(source, part), sib_s.at[index], sib_r.at[index], sib)
        copy.start()
        passed.append(copy)

    to_x_a.wait_recv()
    via_y = remote(rows(xn, 0), rows(xn, 0), link_s.at[4], link_r.at[4], yn)
    via_y.start()
    pass_on(1, xn, 0)
    to_y_b.wait_recv()
    via_x = remote(rows(yn, 1), rows(yn, 1), link_s.at[5], link_r.at[5], xn)
    via_x.start()
    pass_on(2, yn, 1)
    for copy in sg_copies:
        copy.wait()

    r = lax.broadcasted_iota(jnp.int32, (256, 128), 0)
    lane = lax.broadcasted_iota(jnp.int32, (256, 128), 1)
    for p in range(4):
        target = ((2 * p + lane // 64) * CAP + lax.rem(r, CAP) + 1).astype(F32)
        code = sg[2 * p, 0:8, :] + sg[2 * p + 1, 0:8, :]
        gate = sg[2 * p, 8:16, :] + sg[2 * p + 1, 8:16, :]
        codes_out[:, pl.ds(p * 128, 128)] = code
        code = jnp.broadcast_to(code[:, None, :], (8, CAP, 128)).reshape(256, 128)
        gate = jnp.broadcast_to(gate[:, None, :], (8, CAP, 128)).reshape(256, 128)
        s_t = jnp.where(code == target, gate, 0.0)
        s_f = s_t.T
        hi = jnp.minimum(s_f, 3.3895e38).astype(BF16)
        rest = s_f - hi.astype(F32)
        mid = rest.astype(BF16)
        low = (rest - mid.astype(F32)).astype(BF16)
        s_out[p, 0] = hi
        s_out[p, 1] = mid
        s_out[p, 2] = low

    to_x_b.wait_recv()
    pass_on(3, xn, 1)
    to_y_a.wait_recv()
    pass_on(4, yn, 0)
    via_y.wait_recv()
    pass_on(5, dg, 0)
    via_x.wait_recv()
    pass_on(6, dg, 1)
    for copy in (to_x_a, to_x_b, to_y_b, to_y_a, via_y, via_x):
        copy.wait_send()
    to_sib.wait()
    for copy in passed:
        copy.wait()
    for load in loads:
        load.wait()


def hidden_kernel(w_in, h_in, wd_in, x_all, codes, wg, wu, wd, w_buf, h_out, wd_out, xe, w_sem, d_sem):
    n_exp = wg.shape[0]
    d_ff = wg.shape[2]

    def load(e, part, src):
        s = lax.rem(e, SLOTS)
        return pltpu.make_async_copy(src.at[e], w_buf.at[s, part], w_sem.at[s, part])

    for e in range(EARLY, SLOTS):
        load(e, 0, wg).start()
        load(e, 1, wu).start()
    down = pltpu.make_async_copy(wd.at[:, :, pl.ds(0, COLS)], wd_out, d_sem)

    def hidden_rows(e, cap, slot):
        m = cap * N_DEV
        r = lax.broadcasted_iota(jnp.int32, (m, 512), 0)
        target = ((r // cap) * CAP + lax.rem(r, cap) + 1).astype(F32)
        pick = (target == codes[pl.ds(e, 1), :]).astype(BF16)
        for c in range(0, x_all.shape[1], 512):
            part = jnp.dot(pick, x_all[:, pl.ds(c, 512)], preferred_element_type=F32)
            xe[pl.ds(0, m), pl.ds(c, 512)] = part.astype(BF16)

        def put(act, c, w):
            if cap == CAP:
                h_out[e, :, pl.ds(c, w)] = act
            else:
                for i in range(N_DEV):
                    h_out[e, pl.ds(i * CAP, cap), pl.ds(c, w)] = act[i * cap : (i + 1) * cap]
                    h_out[e, pl.ds(i * CAP + cap, CAP - cap), pl.ds(c, w)] = jnp.zeros((CAP - cap, w), BF16)

        def act_of(a, b):
            return (a * jax.nn.sigmoid(a) * b).astype(BF16)

        rows = xe[pl.ds(0, m), :]
        for c in range(0, d_ff - 128, 256):
            a = jnp.dot(rows, w_buf[slot, 0, :, pl.ds(c, 256)], preferred_element_type=F32)
            b = jnp.dot(rows, w_buf[slot, 1, :, pl.ds(c, 256)], preferred_element_type=F32)
            put(act_of(a, b), c, 256)
        c = d_ff - 128
        both = jnp.concatenate([w_buf[slot, 0, :, pl.ds(c, 128)], w_buf[slot, 1, :, pl.ds(c, 128)]], axis=1)
        ab = jnp.dot(rows, both, preferred_element_type=F32)
        put(act_of(ab[:, :128], ab[:, 128:]), c, 128)

    def step(e, carry):
        slot = lax.rem(e, SLOTS)

        @pl.when(e >= EARLY)
        def _():
            load(e, 0, wg).wait()
            load(e, 1, wu).wait()

        code_row = codes[pl.ds(e, 1), :]
        block = lax.broadcasted_iota(jnp.int32, (1, 512), 1) // 64
        most = jnp.max(code_row - (block * CAP).astype(F32))
        small = most <= 16.0

        @pl.when(small)
        def _():
            hidden_rows(e, CAP // 2, slot)

        @pl.when(jnp.logical_not(small))
        def _():
            hidden_rows(e, CAP, slot)

        @pl.when(e + SLOTS < n_exp)
        def _():
            load(e + SLOTS, 0, wg).start()
            load(e + SLOTS, 1, wu).start()

        @pl.when(e + SLOTS == n_exp)
        def _():
            down.start()

        return carry

    lax.fori_loop(0, n_exp, step, 0)
    down.wait()


def combine_kernel(h, s, wd_on, wd, y_out, wd_buf, o, part, d2d, h1a, h1b, h2a, h2b, w_sem, ds, dr, h1as, h1ar, h1bs, h1br, h2as, h2ar, h2bs, h2br):
    me, core, x, y, sib, xn, yn = place()
    n_blk = wd.shape[2] // COLS
    n_buf = wd_buf.shape[0]
    n_exp = h.shape[0]
    half = 32
    first, second = pl.ds(0, half), pl.ds(half, half)

    def load(b):
        slot = lax.rem(b - 1, n_buf)
        return pltpu.make_async_copy(wd.at[:, :, pl.ds(pl.multiple_of(b * COLS, COLS), COLS)], wd_buf.at[slot], w_sem.at[slot])

    load(1).start()
    barrier = pltpu.get_barrier_semaphore()
    for d in range(1, N_DEV):
        pl.semaphore_signal(barrier, inc=1, device_id={"ep": lax.rem(me + d, N_DEV)}, device_id_type=MESH)

    def send_d2d(b):
        return remote(part.at[b, 1 - core], d2d.at[b], ds.at[b], dr.at[b], sib)

    def send_1a(b):
        return remote(part.at[b, core, :, 1 - x, first], h1a.at[b], h1as.at[b], h1ar.at[b], xn)

    def send_1b(b):
        return remote(part.at[b, core, 1 - y, :, second], h1b.at[b], h1bs.at[b], h1br.at[b], yn)

    def send_2a(b):
        return remote(part.at[b, core, 1 - y, x, first], h2a.at[b], h2as.at[b], h2ar.at[b], yn)

    def send_2b(b):
        return remote(part.at[b, core, y, 1 - x, second], h2b.at[b], h2bs.at[b], h2br.at[b], xn)

    def lag(b, k, body):
        @pl.when((b >= k) & (b < n_blk + k))
        def _():
            body(b - k)

    def stage_1(b):
        send_d2d(b).start()

    def stage_2(b):
        send_d2d(b).wait_recv()
        part[b, core] += d2d[b]
        send_1a(b).start()
        send_1b(b).start()

    def stage_3(b):
        send_1a(b).wait_recv()
        send_1b(b).wait_recv()
        part[b, core, :, x, first] += h1a[b]
        part[b, core, y, :, second] += h1b[b]
        send_2a(b).start()
        send_2b(b).start()

    def stage_4(b):
        send_2a(b).wait_recv()
        send_2b(b).wait_recv()
        cols = pl.ds(pl.multiple_of(b * COLS, COLS), COLS)
        y_out[first, cols] = (part[b, core, y, x, first] + h2a[b]).astype(BF16)
        y_out[second, cols] = (part[b, core, y, x, second] + h2b[b]).astype(BF16)

    def down(e, weights):
        out = jnp.dot(h[e], weights[e], preferred_element_type=F32).astype(BF16)
        for i in range(N_DEV):
            o[i, pl.ds(e * CAP, CAP), :] = out[i * CAP : (i + 1) * CAP]

    def front(b, weights):
        for e in range(FRONT):
            down(e, weights)

        @pl.when(b + 2 < n_blk)
        def _():
            load(b + 2).start()

    def back(b, weights):
        for e in range(FRONT, n_exp):
            down(e, weights)
        for i in range(N_DEV):
            gates = s[i // 2, :, pl.ds((i % 2) * 64, 64), :].reshape(192, 256)
            terms = jnp.dot(gates, o[i], preferred_element_type=F32)
            part[b, i % 2, i // 4, (i // 2) % 2] = terms[0:64] + terms[64:128] + terms[128:192]

    front(0, wd_on)
    back(0, wd_on)
    pl.semaphore_wait(barrier, N_DEV - 1)

    def step(b, carry):
        lag(b, 1, stage_1)
        weights = wd_buf.at[lax.rem(b - 1, n_buf)]

        @pl.when(b < n_blk)
        def _():
            load(b).wait()
            front(b, weights)

        lag(b, 1, stage_2)
        lag(b, LAG_3, stage_3)
        lag(b, LAG_4, stage_4)

        @pl.when(b < n_blk)
        def _():
            back(b, weights)

        return carry

    lax.fori_loop(1, n_blk + LAG_4, step, 0)

    def drain(b, carry):
        for send in (send_d2d, send_1a, send_1b, send_2a, send_2b):
            send(b).wait_send()
        return carry

    lax.fori_loop(0, n_blk, drain, 0)


def solution(mesh):
    row_spec = P(("dp", "ep"))
    expert_spec = P("ep")
    dma = pltpu.SemaphoreType.DMA

    def local_step(tok, route, gate, wg, wu, wd):
        n_exp, d_model, d_ff = wg.shape
        n_tok = tok.shape[0]
        n_blk = d_model // COLS
        hidden = (n_exp, N_DEV * CAP, d_ff)
        w_on, x_all, codes, h, s, wd_on = pl.pallas_call(
            gather_kernel,
            out_shape=[on_chip((SLOTS, 2, d_model, d_ff), BF16), on_chip((N_DEV * n_tok, d_model), BF16), on_chip((8, 512), F32), on_chip(hidden, BF16), on_chip((4, 3, 128, 256), BF16), on_chip((n_exp, d_ff, COLS), BF16)],
            in_specs=[ANY] * 5,
            out_specs=[VMEM] * 6,
            scratch_shapes=[
                pltpu.VMEM((6, n_tok), jnp.int32),
                pltpu.VMEM((6, n_tok), F32),
                pltpu.VMEM((2, 8, 128), F32),
                pltpu.VMEM((N_DEV, 16, 128), F32),
                pltpu.VMEM((N_DEV, 16, 128), F32),
                dma((EARLY, 2)),
                dma((3,)),
                dma((7,)),
                dma((7,)),
                dma((6,)),
                dma((6,)),
                dma((N_DEV,)),
                dma((N_DEV,)),
            ],
            compiler_params=pltpu.CompilerParams(collective_id=0, has_side_effects=True, vmem_limit_bytes=LIMIT),
            name="gather",
        )(tok, route.T, gate.T, wg, wu)
        unused, h, wd_on = pl.pallas_call(
            hidden_kernel,
            out_shape=[on_chip(w_on.shape, BF16), on_chip(hidden, BF16), on_chip(wd_on.shape, BF16)],
            in_specs=[VMEM] * 5 + [ANY] * 3,
            out_specs=[VMEM] * 3,
            scratch_shapes=[pltpu.VMEM((256, d_model), BF16), dma((SLOTS, 2)), dma],
            input_output_aliases={0: 0, 1: 1, 2: 2},
            compiler_params=pltpu.CompilerParams(vmem_limit_bytes=LIMIT),
            name="hidden",
        )(pin(w_on), pin(h), pin(wd_on), pin(x_all), pin(codes), wg, wu, wd)
        return pl.pallas_call(
            combine_kernel,
            out_shape=jax.ShapeDtypeStruct((n_tok, d_model), BF16),
            in_specs=[VMEM] * 3 + [ANY],
            out_specs=VMEM,
            scratch_shapes=[
                pltpu.VMEM((3, n_exp, d_ff, COLS), BF16),
                pltpu.VMEM((N_DEV, 256, COLS), BF16),
                pltpu.VMEM((n_blk, 2, 2, 2, n_tok, COLS), F32),
                pltpu.VMEM((n_blk, 2, 2, n_tok, COLS), F32),
                pltpu.VMEM((n_blk, 2, n_tok // 2, COLS), F32),
                pltpu.VMEM((n_blk, 2, n_tok // 2, COLS), F32),
                pltpu.VMEM((n_blk, n_tok // 2, COLS), F32),
                pltpu.VMEM((n_blk, n_tok // 2, COLS), F32),
                dma((3,)),
            ]
            + [dma((n_blk,))] * 10,
            compiler_params=pltpu.CompilerParams(collective_id=1, has_side_effects=True, vmem_limit_bytes=32 << 20),
            name="combine",
        )(pin(h), pin(s), pin(wd_on), wd)

    return jax.shard_map(local_step, mesh=mesh, in_specs=(row_spec, row_spec, row_spec, expert_spec, expert_spec, expert_spec), out_specs=row_spec, check_vma=False)
```

```python
import jax
import jax.numpy as jnp
from jax import lax
from jax.experimental import pallas as pl
from jax.experimental.pallas import tpu as pltpu
from jax.sharding import PartitionSpec as P

BF16 = jnp.bfloat16
F32 = jnp.float32
MESH = pl.DeviceIdType.MESH
N_DEV = 8
CAP = 32
SLOTS = 4
WAITS = (0, 3)
FRONT = 6
LAG_3 = 3
LAG_4 = 6
LIMIT = 4 << 20
COLS = 256
VMEM = pl.BlockSpec(memory_space=pltpu.VMEM)
ANY = pl.BlockSpec(memory_space=pl.ANY)


def remote(src, dst, send_sem, recv_sem, peer):
    return pltpu.make_async_remote_copy(src_ref=src, dst_ref=dst, send_sem=send_sem, recv_sem=recv_sem, device_id={"ep": peer}, device_id_type=MESH)


def on_chip(shape, dtype):
    return pltpu.VMEM(shape, dtype)


def pin(v):
    return pltpu.with_memory_space_constraint(v, pltpu.VMEM)


def place():
    me = lax.axis_index("ep")
    core = lax.rem(me, 2)
    x = lax.rem(me // 2, 2)
    y = me // 4
    return me, core, x, y, me + 1 - 2 * core, me + 2 - 4 * x, me + 4 - 8 * y


def entry_barrier(me):
    barrier = pltpu.get_barrier_semaphore()
    for d in range(1, N_DEV):
        pl.semaphore_signal(barrier, inc=1, device_id={"ep": lax.rem(me + d, N_DEV)}, device_id_type=MESH)
    pl.semaphore_wait(barrier, N_DEV - 1)


def gather_kernel(tok, route_t, gate_t, wg, wu, w_out, x_out, codes_out, h_out, s_out, wd_out, pad_i, pad_g, pad, sg_loc, sg, w_sem, in_sem, sib_s, sib_r, link_s, link_r, sg_s, sg_r):
    me, core, x, y, sib, xn, yn = place()
    n_tok = tok.shape[0]
    half = n_tok // 2

    def rows(device, part=0, count=half):
        return x_out.at[pl.ds(pl.multiple_of(device * n_tok + part * half, half), count)]

    own = pltpu.make_async_copy(tok, rows(me, 0, n_tok), in_sem.at[0])
    own_route = pltpu.make_async_copy(route_t, pad_i, in_sem.at[1])
    own_gate = pltpu.make_async_copy(gate_t, pad_g, in_sem.at[2])
    own.start()
    own_route.start()
    own_gate.start()
    barrier = pltpu.get_barrier_semaphore()
    for d in range(1, N_DEV):
        pl.semaphore_signal(barrier, inc=1, device_id={"ep": lax.rem(me + d, N_DEV)}, device_id_type=MESH)
    loads = []
    for e in range(SLOTS):
        loads.append(pltpu.make_async_copy(wg.at[e], w_out.at[e, 0], w_sem.at[e, 0]))
        loads.append(pltpu.make_async_copy(wu.at[e], w_out.at[e, 1], w_sem.at[e, 1]))
    for load in loads:
        load.start()

    pad[...] = jnp.zeros_like(pad)
    own_route.wait()
    pad[0, 0:6, 0:n_tok] = pad_i[...].astype(F32)
    own_gate.wait()
    pad[1, 0:6, 0:n_tok] = pad_g[...]
    routes = pad[0] + pltpu.roll(pad[0], n_tok, 1)
    gates = pad[1] + pltpu.roll(pad[1], n_tok, 1)
    expert = lax.broadcasted_iota(jnp.int32, (64, 128), 0).astype(F32)
    lane = lax.broadcasted_iota(jnp.int32, (64, 128), 1)
    mine = (lane // n_tok) == core
    member = jnp.zeros((64, 128), F32)
    weight = jnp.zeros((64, 128), F32)
    for k in range(6):
        hit = (expert == routes[k : k + 1, :]) & mine
        member = jnp.where(hit, 1.0, member)
        weight = jnp.where(hit, gates[k : k + 1, :], weight)
    row = lax.broadcasted_iota(jnp.int32, (128, 128), 0)
    col = lax.broadcasted_iota(jnp.int32, (128, 128), 1)
    upto = jnp.where((row <= col), 1.0, 0.0).astype(BF16)
    rank = jnp.dot(member.astype(BF16), upto, preferred_element_type=F32)
    code = jnp.where(member > 0.5, rank + (me * CAP).astype(F32), 0.0)
    sg_loc[:, 0:8, :] = code.reshape(8, 8, 128)
    sg_loc[:, 8:16, :] = weight.reshape(8, 8, 128)
    sg[me] = sg_loc[me]
    pl.semaphore_wait(barrier, N_DEV - 1)

    sg_copies = []
    for d in range(1, N_DEV):
        peer = lax.rem(me + d, N_DEV)
        sg_copies.append(remote(sg_loc.at[peer], sg.at[me], sg_s.at[d], sg_r.at[d], peer))
    for copy in sg_copies:
        copy.start()
    to_x_a = remote(rows(me, 0), rows(me, 0), link_s.at[0], link_r.at[0], xn)
    to_x_b = remote(rows(me, 1), rows(me, 1), link_s.at[1], link_r.at[1], xn)
    to_y_b = remote(rows(me, 1), rows(me, 1), link_s.at[2], link_r.at[2], yn)
    to_y_a = remote(rows(me, 0), rows(me, 0), link_s.at[3], link_r.at[3], yn)
    to_sib = remote(rows(me, 0, n_tok), rows(me, 0, n_tok), sib_s.at[0], sib_r.at[0], sib)
    own.wait()
    for copy in (to_x_a, to_y_b, to_x_b, to_y_a, to_sib):
        copy.start()
    dg = lax.rem(xn + 4, N_DEV)
    passed = []

    def pass_on(index, source, part):
        copy = remote(rows(source, part), rows(source, part), sib_s.at[index], sib_r.at[index], sib)
        copy.start()
        passed.append(copy)

    to_x_a.wait_recv()
    via_y = remote(rows(xn, 0), rows(xn, 0), link_s.at[4], link_r.at[4], yn)
    via_y.start()
    pass_on(1, xn, 0)
    to_y_b.wait_recv()
    via_x = remote(rows(yn, 1), rows(yn, 1), link_s.at[5], link_r.at[5], xn)
    via_x.start()
    pass_on(2, yn, 1)
    for copy in sg_copies:
        copy.wait()

    r = lax.broadcasted_iota(jnp.int32, (256, 128), 0)
    lane = lax.broadcasted_iota(jnp.int32, (256, 128), 1)
    for p in range(4):
        target = ((2 * p + lane // 64) * CAP + lax.rem(r, CAP) + 1).astype(F32)
        code = sg[2 * p, 0:8, :] + sg[2 * p + 1, 0:8, :]
        gate = sg[2 * p, 8:16, :] + sg[2 * p + 1, 8:16, :]
        codes_out[:, pl.ds(p * 128, 128)] = code
        code = jnp.broadcast_to(code[:, None, :], (8, CAP, 128)).reshape(256, 128)
        gate = jnp.broadcast_to(gate[:, None, :], (8, CAP, 128)).reshape(256, 128)
        s_t = jnp.where(code == target, gate, 0.0)
        s_f = s_t.T
        hi = jnp.minimum(s_f, 3.3895e38).astype(BF16)
        rest = s_f - hi.astype(F32)
        mid = rest.astype(BF16)
        low = (rest - mid.astype(F32)).astype(BF16)
        s_out[p, 0] = hi
        s_out[p, 1] = mid
        s_out[p, 2] = low

    to_x_b.wait_recv()
    pass_on(3, xn, 1)
    to_y_a.wait_recv()
    pass_on(4, yn, 0)
    via_y.wait_recv()
    pass_on(5, dg, 0)
    via_x.wait_recv()
    pass_on(6, dg, 1)
    for copy in (to_x_a, to_x_b, to_y_b, to_y_a, via_y, via_x):
        copy.wait_send()
    to_sib.wait()
    for copy in passed:
        copy.wait()
    for load in loads:
        load.wait()


def hidden_kernel(w_in, h_in, wd_in, x_all, codes, wg, wu, wd, w_buf, h_out, wd_out, xe, w_sem, d_sem):
    n_exp = wg.shape[0]
    d_ff = wg.shape[2]
    panels = [(c, min(256, d_ff - c)) for c in range(0, d_ff, 256)]
    down = pltpu.make_async_copy(wd.at[:, :, pl.ds(0, COLS)], wd_out, d_sem)

    def load(e, p):
        c, w = panels[p]
        slot = lax.rem(e, SLOTS)
        cols = pl.ds(c, w)
        return [pltpu.make_async_copy(src.at[e, :, cols], w_buf.at[slot, part, :, cols], w_sem.at[slot, part, p]) for part, src in ((0, wg), (1, wu))]

    def hidden_rows(e, cap, before, after):
        m = cap * N_DEV
        slot = lax.rem(e, SLOTS)
        r = lax.broadcasted_iota(jnp.int32, (m, 512), 0)
        target = ((r // cap) * CAP + lax.rem(r, cap) + 1).astype(F32)
        pick = (target == codes[pl.ds(e, 1), :]).astype(BF16)
        for c in range(0, x_all.shape[1], 512):
            part = jnp.dot(pick, x_all[:, pl.ds(c, 512)], preferred_element_type=F32)
            xe[pl.ds(0, m), pl.ds(c, 512)] = part.astype(BF16)

        def put(a, b, c, w):
            act = (a * jax.nn.sigmoid(a) * b).astype(BF16)
            if cap == CAP:
                h_out[e, :, pl.ds(c, w)] = act
            else:
                for i in range(N_DEV):
                    h_out[e, pl.ds(i * CAP, cap), pl.ds(c, w)] = act[i * cap : (i + 1) * cap]
                    h_out[e, pl.ds(i * CAP + cap, CAP - cap), pl.ds(c, w)] = jnp.zeros((CAP - cap, w), BF16)

        rows = xe[pl.ds(0, m), :]
        for p, (c, w) in enumerate(panels):
            before(e, p)
            if w == 256:
                a = jnp.dot(rows, w_buf[slot, 0, :, pl.ds(c, w)], preferred_element_type=F32)
                b = jnp.dot(rows, w_buf[slot, 1, :, pl.ds(c, w)], preferred_element_type=F32)
            else:
                both = jnp.concatenate([w_buf[slot, 0, :, pl.ds(c, w)], w_buf[slot, 1, :, pl.ds(c, w)]], axis=1)
                ab = jnp.dot(rows, both, preferred_element_type=F32)
                a, b = ab[:, :w], ab[:, w:]
            put(a, b, c, w)
            after(e, p)

    def expert(e, before, after):
        code_row = codes[pl.ds(e, 1), :]
        block = lax.broadcasted_iota(jnp.int32, (1, 512), 1) // 64
        small = jnp.max(code_row - (block * CAP).astype(F32)) <= 16.0

        @pl.when(small)
        def _():
            hidden_rows(e, CAP // 2, before, after)

        @pl.when(jnp.logical_not(small))
        def _():
            hidden_rows(e, CAP, before, after)

    def nothing(e, p):
        pass

    def refill(e, p):
        for copy in load(e + SLOTS, p):
            copy.start()

    def arrive(e, p):
        if p in WAITS:
            for q in range(p, min([v for v in WAITS if v > p] + [len(panels)])):
                for copy in load(e, q):
                    copy.wait()

    def early(e, carry):
        expert(e, nothing, refill)
        return carry

    def late(e, carry):
        expert(e, arrive, nothing)
        return carry

    lax.fori_loop(0, SLOTS, early, 0)
    down.start()
    lax.fori_loop(SLOTS, n_exp, late, 0)
    down.wait()


def combine_kernel(h, s, wd_on, wd, y_out, wd_buf, o, part, d2d, h1a, h1b, h2a, h2b, w_sem, ds, dr, h1as, h1ar, h1bs, h1br, h2as, h2ar, h2bs, h2br):
    me, core, x, y, sib, xn, yn = place()
    n_blk = wd.shape[2] // COLS
    n_buf = wd_buf.shape[0]
    n_exp = h.shape[0]
    half = 32
    first, second = pl.ds(0, half), pl.ds(half, half)

    def load(b):
        slot = lax.rem(b - 1, n_buf)
        return pltpu.make_async_copy(wd.at[:, :, pl.ds(pl.multiple_of(b * COLS, COLS), COLS)], wd_buf.at[slot], w_sem.at[slot])

    load(1).start()
    barrier = pltpu.get_barrier_semaphore()
    for d in range(1, N_DEV):
        pl.semaphore_signal(barrier, inc=1, device_id={"ep": lax.rem(me + d, N_DEV)}, device_id_type=MESH)

    def send_d2d(b):
        return remote(part.at[b, 1 - core], d2d.at[b], ds.at[b], dr.at[b], sib)

    def send_1a(b):
        return remote(part.at[b, core, :, 1 - x, first], h1a.at[b], h1as.at[b], h1ar.at[b], xn)

    def send_1b(b):
        return remote(part.at[b, core, 1 - y, :, second], h1b.at[b], h1bs.at[b], h1br.at[b], yn)

    def send_2a(b):
        return remote(part.at[b, core, 1 - y, x, first], h2a.at[b], h2as.at[b], h2ar.at[b], yn)

    def send_2b(b):
        return remote(part.at[b, core, y, 1 - x, second], h2b.at[b], h2bs.at[b], h2br.at[b], xn)

    def lag(b, k, body):
        @pl.when((b >= k) & (b < n_blk + k))
        def _():
            body(b - k)

    def stage_1(b):
        send_d2d(b).start()

    def stage_2(b):
        send_d2d(b).wait_recv()
        part[b, core] += d2d[b]
        send_1a(b).start()
        send_1b(b).start()

    def stage_3(b):
        send_1a(b).wait_recv()
        send_1b(b).wait_recv()
        part[b, core, :, x, first] += h1a[b]
        part[b, core, y, :, second] += h1b[b]
        send_2a(b).start()
        send_2b(b).start()

    def stage_4(b):
        send_2a(b).wait_recv()
        send_2b(b).wait_recv()
        cols = pl.ds(pl.multiple_of(b * COLS, COLS), COLS)
        y_out[first, cols] = (part[b, core, y, x, first] + h2a[b]).astype(BF16)
        y_out[second, cols] = (part[b, core, y, x, second] + h2b[b]).astype(BF16)

    def down(e, weights):
        out = jnp.dot(h[e], weights[e], preferred_element_type=F32).astype(BF16)
        for i in range(N_DEV):
            o[i, pl.ds(e * CAP, CAP), :] = out[i * CAP : (i + 1) * CAP]

    def front(b, weights):
        for e in range(FRONT):
            down(e, weights)

        @pl.when(b + 2 < n_blk)
        def _():
            load(b + 2).start()

    def back(b, weights):
        for e in range(FRONT, n_exp):
            down(e, weights)
        for i in range(N_DEV):
            gates = s[i // 2, :, pl.ds((i % 2) * 64, 64), :].reshape(192, 256)
            terms = jnp.dot(gates, o[i], preferred_element_type=F32)
            part[b, i % 2, i // 4, (i // 2) % 2] = terms[0:64] + terms[64:128] + terms[128:192]

    front(0, wd_on)
    back(0, wd_on)
    pl.semaphore_wait(barrier, N_DEV - 1)

    def step(b, carry):
        lag(b, 1, stage_1)
        weights = wd_buf.at[lax.rem(b - 1, n_buf)]

        @pl.when(b < n_blk)
        def _():
            load(b).wait()
            front(b, weights)

        lag(b, 1, stage_2)
        lag(b, LAG_3, stage_3)
        lag(b, LAG_4, stage_4)

        @pl.when(b < n_blk)
        def _():
            back(b, weights)

        return carry

    lax.fori_loop(1, n_blk + LAG_4, step, 0)

    def drain(b, carry):
        for send in (send_d2d, send_1a, send_1b, send_2a, send_2b):
            send(b).wait_send()
        return carry

    lax.fori_loop(0, n_blk, drain, 0)


def solution(mesh):
    row_spec = P(("dp", "ep"))
    expert_spec = P("ep")
    dma = pltpu.SemaphoreType.DMA

    def local_step(tok, route, gate, wg, wu, wd):
        n_exp, d_model, d_ff = wg.shape
        n_tok = tok.shape[0]
        n_blk = d_model // COLS
        hidden = (n_exp, N_DEV * CAP, d_ff)
        w_on, x_all, codes, h, s, wd_on = pl.pallas_call(
            gather_kernel,
            out_shape=[on_chip((SLOTS, 2, d_model, d_ff), BF16), on_chip((N_DEV * n_tok, d_model), BF16), on_chip((8, 512), F32), on_chip(hidden, BF16), on_chip((4, 3, 128, 256), BF16), on_chip((n_exp, d_ff, COLS), BF16)],
            in_specs=[ANY] * 5,
            out_specs=[VMEM] * 6,
            scratch_shapes=[
                pltpu.VMEM((6, n_tok), jnp.int32),
                pltpu.VMEM((6, n_tok), F32),
                pltpu.VMEM((2, 8, 128), F32),
                pltpu.VMEM((N_DEV, 16, 128), F32),
                pltpu.VMEM((N_DEV, 16, 128), F32),
                dma((SLOTS, 2)),
                dma((3,)),
                dma((7,)),
                dma((7,)),
                dma((6,)),
                dma((6,)),
                dma((N_DEV,)),
                dma((N_DEV,)),
            ],
            compiler_params=pltpu.CompilerParams(collective_id=0, has_side_effects=True, vmem_limit_bytes=LIMIT),
            name="gather",
        )(tok, route.T, gate.T, wg, wu)
        unused, h, wd_on = pl.pallas_call(
            hidden_kernel,
            out_shape=[on_chip(w_on.shape, BF16), on_chip(hidden, BF16), on_chip(wd_on.shape, BF16)],
            in_specs=[VMEM] * 5 + [ANY] * 3,
            out_specs=[VMEM] * 3,
            scratch_shapes=[pltpu.VMEM((256, d_model), BF16), dma((SLOTS, 2, 6)), dma],
            input_output_aliases={0: 0, 1: 1, 2: 2},
            compiler_params=pltpu.CompilerParams(vmem_limit_bytes=LIMIT),
            name="hidden",
        )(pin(w_on), pin(h), pin(wd_on), pin(x_all), pin(codes), wg, wu, wd)
        return pl.pallas_call(
            combine_kernel,
            out_shape=jax.ShapeDtypeStruct((n_tok, d_model), BF16),
            in_specs=[VMEM] * 3 + [ANY],
            out_specs=VMEM,
            scratch_shapes=[
                pltpu.VMEM((3, n_exp, d_ff, COLS), BF16),
                pltpu.VMEM((N_DEV, 256, COLS), BF16),
                pltpu.VMEM((n_blk, 2, 2, 2, n_tok, COLS), F32),
                pltpu.VMEM((n_blk, 2, 2, n_tok, COLS), F32),
                pltpu.VMEM((n_blk, 2, n_tok // 2, COLS), F32),
                pltpu.VMEM((n_blk, 2, n_tok // 2, COLS), F32),
                pltpu.VMEM((n_blk, n_tok // 2, COLS), F32),
                pltpu.VMEM((n_blk, n_tok // 2, COLS), F32),
                dma((3,)),
            ]
            + [dma((n_blk,))] * 10,
            compiler_params=pltpu.CompilerParams(collective_id=1, has_side_effects=True, vmem_limit_bytes=32 << 20),
            name="combine",
        )(pin(h), pin(s), pin(wd_on), wd)

    return jax.shard_map(local_step, mesh=mesh, in_specs=(row_spec, row_spec, row_spec, expert_spec, expert_spec, expert_spec), out_specs=row_spec, check_vma=False)
```

```python
import jax
import jax.numpy as jnp
from jax import lax
from jax.experimental import pallas as pl
from jax.experimental.pallas import tpu as pltpu
from jax.sharding import PartitionSpec as P

BF16 = jnp.bfloat16
F32 = jnp.float32
MESH = pl.DeviceIdType.MESH
N_DEV = 8
CAP = 32
SLOTS = 4
SPLIT = 768
FRONT = 6
LAG_3 = 3
LAG_4 = 6
LIMIT = 4 << 20
COLS = 256
VMEM = pl.BlockSpec(memory_space=pltpu.VMEM)
ANY = pl.BlockSpec(memory_space=pl.ANY)


def remote(src, dst, send_sem, recv_sem, peer):
    return pltpu.make_async_remote_copy(src_ref=src, dst_ref=dst, send_sem=send_sem, recv_sem=recv_sem, device_id={"ep": peer}, device_id_type=MESH)


def on_chip(shape, dtype):
    return pltpu.VMEM(shape, dtype)


def pin(v):
    return pltpu.with_memory_space_constraint(v, pltpu.VMEM)


def place():
    me = lax.axis_index("ep")
    core = lax.rem(me, 2)
    x = lax.rem(me // 2, 2)
    y = me // 4
    return me, core, x, y, me + 1 - 2 * core, me + 2 - 4 * x, me + 4 - 8 * y


def entry_barrier(me):
    barrier = pltpu.get_barrier_semaphore()
    for d in range(1, N_DEV):
        pl.semaphore_signal(barrier, inc=1, device_id={"ep": lax.rem(me + d, N_DEV)}, device_id_type=MESH)
    pl.semaphore_wait(barrier, N_DEV - 1)


def gather_kernel(tok, route_t, gate_t, wg, wu, w_out, x_out, codes_out, h_out, s_out, wd_out, pad_i, pad_g, pad, sg_loc, sg, w_sem, in_sem, sib_s, sib_r, link_s, link_r, sg_s, sg_r):
    me, core, x, y, sib, xn, yn = place()
    n_tok = tok.shape[0]
    half = n_tok // 2

    def rows(device, part=0, count=half):
        return x_out.at[pl.ds(pl.multiple_of(device * n_tok + part * half, half), count)]

    own = pltpu.make_async_copy(tok, rows(me, 0, n_tok), in_sem.at[0])
    own_route = pltpu.make_async_copy(route_t, pad_i, in_sem.at[1])
    own_gate = pltpu.make_async_copy(gate_t, pad_g, in_sem.at[2])
    own.start()
    own_route.start()
    own_gate.start()
    barrier = pltpu.get_barrier_semaphore()
    for d in range(1, N_DEV):
        pl.semaphore_signal(barrier, inc=1, device_id={"ep": lax.rem(me + d, N_DEV)}, device_id_type=MESH)
    loads = []
    for e in range(SLOTS):
        loads.append(pltpu.make_async_copy(wg.at[e], w_out.at[e, 0], w_sem.at[e, 0]))
        loads.append(pltpu.make_async_copy(wu.at[e], w_out.at[e, 1], w_sem.at[e, 1]))
    for load in loads:
        load.start()

    pad[...] = jnp.zeros_like(pad)
    own_route.wait()
    pad[0, 0:6, 0:n_tok] = pad_i[...].astype(F32)
    own_gate.wait()
    pad[1, 0:6, 0:n_tok] = pad_g[...]
    routes = pad[0] + pltpu.roll(pad[0], n_tok, 1)
    gates = pad[1] + pltpu.roll(pad[1], n_tok, 1)
    expert = lax.broadcasted_iota(jnp.int32, (64, 128), 0).astype(F32)
    lane = lax.broadcasted_iota(jnp.int32, (64, 128), 1)
    mine = (lane // n_tok) == core
    member = jnp.zeros((64, 128), F32)
    weight = jnp.zeros((64, 128), F32)
    for k in range(6):
        hit = (expert == routes[k : k + 1, :]) & mine
        member = jnp.where(hit, 1.0, member)
        weight = jnp.where(hit, gates[k : k + 1, :], weight)
    row = lax.broadcasted_iota(jnp.int32, (128, 128), 0)
    col = lax.broadcasted_iota(jnp.int32, (128, 128), 1)
    upto = jnp.where((row <= col), 1.0, 0.0).astype(BF16)
    rank = jnp.dot(member.astype(BF16), upto, preferred_element_type=F32)
    code = jnp.where(member > 0.5, rank + (me * CAP).astype(F32), 0.0)
    sg_loc[:, 0:8, :] = code.reshape(8, 8, 128)
    sg_loc[:, 8:16, :] = weight.reshape(8, 8, 128)
    sg[me] = sg_loc[me]
    pl.semaphore_wait(barrier, N_DEV - 1)

    sg_copies = []
    for d in range(1, N_DEV):
        peer = lax.rem(me + d, N_DEV)
        sg_copies.append(remote(sg_loc.at[peer], sg.at[me], sg_s.at[d], sg_r.at[d], peer))
    for copy in sg_copies:
        copy.start()
    to_x_a = remote(rows(me, 0), rows(me, 0), link_s.at[0], link_r.at[0], xn)
    to_x_b = remote(rows(me, 1), rows(me, 1), link_s.at[1], link_r.at[1], xn)
    to_y_b = remote(rows(me, 1), rows(me, 1), link_s.at[2], link_r.at[2], yn)
    to_y_a = remote(rows(me, 0), rows(me, 0), link_s.at[3], link_r.at[3], yn)
    to_sib = remote(rows(me, 0, n_tok), rows(me, 0, n_tok), sib_s.at[0], sib_r.at[0], sib)
    own.wait()
    for copy in (to_x_a, to_y_b, to_x_b, to_y_a, to_sib):
        copy.start()
    dg = lax.rem(xn + 4, N_DEV)
    passed = []

    def pass_on(index, source, part):
        copy = remote(rows(source, part), rows(source, part), sib_s.at[index], sib_r.at[index], sib)
        copy.start()
        passed.append(copy)

    to_x_a.wait_recv()
    via_y = remote(rows(xn, 0), rows(xn, 0), link_s.at[4], link_r.at[4], yn)
    via_y.start()
    pass_on(1, xn, 0)
    to_y_b.wait_recv()
    via_x = remote(rows(yn, 1), rows(yn, 1), link_s.at[5], link_r.at[5], xn)
    via_x.start()
    pass_on(2, yn, 1)
    for copy in sg_copies:
        copy.wait()

    r = lax.broadcasted_iota(jnp.int32, (256, 128), 0)
    lane = lax.broadcasted_iota(jnp.int32, (256, 128), 1)
    for p in range(4):
        target = ((2 * p + lane // 64) * CAP + lax.rem(r, CAP) + 1).astype(F32)
        code = sg[2 * p, 0:8, :] + sg[2 * p + 1, 0:8, :]
        gate = sg[2 * p, 8:16, :] + sg[2 * p + 1, 8:16, :]
        codes_out[:, pl.ds(p * 128, 128)] = code
        code = jnp.broadcast_to(code[:, None, :], (8, CAP, 128)).reshape(256, 128)
        gate = jnp.broadcast_to(gate[:, None, :], (8, CAP, 128)).reshape(256, 128)
        s_t = jnp.where(code == target, gate, 0.0)
        s_f = s_t.T
        hi = jnp.minimum(s_f, 3.3895e38).astype(BF16)
        rest = s_f - hi.astype(F32)
        mid = rest.astype(BF16)
        low = (rest - mid.astype(F32)).astype(BF16)
        s_out[p, 0] = hi
        s_out[p, 1] = mid
        s_out[p, 2] = low

    to_x_b.wait_recv()
    pass_on(3, xn, 1)
    to_y_a.wait_recv()
    pass_on(4, yn, 0)
    via_y.wait_recv()
    pass_on(5, dg, 0)
    via_x.wait_recv()
    pass_on(6, dg, 1)
    for copy in (to_x_a, to_x_b, to_y_b, to_y_a, via_y, via_x):
        copy.wait_send()
    to_sib.wait()
    for copy in passed:
        copy.wait()
    for load in loads:
        load.wait()


def hidden_kernel(w_in, h_in, wd_in, x_all, codes, wg, wu, wd, w_buf, h_out, wd_out, xe, w_sem, d_sem):
    n_exp = wg.shape[0]
    d_ff = wg.shape[2]
    panels = [(c, min(256, d_ff - c)) for c in range(0, d_ff, 256)]
    down = pltpu.make_async_copy(wd.at[:, :, pl.ds(0, COLS)], wd_out, d_sem)

    def load(e, p):
        slot = lax.rem(e, SLOTS)
        cols = pl.ds(p * SPLIT, SPLIT if p == 0 else d_ff - SPLIT)
        return [pltpu.make_async_copy(src.at[e, :, cols], w_buf.at[slot, part, :, cols], w_sem.at[slot, part, p]) for part, src in ((0, wg), (1, wu))]

    def hidden_rows(e, cap, before, after):
        m = cap * N_DEV
        slot = lax.rem(e, SLOTS)
        r = lax.broadcasted_iota(jnp.int32, (m, 512), 0)
        target = ((r // cap) * CAP + lax.rem(r, cap) + 1).astype(F32)
        pick = (target == codes[pl.ds(e, 1), :]).astype(BF16)
        for c in range(0, x_all.shape[1], 512):
            part = jnp.dot(pick, x_all[:, pl.ds(c, 512)], preferred_element_type=F32)
            xe[pl.ds(0, m), pl.ds(c, 512)] = part.astype(BF16)

        def put(a, b, c, w):
            act = (a * jax.nn.sigmoid(a) * b).astype(BF16)
            if cap == CAP:
                h_out[e, :, pl.ds(c, w)] = act
            else:
                for i in range(N_DEV):
                    h_out[e, pl.ds(i * CAP, cap), pl.ds(c, w)] = act[i * cap : (i + 1) * cap]
                    h_out[e, pl.ds(i * CAP + cap, CAP - cap), pl.ds(c, w)] = jnp.zeros((CAP - cap, w), BF16)

        rows = xe[pl.ds(0, m), :]
        for p, (c, w) in enumerate(panels):
            before(e, p)
            if w == 256:
                a = jnp.dot(rows, w_buf[slot, 0, :, pl.ds(c, w)], preferred_element_type=F32)
                b = jnp.dot(rows, w_buf[slot, 1, :, pl.ds(c, w)], preferred_element_type=F32)
            else:
                both = jnp.concatenate([w_buf[slot, 0, :, pl.ds(c, w)], w_buf[slot, 1, :, pl.ds(c, w)]], axis=1)
                ab = jnp.dot(rows, both, preferred_element_type=F32)
                a, b = ab[:, :w], ab[:, w:]
            put(a, b, c, w)
            after(e, p)

    def expert(e, before, after):
        code_row = codes[pl.ds(e, 1), :]
        block = lax.broadcasted_iota(jnp.int32, (1, 512), 1) // 64
        small = jnp.max(code_row - (block * CAP).astype(F32)) <= 16.0

        @pl.when(small)
        def _():
            hidden_rows(e, CAP // 2, before, after)

        @pl.when(jnp.logical_not(small))
        def _():
            hidden_rows(e, CAP, before, after)

    def nothing(e, p):
        pass

    def refill(e, p):
        if panels[p][0] + 256 == SPLIT or p == len(panels) - 1:
            for copy in load(e + SLOTS, p // 3):
                copy.start()

    def arrive(e, p):
        if panels[p][0] in (0, SPLIT):
            for copy in load(e, p // 3):
                copy.wait()

    def early(e, carry):
        expert(e, nothing, refill)
        return carry

    def late(e, carry):
        expert(e, arrive, nothing)
        return carry

    down.start()
    lax.fori_loop(0, SLOTS, early, 0)
    lax.fori_loop(SLOTS, n_exp, late, 0)
    down.wait()


def combine_kernel(h, s, wd_on, wd, y_out, wd_one, wd_pair, o, part, d2d, h1a, h1b, h2a, h2b, one_sem, pair_sem, ds, dr, h1as, h1ar, h1bs, h1br, h2as, h2ar, h2bs, h2br):
    me, core, x, y, sib, xn, yn = place()
    n_blk = wd.shape[2] // COLS
    n_exp = h.shape[0]
    half = 32
    first, second = pl.ds(0, half), pl.ds(half, half)

    one = pltpu.make_async_copy(wd.at[:, :, pl.ds(COLS, COLS)], wd_one, one_sem)

    def pair(q):
        cols = pl.ds(pl.multiple_of((q + 1) * 2 * COLS, 2 * COLS), 2 * COLS)
        slot = lax.rem(q, 2)
        return pltpu.make_async_copy(wd.at[:, :, cols], wd_pair.at[slot], pair_sem.at[slot])

    one.start()
    barrier = pltpu.get_barrier_semaphore()
    for d in range(1, N_DEV):
        pl.semaphore_signal(barrier, inc=1, device_id={"ep": lax.rem(me + d, N_DEV)}, device_id_type=MESH)

    def send_d2d(b):
        return remote(part.at[b, 1 - core], d2d.at[b], ds.at[b], dr.at[b], sib)

    def send_1a(b):
        return remote(part.at[b, core, :, 1 - x, first], h1a.at[b], h1as.at[b], h1ar.at[b], xn)

    def send_1b(b):
        return remote(part.at[b, core, 1 - y, :, second], h1b.at[b], h1bs.at[b], h1br.at[b], yn)

    def send_2a(b):
        return remote(part.at[b, core, 1 - y, x, first], h2a.at[b], h2as.at[b], h2ar.at[b], yn)

    def send_2b(b):
        return remote(part.at[b, core, y, 1 - x, second], h2b.at[b], h2bs.at[b], h2br.at[b], xn)

    def lag(b, k, body):
        @pl.when((b >= k) & (b < n_blk + k))
        def _():
            body(b - k)

    def stage_1(b):
        send_d2d(b).start()

    def stage_2(b):
        send_d2d(b).wait_recv()
        part[b, core] += d2d[b]
        send_1a(b).start()
        send_1b(b).start()

    def stage_3(b):
        send_1a(b).wait_recv()
        send_1b(b).wait_recv()
        part[b, core, :, x, first] += h1a[b]
        part[b, core, y, :, second] += h1b[b]
        send_2a(b).start()
        send_2b(b).start()

    def stage_4(b):
        send_2a(b).wait_recv()
        send_2b(b).wait_recv()
        cols = pl.ds(pl.multiple_of(b * COLS, COLS), COLS)
        y_out[first, cols] = (part[b, core, y, x, first] + h2a[b]).astype(BF16)
        y_out[second, cols] = (part[b, core, y, x, second] + h2b[b]).astype(BF16)

    def down(e, weights):
        out = jnp.dot(h[e], weights[e], preferred_element_type=F32).astype(BF16)
        for i in range(N_DEV):
            o[i, pl.ds(e * CAP, CAP), :] = out[i * CAP : (i + 1) * CAP]

    def front(weights):
        for e in range(FRONT):
            down(e, weights)

    def back(b, weights):
        for e in range(FRONT, n_exp):
            down(e, weights)
        for i in range(N_DEV):
            gates = s[i // 2, :, pl.ds((i % 2) * 64, 64), :].reshape(192, 256)
            terms = jnp.dot(gates, o[i], preferred_element_type=F32)
            part[b, i % 2, i // 4, (i // 2) % 2] = terms[0:64] + terms[64:128] + terms[128:192]

    front(wd_on)
    pair(0).start()
    back(0, wd_on)
    pl.semaphore_wait(barrier, N_DEV - 1)
    stage_1(0)
    one.wait()
    front(wd_one)
    stage_2(0)
    pair(1).start()
    back(1, wd_one)

    def step(b, carry):
        lag(b, 1, stage_1)
        q = (b - 2) // 2
        cols = pl.ds(pl.multiple_of(lax.rem(b, 2) * COLS, COLS), COLS)
        weights = wd_pair.at[lax.rem(q, 2), :, :, cols]

        @pl.when((b < n_blk) & (lax.rem(b, 2) == 0))
        def _():
            pair(q).wait()

        @pl.when(b < n_blk)
        def _():
            front(weights)

        lag(b, 1, stage_2)
        lag(b, LAG_3, stage_3)
        lag(b, LAG_4, stage_4)

        @pl.when(b < n_blk)
        def _():
            back(b, weights)

        @pl.when((lax.rem(b, 2) == 1) & (b + 4 < n_blk))
        def _():
            pair(q + 2).start()

        return carry

    lax.fori_loop(2, n_blk + LAG_4, step, 0)

    def drain(b, carry):
        for send in (send_d2d, send_1a, send_1b, send_2a, send_2b):
            send(b).wait_send()
        return carry

    lax.fori_loop(0, n_blk, drain, 0)


def solution(mesh):
    row_spec = P(("dp", "ep"))
    expert_spec = P("ep")
    dma = pltpu.SemaphoreType.DMA

    def local_step(tok, route, gate, wg, wu, wd):
        n_exp, d_model, d_ff = wg.shape
        n_tok = tok.shape[0]
        n_blk = d_model // COLS
        hidden = (n_exp, N_DEV * CAP, d_ff)
        w_on, x_all, codes, h, s, wd_on = pl.pallas_call(
            gather_kernel,
            out_shape=[on_chip((SLOTS, 2, d_model, d_ff), BF16), on_chip((N_DEV * n_tok, d_model), BF16), on_chip((8, 512), F32), on_chip(hidden, BF16), on_chip((4, 3, 128, 256), BF16), on_chip((n_exp, d_ff, COLS), BF16)],
            in_specs=[ANY] * 5,
            out_specs=[VMEM] * 6,
            scratch_shapes=[
                pltpu.VMEM((6, n_tok), jnp.int32),
                pltpu.VMEM((6, n_tok), F32),
                pltpu.VMEM((2, 8, 128), F32),
                pltpu.VMEM((N_DEV, 16, 128), F32),
                pltpu.VMEM((N_DEV, 16, 128), F32),
                dma((SLOTS, 2)),
                dma((3,)),
                dma((7,)),
                dma((7,)),
                dma((6,)),
                dma((6,)),
                dma((N_DEV,)),
                dma((N_DEV,)),
            ],
            compiler_params=pltpu.CompilerParams(collective_id=0, has_side_effects=True, vmem_limit_bytes=LIMIT),
            name="gather",
        )(tok, route.T, gate.T, wg, wu)
        unused, h, wd_on = pl.pallas_call(
            hidden_kernel,
            out_shape=[on_chip(w_on.shape, BF16), on_chip(hidden, BF16), on_chip(wd_on.shape, BF16)],
            in_specs=[VMEM] * 5 + [ANY] * 3,
            out_specs=[VMEM] * 3,
            scratch_shapes=[pltpu.VMEM((256, d_model), BF16), dma((SLOTS, 2, 2)), dma],
            input_output_aliases={0: 0, 1: 1, 2: 2},
            compiler_params=pltpu.CompilerParams(vmem_limit_bytes=LIMIT),
            name="hidden",
        )(pin(w_on), pin(h), pin(wd_on), pin(x_all), pin(codes), wg, wu, wd)
        return pl.pallas_call(
            combine_kernel,
            out_shape=jax.ShapeDtypeStruct((n_tok, d_model), BF16),
            in_specs=[VMEM] * 3 + [ANY],
            out_specs=VMEM,
            scratch_shapes=[
                pltpu.VMEM((n_exp, d_ff, COLS), BF16),
                pltpu.VMEM((2, n_exp, d_ff, 2 * COLS), BF16),
                pltpu.VMEM((N_DEV, 256, COLS), BF16),
                pltpu.VMEM((n_blk, 2, 2, 2, n_tok, COLS), F32),
                pltpu.VMEM((n_blk, 2, 2, n_tok, COLS), F32),
                pltpu.VMEM((n_blk, 2, n_tok // 2, COLS), F32),
                pltpu.VMEM((n_blk, 2, n_tok // 2, COLS), F32),
                pltpu.VMEM((n_blk, n_tok // 2, COLS), F32),
                pltpu.VMEM((n_blk, n_tok // 2, COLS), F32),
                dma,
                dma((2,)),
            ]
            + [dma((n_blk,))] * 10,
            compiler_params=pltpu.CompilerParams(collective_id=1, has_side_effects=True, vmem_limit_bytes=38 << 20),
            name="combine",
        )(pin(h), pin(s), pin(wd_on), wd)

    return jax.shard_map(local_step, mesh=mesh, in_specs=(row_spec, row_spec, row_spec, expert_spec, expert_spec, expert_spec), out_specs=row_spec, check_vma=False)
```

```python
import jax
import jax.numpy as jnp
from jax import lax
from jax.experimental import pallas as pl
from jax.experimental.pallas import tpu as pltpu
from jax.sharding import PartitionSpec as P

BF16 = jnp.bfloat16
F32 = jnp.float32
MESH = pl.DeviceIdType.MESH
N_DEV = 8
CAP = 32
SLOTS = 3
AHEAD = 2
FRONT = 6
LAG_3 = 3
LAG_4 = 6
LIMIT = 4 << 20
COLS = 256
VMEM = pl.BlockSpec(memory_space=pltpu.VMEM)
ANY = pl.BlockSpec(memory_space=pl.ANY)


def remote(src, dst, send_sem, recv_sem, peer):
    return pltpu.make_async_remote_copy(src_ref=src, dst_ref=dst, send_sem=send_sem, recv_sem=recv_sem, device_id={"ep": peer}, device_id_type=MESH)


def on_chip(shape, dtype):
    return pltpu.VMEM(shape, dtype)


def pin(v):
    return pltpu.with_memory_space_constraint(v, pltpu.VMEM)


def place():
    me = lax.axis_index("ep")
    core = lax.rem(me, 2)
    x = lax.rem(me // 2, 2)
    y = me // 4
    return me, core, x, y, me + 1 - 2 * core, me + 2 - 4 * x, me + 4 - 8 * y


def entry_barrier(me):
    barrier = pltpu.get_barrier_semaphore()
    for d in range(1, N_DEV):
        pl.semaphore_signal(barrier, inc=1, device_id={"ep": lax.rem(me + d, N_DEV)}, device_id_type=MESH)
    pl.semaphore_wait(barrier, N_DEV - 1)


def gather_kernel(tok, route_t, gate_t, wg, wu, wd, w_out, x_out, codes_out, s_out, wd_out, h_out, o_out, pad_i, pad_g, pad, sg_loc, sg, w_sem, d_sem, in_sem, sib_s, sib_r, link_s, link_r, sg_s, sg_r):
    me, core, x, y, sib, xn, yn = place()
    n_tok = tok.shape[0]
    half = n_tok // 2

    def rows(device, part=0, count=half):
        return x_out.at[pl.ds(pl.multiple_of(device * n_tok + part * half, half), count)]

    own = pltpu.make_async_copy(tok, rows(me, 0, n_tok), in_sem.at[0])
    own_route = pltpu.make_async_copy(route_t, pad_i, in_sem.at[1])
    own_gate = pltpu.make_async_copy(gate_t, pad_g, in_sem.at[2])
    own.start()
    own_route.start()
    own_gate.start()
    barrier = pltpu.get_barrier_semaphore()
    for d in range(1, N_DEV):
        pl.semaphore_signal(barrier, inc=1, device_id={"ep": lax.rem(me + d, N_DEV)}, device_id_type=MESH)
    loads = []
    for e in range(SLOTS):
        loads.append(pltpu.make_async_copy(wg.at[e], w_out.at[e, 0], w_sem.at[e, 0]))
        loads.append(pltpu.make_async_copy(wu.at[e], w_out.at[e, 1], w_sem.at[e, 1]))
    loads.append(pltpu.make_async_copy(wd.at[:, :, pl.ds(0, AHEAD * COLS)], wd_out, d_sem))
    for load in loads:
        load.start()

    pad[...] = jnp.zeros_like(pad)
    own_route.wait()
    pad[0, 0:6, 0:n_tok] = pad_i[...].astype(F32)
    own_gate.wait()
    pad[1, 0:6, 0:n_tok] = pad_g[...]
    routes = pad[0] + pltpu.roll(pad[0], n_tok, 1)
    gates = pad[1] + pltpu.roll(pad[1], n_tok, 1)
    expert = lax.broadcasted_iota(jnp.int32, (64, 128), 0).astype(F32)
    lane = lax.broadcasted_iota(jnp.int32, (64, 128), 1)
    mine = (lane // n_tok) == core
    member = jnp.zeros((64, 128), F32)
    weight = jnp.zeros((64, 128), F32)
    for k in range(6):
        hit = (expert == routes[k : k + 1, :]) & mine
        member = jnp.where(hit, 1.0, member)
        weight = jnp.where(hit, gates[k : k + 1, :], weight)
    row = lax.broadcasted_iota(jnp.int32, (128, 128), 0)
    col = lax.broadcasted_iota(jnp.int32, (128, 128), 1)
    upto = jnp.where((row <= col), 1.0, 0.0).astype(BF16)
    rank = jnp.dot(member.astype(BF16), upto, preferred_element_type=F32)
    code = jnp.where(member > 0.5, rank + (me * CAP).astype(F32), 0.0)
    sg_loc[:, 0:8, :] = code.reshape(8, 8, 128)
    sg_loc[:, 8:16, :] = weight.reshape(8, 8, 128)
    sg[me] = sg_loc[me]
    pl.semaphore_wait(barrier, N_DEV - 1)

    sg_copies = []
    for d in range(1, N_DEV):
        peer = lax.rem(me + d, N_DEV)
        sg_copies.append(remote(sg_loc.at[peer], sg.at[me], sg_s.at[d], sg_r.at[d], peer))
    for copy in sg_copies:
        copy.start()
    to_x_a = remote(rows(me, 0), rows(me, 0), link_s.at[0], link_r.at[0], xn)
    to_x_b = remote(rows(me, 1), rows(me, 1), link_s.at[1], link_r.at[1], xn)
    to_y_b = remote(rows(me, 1), rows(me, 1), link_s.at[2], link_r.at[2], yn)
    to_y_a = remote(rows(me, 0), rows(me, 0), link_s.at[3], link_r.at[3], yn)
    to_sib = remote(rows(me, 0, n_tok), rows(me, 0, n_tok), sib_s.at[0], sib_r.at[0], sib)
    own.wait()
    for copy in (to_x_a, to_y_b, to_x_b, to_y_a, to_sib):
        copy.start()
    dg = lax.rem(xn + 4, N_DEV)
    passed = []

    def pass_on(index, source, part):
        copy = remote(rows(source, part), rows(source, part), sib_s.at[index], sib_r.at[index], sib)
        copy.start()
        passed.append(copy)

    to_x_a.wait_recv()
    via_y = remote(rows(xn, 0), rows(xn, 0), link_s.at[4], link_r.at[4], yn)
    via_y.start()
    pass_on(1, xn, 0)
    to_y_b.wait_recv()
    via_x = remote(rows(yn, 1), rows(yn, 1), link_s.at[5], link_r.at[5], xn)
    via_x.start()
    pass_on(2, yn, 1)
    for copy in sg_copies:
        copy.wait()

    r = lax.broadcasted_iota(jnp.int32, (256, 128), 0)
    lane = lax.broadcasted_iota(jnp.int32, (256, 128), 1)
    for p in range(4):
        target = ((2 * p + lane // 64) * CAP + lax.rem(r, CAP) + 1).astype(F32)
        code = sg[2 * p, 0:8, :] + sg[2 * p + 1, 0:8, :]
        gate = sg[2 * p, 8:16, :] + sg[2 * p + 1, 8:16, :]
        codes_out[:, pl.ds(p * 128, 128)] = code
        code = jnp.broadcast_to(code[:, None, :], (8, CAP, 128)).reshape(256, 128)
        gate = jnp.broadcast_to(gate[:, None, :], (8, CAP, 128)).reshape(256, 128)
        s_t = jnp.where(code == target, gate, 0.0)
        s_f = s_t.T
        hi = jnp.minimum(s_f, 3.3895e38).astype(BF16)
        rest = s_f - hi.astype(F32)
        mid = rest.astype(BF16)
        low = (rest - mid.astype(F32)).astype(BF16)
        s_out[p, 0] = hi
        s_out[p, 1] = mid
        s_out[p, 2] = low

    to_x_b.wait_recv()
    pass_on(3, xn, 1)
    to_y_a.wait_recv()
    pass_on(4, yn, 0)
    via_y.wait_recv()
    pass_on(5, dg, 0)
    via_x.wait_recv()
    pass_on(6, dg, 1)
    for copy in (to_x_a, to_x_b, to_y_b, to_y_a, via_y, via_x):
        copy.wait_send()
    to_sib.wait()
    for copy in passed:
        copy.wait()
    for load in loads:
        load.wait()


def hidden_kernel(w_in, h_in, o_in, x_all, codes, wd_on, wg, wu, w_buf, h_out, o_out, xe, hc, w_sem):
    n_exp = wg.shape[0]
    d_ff = wg.shape[2]
    panels = [(c, min(256, d_ff - c)) for c in range(0, d_ff, 256)]

    def load(e, part, src):
        slot = lax.rem(e, SLOTS)
        return pltpu.make_async_copy(src.at[e], w_buf.at[slot, part], w_sem.at[slot, part])

    def hidden_rows(e, cap):
        m = cap * N_DEV
        slot = lax.rem(e, SLOTS)
        r = lax.broadcasted_iota(jnp.int32, (m, 512), 0)
        target = ((r // cap) * CAP + lax.rem(r, cap) + 1).astype(F32)
        pick = (target == codes[pl.ds(e, 1), :]).astype(BF16)
        for c in range(0, x_all.shape[1], 512):
            part = jnp.dot(pick, x_all[:, pl.ds(c, 512)], preferred_element_type=F32)
            xe[pl.ds(0, m), pl.ds(c, 512)] = part.astype(BF16)

        rows = xe[pl.ds(0, m), :]
        for c, w in panels:
            if w == 256:
                a = jnp.dot(rows, w_buf[slot, 0, :, pl.ds(c, w)], preferred_element_type=F32)
                b = jnp.dot(rows, w_buf[slot, 1, :, pl.ds(c, w)], preferred_element_type=F32)
            else:
                both = jnp.concatenate([w_buf[slot, 0, :, pl.ds(c, w)], w_buf[slot, 1, :, pl.ds(c, w)]], axis=1)
                ab = jnp.dot(rows, both, preferred_element_type=F32)
                a, b = ab[:, :w], ab[:, w:]
            act = (a * jax.nn.sigmoid(a) * b).astype(BF16)
            hc[pl.ds(0, m), pl.ds(c, w)] = act
            if cap == CAP:
                h_out[e, :, pl.ds(c, w)] = act
            else:
                for i in range(N_DEV):
                    h_out[e, pl.ds(i * CAP, cap), pl.ds(c, w)] = act[i * cap : (i + 1) * cap]
                    h_out[e, pl.ds(i * CAP + cap, CAP - cap), pl.ds(c, w)] = jnp.zeros((CAP - cap, w), BF16)

        at = pl.multiple_of(e * CAP, CAP)
        out = jnp.dot(hc[pl.ds(0, m), :], wd_on[e], preferred_element_type=F32).astype(BF16)
        for k in range(AHEAD):
            for i in range(N_DEV):
                o_out[k, i, pl.ds(at, cap), :] = out[i * cap : (i + 1) * cap, k * COLS : (k + 1) * COLS]
                if cap < CAP:
                    o_out[k, i, pl.ds(at + cap, CAP - cap), :] = jnp.zeros((CAP - cap, COLS), BF16)

    def step(e, carry):
        @pl.when(e >= SLOTS)
        def _():
            load(e, 0, wg).wait()
            load(e, 1, wu).wait()

        code_row = codes[pl.ds(e, 1), :]
        block = lax.broadcasted_iota(jnp.int32, (1, 512), 1) // 64
        small = jnp.max(code_row - (block * CAP).astype(F32)) <= 16.0

        @pl.when(small)
        def _():
            hidden_rows(e, CAP // 2)

        @pl.when(jnp.logical_not(small))
        def _():
            hidden_rows(e, CAP)

        @pl.when(e + SLOTS < n_exp)
        def _():
            load(e + SLOTS, 0, wg).start()
            load(e + SLOTS, 1, wu).start()

        return carry

    lax.fori_loop(0, n_exp, step, 0)


def combine_kernel(h, s, o_on, wd, y_out, wd_buf, o, part, d2d, h1a, h1b, h2a, h2b, w_sem, ds, dr, h1as, h1ar, h1bs, h1br, h2as, h2ar, h2bs, h2br):
    me, core, x, y, sib, xn, yn = place()
    n_blk = wd.shape[2] // COLS
    n_exp = h.shape[0]
    half = 32
    first, second = pl.ds(0, half), pl.ds(half, half)

    n_buf = wd_buf.shape[0]

    def load(b):
        slot = lax.rem(b - AHEAD, n_buf)
        return pltpu.make_async_copy(wd.at[:, :, pl.ds(pl.multiple_of(b * COLS, COLS), COLS)], wd_buf.at[slot], w_sem.at[slot])

    load(AHEAD).start()
    barrier = pltpu.get_barrier_semaphore()
    for d in range(1, N_DEV):
        pl.semaphore_signal(barrier, inc=1, device_id={"ep": lax.rem(me + d, N_DEV)}, device_id_type=MESH)

    def send_d2d(b):
        return remote(part.at[b, 1 - core], d2d.at[b], ds.at[b], dr.at[b], sib)

    def send_1a(b):
        return remote(part.at[b, core, :, 1 - x, first], h1a.at[b], h1as.at[b], h1ar.at[b], xn)

    def send_1b(b):
        return remote(part.at[b, core, 1 - y, :, second], h1b.at[b], h1bs.at[b], h1br.at[b], yn)

    def send_2a(b):
        return remote(part.at[b, core, 1 - y, x, first], h2a.at[b], h2as.at[b], h2ar.at[b], yn)

    def send_2b(b):
        return remote(part.at[b, core, y, 1 - x, second], h2b.at[b], h2bs.at[b], h2br.at[b], xn)

    def lag(b, k, body):
        @pl.when((b >= k) & (b < n_blk + k))
        def _():
            body(b - k)

    def stage_1(b):
        send_d2d(b).start()

    def stage_2(b):
        send_d2d(b).wait_recv()
        part[b, core] += d2d[b]
        send_1a(b).start()
        send_1b(b).start()

    def stage_3(b):
        send_1a(b).wait_recv()
        send_1b(b).wait_recv()
        part[b, core, :, x, first] += h1a[b]
        part[b, core, y, :, second] += h1b[b]
        send_2a(b).start()
        send_2b(b).start()

    def stage_4(b):
        send_2a(b).wait_recv()
        send_2b(b).wait_recv()
        cols = pl.ds(pl.multiple_of(b * COLS, COLS), COLS)
        y_out[first, cols] = (part[b, core, y, x, first] + h2a[b]).astype(BF16)
        y_out[second, cols] = (part[b, core, y, x, second] + h2b[b]).astype(BF16)

    def down(e, weights):
        out = jnp.dot(h[e], weights[e], preferred_element_type=F32).astype(BF16)
        for i in range(N_DEV):
            o[i, pl.ds(e * CAP, CAP), :] = out[i * CAP : (i + 1) * CAP]

    def gather_sum(b, out):
        for i in range(N_DEV):
            gates = s[i // 2, :, pl.ds((i % 2) * 64, 64), :].reshape(192, 256)
            terms = jnp.dot(gates, out[i], preferred_element_type=F32)
            part[b, i % 2, i // 4, (i // 2) % 2] = terms[0:64] + terms[64:128] + terms[128:192]

    gather_sum(0, o_on.at[0])
    pl.semaphore_wait(barrier, N_DEV - 1)
    stage_1(0)
    gather_sum(1, o_on.at[1])
    stage_1(1)
    load(AHEAD + 1).start()
    stage_2(0)
    stage_2(1)

    def step(b, carry):
        @pl.when((b > AHEAD) & (b < n_blk + 1))
        def _():
            stage_1(b - 1)

        weights = wd_buf.at[lax.rem(b - AHEAD, n_buf)]

        @pl.when(b < n_blk)
        def _():
            load(b).wait()
            for e in range(FRONT):
                down(e, weights)

        @pl.when(b + 2 < n_blk)
        def _():
            load(b + 2).start()

        @pl.when((b > AHEAD) & (b < n_blk + 1))
        def _():
            stage_2(b - 1)

        lag(b, LAG_3, stage_3)
        lag(b, LAG_4, stage_4)

        @pl.when(b < n_blk)
        def _():
            for e in range(FRONT, n_exp):
                down(e, weights)
            gather_sum(b, o)

        return carry

    lax.fori_loop(AHEAD, n_blk + LAG_4, step, 0)

    def drain(b, carry):
        for send in (send_d2d, send_1a, send_1b, send_2a, send_2b):
            send(b).wait_send()
        return carry

    lax.fori_loop(0, n_blk, drain, 0)


def solution(mesh):
    row_spec = P(("dp", "ep"))
    expert_spec = P("ep")
    dma = pltpu.SemaphoreType.DMA

    def local_step(tok, route, gate, wg, wu, wd):
        n_exp, d_model, d_ff = wg.shape
        n_tok = tok.shape[0]
        n_blk = d_model // COLS
        hidden = (n_exp, N_DEV * CAP, d_ff)
        down_2, rows_2 = (n_exp, d_ff, AHEAD * COLS), (AHEAD, N_DEV, 256, COLS)
        w_on, x_all, codes, s, wd_on, h, o_on = pl.pallas_call(
            gather_kernel,
            out_shape=[on_chip((SLOTS, 2, d_model, d_ff), BF16), on_chip((N_DEV * n_tok, d_model), BF16), on_chip((8, 512), F32), on_chip((4, 3, 128, 256), BF16), on_chip(down_2, BF16), on_chip(hidden, BF16), on_chip(rows_2, BF16)],
            in_specs=[ANY] * 6,
            out_specs=[VMEM] * 7,
            scratch_shapes=[
                pltpu.VMEM((6, n_tok), jnp.int32),
                pltpu.VMEM((6, n_tok), F32),
                pltpu.VMEM((2, 8, 128), F32),
                pltpu.VMEM((N_DEV, 16, 128), F32),
                pltpu.VMEM((N_DEV, 16, 128), F32),
                dma((SLOTS, 2)),
                dma,
                dma((3,)),
                dma((7,)),
                dma((7,)),
                dma((6,)),
                dma((6,)),
                dma((N_DEV,)),
                dma((N_DEV,)),
            ],
            compiler_params=pltpu.CompilerParams(collective_id=0, has_side_effects=True, vmem_limit_bytes=LIMIT),
            name="gather",
        )(tok, route.T, gate.T, wg, wu, wd)
        unused, h, o_on = pl.pallas_call(
            hidden_kernel,
            out_shape=[on_chip(w_on.shape, BF16), on_chip(hidden, BF16), on_chip(rows_2, BF16)],
            in_specs=[VMEM] * 6 + [ANY] * 2,
            out_specs=[VMEM] * 3,
            scratch_shapes=[pltpu.VMEM((256, d_model), BF16), pltpu.VMEM((256, d_ff), BF16), dma((SLOTS, 2))],
            input_output_aliases={0: 0, 1: 1, 2: 2},
            compiler_params=pltpu.CompilerParams(vmem_limit_bytes=LIMIT),
            name="hidden",
        )(pin(w_on), pin(h), pin(o_on), pin(x_all), pin(codes), pin(wd_on), wg, wu)
        return pl.pallas_call(
            combine_kernel,
            out_shape=jax.ShapeDtypeStruct((n_tok, d_model), BF16),
            in_specs=[VMEM] * 3 + [ANY],
            out_specs=VMEM,
            scratch_shapes=[
                pltpu.VMEM((3, n_exp, d_ff, COLS), BF16),
                pltpu.VMEM((N_DEV, 256, COLS), BF16),
                pltpu.VMEM((n_blk, 2, 2, 2, n_tok, COLS), F32),
                pltpu.VMEM((n_blk, 2, 2, n_tok, COLS), F32),
                pltpu.VMEM((n_blk, 2, n_tok // 2, COLS), F32),
                pltpu.VMEM((n_blk, 2, n_tok // 2, COLS), F32),
                pltpu.VMEM((n_blk, n_tok // 2, COLS), F32),
                pltpu.VMEM((n_blk, n_tok // 2, COLS), F32),
                dma((3,)),
            ]
            + [dma((n_blk,))] * 10,
            compiler_params=pltpu.CompilerParams(collective_id=1, has_side_effects=True, vmem_limit_bytes=29 << 20),
            name="combine",
        )(pin(h), pin(s), pin(o_on), wd)

    return jax.shard_map(local_step, mesh=mesh, in_specs=(row_spec, row_spec, row_spec, expert_spec, expert_spec, expert_spec), out_specs=row_spec, check_vma=False)
```

```python
import jax
import jax.numpy as jnp
from jax import lax
from jax.experimental import pallas as pl
from jax.experimental.pallas import tpu as pltpu
from jax.sharding import PartitionSpec as P

BF16 = jnp.bfloat16
F32 = jnp.float32
MESH = pl.DeviceIdType.MESH
N_DEV = 8
CAP = 32
SLOTS = 4
EARLY = 3
FRONT = 6
LAG_3 = 3
LAG_4 = 6
LIMIT = 4 << 20
COLS = 256
VMEM = pl.BlockSpec(memory_space=pltpu.VMEM)
ANY = pl.BlockSpec(memory_space=pl.ANY)


def remote(src, dst, send_sem, recv_sem, peer):
    return pltpu.make_async_remote_copy(src_ref=src, dst_ref=dst, send_sem=send_sem, recv_sem=recv_sem, device_id={"ep": peer}, device_id_type=MESH)


def on_chip(shape, dtype):
    return pltpu.VMEM(shape, dtype)


def pin(v):
    return pltpu.with_memory_space_constraint(v, pltpu.VMEM)


def place():
    me = lax.axis_index("ep")
    core = lax.rem(me, 2)
    x = lax.rem(me // 2, 2)
    y = me // 4
    return me, core, x, y, me + 1 - 2 * core, me + 2 - 4 * x, me + 4 - 8 * y


def entry_barrier(me):
    barrier = pltpu.get_barrier_semaphore()
    for d in range(1, N_DEV):
        pl.semaphore_signal(barrier, inc=1, device_id={"ep": lax.rem(me + d, N_DEV)}, device_id_type=MESH)
    pl.semaphore_wait(barrier, N_DEV - 1)


def gather_kernel(tok, route_t, gate_t, wg, wu, w_out, x_out, codes_out, h_out, s_out, wd_out, pad_i, pad_g, pad, sg_loc, sg, w_sem, in_sem, sib_s, sib_r, link_s, link_r, sg_s, sg_r):
    me, core, x, y, sib, xn, yn = place()
    n_tok = tok.shape[0]
    half = n_tok // 2

    def rows(device, part=0, count=half):
        return x_out.at[pl.ds(pl.multiple_of(device * n_tok + part * half, half), count)]

    own = pltpu.make_async_copy(tok, rows(me, 0, n_tok), in_sem.at[0])
    own_route = pltpu.make_async_copy(route_t, pad_i, in_sem.at[1])
    own_gate = pltpu.make_async_copy(gate_t, pad_g, in_sem.at[2])
    own.start()
    own_route.start()
    own_gate.start()
    barrier = pltpu.get_barrier_semaphore()
    for d in range(1, N_DEV):
        pl.semaphore_signal(barrier, inc=1, device_id={"ep": lax.rem(me + d, N_DEV)}, device_id_type=MESH)
    loads = []
    for e in range(EARLY):
        loads.append(pltpu.make_async_copy(wg.at[e], w_out.at[e, 0], w_sem.at[e, 0]))
        loads.append(pltpu.make_async_copy(wu.at[e], w_out.at[e, 1], w_sem.at[e, 1]))
    loads.append(pltpu.make_async_copy(wg.at[EARLY], w_out.at[EARLY, 0], w_sem.at[EARLY, 0]))
    for load in loads:
        load.start()

    pad[...] = jnp.zeros_like(pad)
    own_route.wait()
    pad[0, 0:6, 0:n_tok] = pad_i[...].astype(F32)
    own_gate.wait()
    pad[1, 0:6, 0:n_tok] = pad_g[...]
    routes = pad[0] + pltpu.roll(pad[0], n_tok, 1)
    gates = pad[1] + pltpu.roll(pad[1], n_tok, 1)
    expert = lax.broadcasted_iota(jnp.int32, (64, 128), 0).astype(F32)
    lane = lax.broadcasted_iota(jnp.int32, (64, 128), 1)
    mine = (lane // n_tok) == core
    member = jnp.zeros((64, 128), F32)
    weight = jnp.zeros((64, 128), F32)
    for k in range(6):
        hit = (expert == routes[k : k + 1, :]) & mine
        member = jnp.where(hit, 1.0, member)
        weight = jnp.where(hit, gates[k : k + 1, :], weight)
    row = lax.broadcasted_iota(jnp.int32, (128, 128), 0)
    col = lax.broadcasted_iota(jnp.int32, (128, 128), 1)
    upto = jnp.where((row <= col), 1.0, 0.0).astype(BF16)
    rank = jnp.dot(member.astype(BF16), upto, preferred_element_type=F32)
    code = jnp.where(member > 0.5, rank + (me * CAP).astype(F32), 0.0)
    sg_loc[:, 0:8, :] = code.reshape(8, 8, 128)
    sg_loc[:, 8:16, :] = weight.reshape(8, 8, 128)
    sg[me] = sg_loc[me]
    pl.semaphore_wait(barrier, N_DEV - 1)

    sg_copies = []
    for d in range(1, N_DEV):
        peer = lax.rem(me + d, N_DEV)
        sg_copies.append(remote(sg_loc.at[peer], sg.at[me], sg_s.at[d], sg_r.at[d], peer))
    for copy in sg_copies:
        copy.start()
    to_x_a = remote(rows(me, 0), rows(me, 0), link_s.at[0], link_r.at[0], xn)
    to_x_b = remote(rows(me, 1), rows(me, 1), link_s.at[1], link_r.at[1], xn)
    to_y_b = remote(rows(me, 1), rows(me, 1), link_s.at[2], link_r.at[2], yn)
    to_y_a = remote(rows(me, 0), rows(me, 0), link_s.at[3], link_r.at[3], yn)
    to_sib = remote(rows(me, 0, n_tok), rows(me, 0, n_tok), sib_s.at[0], sib_r.at[0], sib)
    own.wait()
    for copy in (to_x_a, to_y_b, to_x_b, to_y_a, to_sib):
        copy.start()
    dg = lax.rem(xn + 4, N_DEV)
    passed = []

    def pass_on(index, source, part):
        copy = remote(rows(source, part), rows(source, part), sib_s.at[index], sib_r.at[index], sib)
        copy.start()
        passed.append(copy)

    to_x_a.wait_recv()
    via_y = remote(rows(xn, 0), rows(xn, 0), link_s.at[4], link_r.at[4], yn)
    via_y.start()
    pass_on(1, xn, 0)
    to_y_b.wait_recv()
    via_x = remote(rows(yn, 1), rows(yn, 1), link_s.at[5], link_r.at[5], xn)
    via_x.start()
    pass_on(2, yn, 1)
    for copy in sg_copies:
        copy.wait()

    r = lax.broadcasted_iota(jnp.int32, (256, 128), 0)
    lane = lax.broadcasted_iota(jnp.int32, (256, 128), 1)
    for p in range(4):
        target = ((2 * p + lane // 64) * CAP + lax.rem(r, CAP) + 1).astype(F32)
        code = sg[2 * p, 0:8, :] + sg[2 * p + 1, 0:8, :]
        gate = sg[2 * p, 8:16, :] + sg[2 * p + 1, 8:16, :]
        codes_out[:, pl.ds(p * 128, 128)] = code
        code = jnp.broadcast_to(code[:, None, :], (8, CAP, 128)).reshape(256, 128)
        gate = jnp.broadcast_to(gate[:, None, :], (8, CAP, 128)).reshape(256, 128)
        s_t = jnp.where(code == target, gate, 0.0)
        s_f = s_t.T
        hi = jnp.minimum(s_f, 3.3895e38).astype(BF16)
        rest = s_f - hi.astype(F32)
        mid = rest.astype(BF16)
        low = (rest - mid.astype(F32)).astype(BF16)
        s_out[p, 0] = hi
        s_out[p, 1] = mid
        s_out[p, 2] = low

    to_x_b.wait_recv()
    pass_on(3, xn, 1)
    to_y_a.wait_recv()
    pass_on(4, yn, 0)
    via_y.wait_recv()
    pass_on(5, dg, 0)
    via_x.wait_recv()
    pass_on(6, dg, 1)
    for copy in (to_x_a, to_x_b, to_y_b, to_y_a, via_y, via_x):
        copy.wait_send()
    to_sib.wait()
    for copy in passed:
        copy.wait()
    for load in loads:
        load.wait()


def hidden_kernel(w_in, h_in, wd_in, x_all, codes, wg, wu, wd, w_buf, h_out, wd_out, xe, order, w_sem, d_sem):
    n_exp = wg.shape[0]
    d_ff = wg.shape[2]

    def load(n, e, part, src):
        s = lax.rem(n, SLOTS)
        return pltpu.make_async_copy(src.at[e], w_buf.at[s, part], w_sem.at[s, part])

    load(EARLY, EARLY, 1, wu).start()
    down = pltpu.make_async_copy(wd.at[:, :, pl.ds(0, COLS)], wd_out, d_sem)

    def hidden_rows(e, cap, slot):
        m = cap * N_DEV
        r = lax.broadcasted_iota(jnp.int32, (m, 512), 0)
        target = ((r // cap) * CAP + lax.rem(r, cap) + 1).astype(F32)
        pick = (target == codes[pl.ds(e, 1), :]).astype(BF16)
        for c in range(0, x_all.shape[1], 512):
            part = jnp.dot(pick, x_all[:, pl.ds(c, 512)], preferred_element_type=F32)
            xe[pl.ds(0, m), pl.ds(c, 512)] = part.astype(BF16)

        def put(act, c, w):
            if cap == CAP:
                h_out[e, :, pl.ds(c, w)] = act
            else:
                for i in range(N_DEV):
                    h_out[e, pl.ds(i * CAP, cap), pl.ds(c, w)] = act[i * cap : (i + 1) * cap]
                    h_out[e, pl.ds(i * CAP + cap, CAP - cap), pl.ds(c, w)] = jnp.zeros((CAP - cap, w), BF16)

        def act_of(a, b):
            return (a * jax.nn.sigmoid(a) * b).astype(BF16)

        rows = xe[pl.ds(0, m), :]
        for c in range(0, d_ff - 128, 256):
            a = jnp.dot(rows, w_buf[slot, 0, :, pl.ds(c, 256)], preferred_element_type=F32)
            b = jnp.dot(rows, w_buf[slot, 1, :, pl.ds(c, 256)], preferred_element_type=F32)
            put(act_of(a, b), c, 256)
        c = d_ff - 128
        both = jnp.concatenate([w_buf[slot, 0, :, pl.ds(c, 128)], w_buf[slot, 1, :, pl.ds(c, 128)]], axis=1)
        ab = jnp.dot(rows, both, preferred_element_type=F32)
        put(act_of(ab[:, :128], ab[:, 128:]), c, 128)

    block = lax.broadcasted_iota(jnp.int32, (1, 512), 1) // 64

    def few(e):
        return jnp.max(codes[pl.ds(e, 1), :] - (block * CAP).astype(F32)) <= 16.0

    for e in range(SLOTS):
        order[e] = e
    small_of = [few(e).astype(jnp.int32) for e in range(SLOTS, n_exp)]
    n_large = len(small_of) - sum(small_of)
    large_seen, small_seen = jnp.int32(0), n_large
    for e, is_small in enumerate(small_of):
        order[SLOTS + jnp.where(is_small == 1, small_seen, large_seen)] = e + SLOTS
        small_seen = small_seen + is_small
        large_seen = large_seen + 1 - is_small

    def step(n, carry):
        e = order[n]
        slot = lax.rem(n, SLOTS)

        @pl.when(n > EARLY)
        def _():
            load(n, e, 0, wg).wait()

        @pl.when(n >= EARLY)
        def _():
            load(n, e, 1, wu).wait()

        small = few(e)

        @pl.when(small)
        def _():
            hidden_rows(e, CAP // 2, slot)

        @pl.when(jnp.logical_not(small))
        def _():
            hidden_rows(e, CAP, slot)

        @pl.when(n + SLOTS < n_exp)
        def _():
            following = order[jnp.minimum(n + SLOTS, n_exp - 1)]
            load(n + SLOTS, following, 0, wg).start()
            load(n + SLOTS, following, 1, wu).start()

        @pl.when(n + SLOTS == n_exp)
        def _():
            down.start()

        return carry

    lax.fori_loop(0, n_exp, step, 0)
    down.wait()


def combine_kernel(h, s, wd_on, wd, y_out, wd_buf, o, part, d2d, h1a, h1b, h2a, h2b, w_sem, ds, dr, h1as, h1ar, h1bs, h1br, h2as, h2ar, h2bs, h2br):
    me, core, x, y, sib, xn, yn = place()
    n_blk = wd.shape[2] // COLS
    n_buf = wd_buf.shape[0]
    n_exp = h.shape[0]
    half = 32
    first, second = pl.ds(0, half), pl.ds(half, half)

    def load(b):
        slot = lax.rem(b - 1, n_buf)
        return pltpu.make_async_copy(wd.at[:, :, pl.ds(pl.multiple_of(b * COLS, COLS), COLS)], wd_buf.at[slot], w_sem.at[slot])

    load(1).start()
    barrier = pltpu.get_barrier_semaphore()
    for d in range(1, N_DEV):
        pl.semaphore_signal(barrier, inc=1, device_id={"ep": lax.rem(me + d, N_DEV)}, device_id_type=MESH)

    def send_d2d(b):
        return remote(part.at[b, 1 - core], d2d.at[b], ds.at[b], dr.at[b], sib)

    def send_1a(b):
        return remote(part.at[b, core, :, 1 - x, first], h1a.at[b], h1as.at[b], h1ar.at[b], xn)

    def send_1b(b):
        return remote(part.at[b, core, 1 - y, :, second], h1b.at[b], h1bs.at[b], h1br.at[b], yn)

    def send_2a(b):
        return remote(part.at[b, core, 1 - y, x, first], h2a.at[b], h2as.at[b], h2ar.at[b], yn)

    def send_2b(b):
        return remote(part.at[b, core, y, 1 - x, second], h2b.at[b], h2bs.at[b], h2br.at[b], xn)

    def lag(b, k, body):
        @pl.when((b >= k) & (b < n_blk + k))
        def _():
            body(b - k)

    def stage_1(b):
        send_d2d(b).start()

    def stage_2(b):
        send_d2d(b).wait_recv()
        part[b, core] += d2d[b]
        send_1a(b).start()
        send_1b(b).start()

    def stage_3(b):
        send_1a(b).wait_recv()
        send_1b(b).wait_recv()
        part[b, core, :, x, first] += h1a[b]
        part[b, core, y, :, second] += h1b[b]
        send_2a(b).start()
        send_2b(b).start()

    def stage_4(b):
        send_2a(b).wait_recv()
        send_2b(b).wait_recv()
        cols = pl.ds(pl.multiple_of(b * COLS, COLS), COLS)
        y_out[first, cols] = (part[b, core, y, x, first] + h2a[b]).astype(BF16)
        y_out[second, cols] = (part[b, core, y, x, second] + h2b[b]).astype(BF16)

    def down(e, weights):
        out = jnp.dot(h[e], weights[e], preferred_element_type=F32).astype(BF16)
        for i in range(N_DEV):
            o[i, pl.ds(e * CAP, CAP), :] = out[i * CAP : (i + 1) * CAP]

    def front(b, weights):
        for e in range(FRONT):
            down(e, weights)

        @pl.when(b + 2 < n_blk)
        def _():
            load(b + 2).start()

    def back(b, weights):
        for e in range(FRONT, n_exp):
            down(e, weights)
        for i in range(N_DEV):
            gates = s[i // 2, :, pl.ds((i % 2) * 64, 64), :].reshape(192, 256)
            terms = jnp.dot(gates, o[i], preferred_element_type=F32)
            part[b, i % 2, i // 4, (i // 2) % 2] = terms[0:64] + terms[64:128] + terms[128:192]

    front(0, wd_on)
    back(0, wd_on)
    pl.semaphore_wait(barrier, N_DEV - 1)

    def step(b, carry):
        lag(b, 1, stage_1)
        weights = wd_buf.at[lax.rem(b - 1, n_buf)]

        @pl.when(b < n_blk)
        def _():
            load(b).wait()
            front(b, weights)

        lag(b, 1, stage_2)
        lag(b, LAG_3, stage_3)
        lag(b, LAG_4, stage_4)

        @pl.when(b < n_blk)
        def _():
            back(b, weights)

        return carry

    lax.fori_loop(1, n_blk + LAG_4, step, 0)

    def drain(b, carry):
        for send in (send_d2d, send_1a, send_1b, send_2a, send_2b):
            send(b).wait_send()
        return carry

    lax.fori_loop(0, n_blk, drain, 0)


def solution(mesh):
    row_spec = P(("dp", "ep"))
    expert_spec = P("ep")
    dma = pltpu.SemaphoreType.DMA

    def local_step(tok, route, gate, wg, wu, wd):
        n_exp, d_model, d_ff = wg.shape
        n_tok = tok.shape[0]
        n_blk = d_model // COLS
        hidden = (n_exp, N_DEV * CAP, d_ff)
        w_on, x_all, codes, h, s, wd_on = pl.pallas_call(
            gather_kernel,
            out_shape=[on_chip((SLOTS, 2, d_model, d_ff), BF16), on_chip((N_DEV * n_tok, d_model), BF16), on_chip((8, 512), F32), on_chip(hidden, BF16), on_chip((4, 3, 128, 256), BF16), on_chip((n_exp, d_ff, COLS), BF16)],
            in_specs=[ANY] * 5,
            out_specs=[VMEM] * 6,
            scratch_shapes=[
                pltpu.VMEM((6, n_tok), jnp.int32),
                pltpu.VMEM((6, n_tok), F32),
                pltpu.VMEM((2, 8, 128), F32),
                pltpu.VMEM((N_DEV, 16, 128), F32),
                pltpu.VMEM((N_DEV, 16, 128), F32),
                dma((SLOTS, 2)),
                dma((3,)),
                dma((7,)),
                dma((7,)),
                dma((6,)),
                dma((6,)),
                dma((N_DEV,)),
                dma((N_DEV,)),
            ],
            compiler_params=pltpu.CompilerParams(collective_id=0, has_side_effects=True, vmem_limit_bytes=LIMIT),
            name="gather",
        )(tok, route.T, gate.T, wg, wu)
        unused, h, wd_on = pl.pallas_call(
            hidden_kernel,
            out_shape=[on_chip(w_on.shape, BF16), on_chip(hidden, BF16), on_chip(wd_on.shape, BF16)],
            in_specs=[VMEM] * 5 + [ANY] * 3,
            out_specs=[VMEM] * 3,
            scratch_shapes=[pltpu.VMEM((256, d_model), BF16), pltpu.SMEM((n_exp,), jnp.int32), dma((SLOTS, 2)), dma],
            input_output_aliases={0: 0, 1: 1, 2: 2},
            compiler_params=pltpu.CompilerParams(vmem_limit_bytes=LIMIT),
            name="hidden",
        )(pin(w_on), pin(h), pin(wd_on), pin(x_all), pin(codes), wg, wu, wd)
        return pl.pallas_call(
            combine_kernel,
            out_shape=jax.ShapeDtypeStruct((n_tok, d_model), BF16),
            in_specs=[VMEM] * 3 + [ANY],
            out_specs=VMEM,
            scratch_shapes=[
                pltpu.VMEM((3, n_exp, d_ff, COLS), BF16),
                pltpu.VMEM((N_DEV, 256, COLS), BF16),
                pltpu.VMEM((n_blk, 2, 2, 2, n_tok, COLS), F32),
                pltpu.VMEM((n_blk, 2, 2, n_tok, COLS), F32),
                pltpu.VMEM((n_blk, 2, n_tok // 2, COLS), F32),
                pltpu.VMEM((n_blk, 2, n_tok // 2, COLS), F32),
                pltpu.VMEM((n_blk, n_tok // 2, COLS), F32),
                pltpu.VMEM((n_blk, n_tok // 2, COLS), F32),
                dma((3,)),
            ]
            + [dma((n_blk,))] * 10,
            compiler_params=pltpu.CompilerParams(collective_id=1, has_side_effects=True, vmem_limit_bytes=32 << 20),
            name="combine",
        )(pin(h), pin(s), pin(wd_on), wd)

    return jax.shard_map(local_step, mesh=mesh, in_specs=(row_spec, row_spec, row_spec, expert_spec, expert_spec, expert_spec), out_specs=row_spec, check_vma=False)
```

```python
import jax
import jax.numpy as jnp
from jax import lax
from jax.experimental import pallas as pl
from jax.experimental.pallas import tpu as pltpu
from jax.sharding import PartitionSpec as P

BF16 = jnp.bfloat16
F32 = jnp.float32
MESH = pl.DeviceIdType.MESH
N_DEV = 8
CAP = 32
SLOTS = 4
EARLY = 3
FRONT = 2
LAG_3 = 3
LAG_4 = 6
LIMIT = 4 << 20
COLS = 256
VMEM = pl.BlockSpec(memory_space=pltpu.VMEM)
ANY = pl.BlockSpec(memory_space=pl.ANY)


def remote(src, dst, send_sem, recv_sem, peer):
    return pltpu.make_async_remote_copy(src_ref=src, dst_ref=dst, send_sem=send_sem, recv_sem=recv_sem, device_id={"ep": peer}, device_id_type=MESH)


def on_chip(shape, dtype):
    return pltpu.VMEM(shape, dtype)


def pin(v):
    return pltpu.with_memory_space_constraint(v, pltpu.VMEM)


def place():
    me = lax.axis_index("ep")
    core = lax.rem(me, 2)
    x = lax.rem(me // 2, 2)
    y = me // 4
    return me, core, x, y, me + 1 - 2 * core, me + 2 - 4 * x, me + 4 - 8 * y


def entry_barrier(me):
    barrier = pltpu.get_barrier_semaphore()
    for d in range(1, N_DEV):
        pl.semaphore_signal(barrier, inc=1, device_id={"ep": lax.rem(me + d, N_DEV)}, device_id_type=MESH)
    pl.semaphore_wait(barrier, N_DEV - 1)


def gather_kernel(tok, route_t, gate_t, wg, wu, w_out, x_out, codes_out, h_out, s_out, wd_out, pad_i, pad_g, pad, sg_loc, sg, w_sem, in_sem, sib_s, sib_r, link_s, link_r, sg_s, sg_r):
    me, core, x, y, sib, xn, yn = place()
    n_tok = tok.shape[0]
    half = n_tok // 2

    def rows(device, part=0, count=half):
        return x_out.at[pl.ds(pl.multiple_of(device * n_tok + part * half, half), count)]

    own = pltpu.make_async_copy(tok, rows(me, 0, n_tok), in_sem.at[0])
    own_route = pltpu.make_async_copy(route_t, pad_i, in_sem.at[1])
    own_gate = pltpu.make_async_copy(gate_t, pad_g, in_sem.at[2])
    own.start()
    own_route.start()
    own_gate.start()
    barrier = pltpu.get_barrier_semaphore()
    for d in range(1, N_DEV):
        pl.semaphore_signal(barrier, inc=1, device_id={"ep": lax.rem(me + d, N_DEV)}, device_id_type=MESH)
    loads = []
    for e in range(EARLY):
        loads.append(pltpu.make_async_copy(wg.at[e], w_out.at[e, 0], w_sem.at[e, 0]))
        loads.append(pltpu.make_async_copy(wu.at[e], w_out.at[e, 1], w_sem.at[e, 1]))
    loads.append(pltpu.make_async_copy(wg.at[EARLY], w_out.at[EARLY, 0], w_sem.at[EARLY, 0]))
    for load in loads:
        load.start()

    pad[...] = jnp.zeros_like(pad)
    own_route.wait()
    pad[0, 0:6, 0:n_tok] = pad_i[...].astype(F32)
    own_gate.wait()
    pad[1, 0:6, 0:n_tok] = pad_g[...]
    routes = pad[0] + pltpu.roll(pad[0], n_tok, 1)
    gates = pad[1] + pltpu.roll(pad[1], n_tok, 1)
    expert = lax.broadcasted_iota(jnp.int32, (64, 128), 0).astype(F32)
    lane = lax.broadcasted_iota(jnp.int32, (64, 128), 1)
    mine = (lane // n_tok) == core
    member = jnp.zeros((64, 128), F32)
    weight = jnp.zeros((64, 128), F32)
    for k in range(6):
        hit = (expert == routes[k : k + 1, :]) & mine
        member = jnp.where(hit, 1.0, member)
        weight = jnp.where(hit, gates[k : k + 1, :], weight)
    row = lax.broadcasted_iota(jnp.int32, (128, 128), 0)
    col = lax.broadcasted_iota(jnp.int32, (128, 128), 1)
    upto = jnp.where((row <= col), 1.0, 0.0).astype(BF16)
    rank = jnp.dot(member.astype(BF16), upto, preferred_element_type=F32)
    code = jnp.where(member > 0.5, rank + (me * CAP).astype(F32), 0.0)
    sg_loc[:, 0:8, :] = code.reshape(8, 8, 128)
    sg_loc[:, 8:16, :] = weight.reshape(8, 8, 128)
    sg[me] = sg_loc[me]
    pl.semaphore_wait(barrier, N_DEV - 1)

    sg_copies = []
    for d in range(1, N_DEV):
        peer = lax.rem(me + d, N_DEV)
        sg_copies.append(remote(sg_loc.at[peer], sg.at[me], sg_s.at[d], sg_r.at[d], peer))
    for copy in sg_copies:
        copy.start()
    to_x_a = remote(rows(me, 0), rows(me, 0), link_s.at[0], link_r.at[0], xn)
    to_x_b = remote(rows(me, 1), rows(me, 1), link_s.at[1], link_r.at[1], xn)
    to_y_b = remote(rows(me, 1), rows(me, 1), link_s.at[2], link_r.at[2], yn)
    to_y_a = remote(rows(me, 0), rows(me, 0), link_s.at[3], link_r.at[3], yn)
    to_sib = remote(rows(me, 0, n_tok), rows(me, 0, n_tok), sib_s.at[0], sib_r.at[0], sib)
    own.wait()
    for copy in (to_x_a, to_y_b, to_x_b, to_y_a, to_sib):
        copy.start()
    dg = lax.rem(xn + 4, N_DEV)
    passed = []

    def pass_on(index, source, part):
        copy = remote(rows(source, part), rows(source, part), sib_s.at[index], sib_r.at[index], sib)
        copy.start()
        passed.append(copy)

    to_x_a.wait_recv()
    via_y = remote(rows(xn, 0), rows(xn, 0), link_s.at[4], link_r.at[4], yn)
    via_y.start()
    pass_on(1, xn, 0)
    to_y_b.wait_recv()
    via_x = remote(rows(yn, 1), rows(yn, 1), link_s.at[5], link_r.at[5], xn)
    via_x.start()
    pass_on(2, yn, 1)
    for copy in sg_copies:
        copy.wait()

    r = lax.broadcasted_iota(jnp.int32, (256, 128), 0)
    lane = lax.broadcasted_iota(jnp.int32, (256, 128), 1)
    for p in range(4):
        target = ((2 * p + lane // 64) * CAP + lax.rem(r, CAP) + 1).astype(F32)
        code = sg[2 * p, 0:8, :] + sg[2 * p + 1, 0:8, :]
        gate = sg[2 * p, 8:16, :] + sg[2 * p + 1, 8:16, :]
        codes_out[:, pl.ds(p * 128, 128)] = code
        code = jnp.broadcast_to(code[:, None, :], (8, CAP, 128)).reshape(256, 128)
        gate = jnp.broadcast_to(gate[:, None, :], (8, CAP, 128)).reshape(256, 128)
        s_t = jnp.where(code == target, gate, 0.0)
        s_f = s_t.T
        hi = jnp.minimum(s_f, 3.3895e38).astype(BF16)
        rest = s_f - hi.astype(F32)
        mid = rest.astype(BF16)
        low = (rest - mid.astype(F32)).astype(BF16)
        s_out[p, 0] = hi
        s_out[p, 1] = mid
        s_out[p, 2] = low

    to_x_b.wait_recv()
    pass_on(3, xn, 1)
    to_y_a.wait_recv()
    pass_on(4, yn, 0)
    via_y.wait_recv()
    pass_on(5, dg, 0)
    via_x.wait_recv()
    pass_on(6, dg, 1)
    for copy in (to_x_a, to_x_b, to_y_b, to_y_a, via_y, via_x):
        copy.wait_send()
    to_sib.wait()
    for copy in passed:
        copy.wait()
    for load in loads:
        load.wait()


def hidden_kernel(w_in, h_in, wd_in, x_all, codes, wg, wu, wd, w_buf, h_out, wd_out, xe, order, w_sem, d_sem):
    n_exp = wg.shape[0]
    d_ff = wg.shape[2]

    def load(n, e, part, src):
        s = lax.rem(n, SLOTS)
        return pltpu.make_async_copy(src.at[e], w_buf.at[s, part], w_sem.at[s, part])

    load(EARLY, EARLY, 1, wu).start()
    down = pltpu.make_async_copy(wd.at[:, :, pl.ds(0, COLS)], wd_out, d_sem)

    def hidden_rows(e, cap, slot):
        m = cap * N_DEV
        r = lax.broadcasted_iota(jnp.int32, (m, 512), 0)
        target = ((r // cap) * CAP + lax.rem(r, cap) + 1).astype(F32)
        pick = (target == codes[pl.ds(e, 1), :]).astype(BF16)
        for c in range(0, x_all.shape[1], 512):
            part = jnp.dot(pick, x_all[:, pl.ds(c, 512)], preferred_element_type=F32)
            xe[pl.ds(0, m), pl.ds(c, 512)] = part.astype(BF16)

        def put(act, c, w):
            if cap == CAP:
                h_out[e, :, pl.ds(c, w)] = act
            else:
                for i in range(N_DEV):
                    h_out[e, pl.ds(i * CAP, cap), pl.ds(c, w)] = act[i * cap : (i + 1) * cap]
                    h_out[e, pl.ds(i * CAP + cap, CAP - cap), pl.ds(c, w)] = jnp.zeros((CAP - cap, w), BF16)

        def act_of(a, b):
            return (a * jax.nn.sigmoid(a) * b).astype(BF16)

        rows = xe[pl.ds(0, m), :]
        for c in range(0, d_ff - 128, 256):
            a = jnp.dot(rows, w_buf[slot, 0, :, pl.ds(c, 256)], preferred_element_type=F32)
            b = jnp.dot(rows, w_buf[slot, 1, :, pl.ds(c, 256)], preferred_element_type=F32)
            put(act_of(a, b), c, 256)
        c = d_ff - 128
        both = jnp.concatenate([w_buf[slot, 0, :, pl.ds(c, 128)], w_buf[slot, 1, :, pl.ds(c, 128)]], axis=1)
        ab = jnp.dot(rows, both, preferred_element_type=F32)
        put(act_of(ab[:, :128], ab[:, 128:]), c, 128)

    block = lax.broadcasted_iota(jnp.int32, (1, 512), 1) // 64

    def few(e):
        return jnp.max(codes[pl.ds(e, 1), :] - (block * CAP).astype(F32)) <= 16.0

    for e in range(SLOTS):
        order[e] = e
    small_of = [few(e).astype(jnp.int32) for e in range(SLOTS, n_exp)]
    n_large = len(small_of) - sum(small_of)
    large_seen, small_seen = jnp.int32(0), n_large
    for e, is_small in enumerate(small_of):
        order[SLOTS + jnp.where(is_small == 1, small_seen, large_seen)] = e + SLOTS
        small_seen = small_seen + is_small
        large_seen = large_seen + 1 - is_small

    def step(n, carry):
        e = order[n]
        slot = lax.rem(n, SLOTS)

        @pl.when(n > EARLY)
        def _():
            load(n, e, 0, wg).wait()

        @pl.when(n >= EARLY)
        def _():
            load(n, e, 1, wu).wait()

        small = few(e)

        @pl.when(small)
        def _():
            hidden_rows(e, CAP // 2, slot)

        @pl.when(jnp.logical_not(small))
        def _():
            hidden_rows(e, CAP, slot)

        @pl.when(n + SLOTS < n_exp)
        def _():
            following = order[jnp.minimum(n + SLOTS, n_exp - 1)]
            load(n + SLOTS, following, 0, wg).start()
            load(n + SLOTS, following, 1, wu).start()

        @pl.when(n + SLOTS == n_exp)
        def _():
            down.start()

        return carry

    lax.fori_loop(0, n_exp, step, 0)
    down.wait()


def combine_kernel(h, s, wd_on, wd, y_out, wd_buf, o, part, d2d, h1a, h1b, h2a, h2b, w_sem, ds, dr, h1as, h1ar, h1bs, h1br, h2as, h2ar, h2bs, h2br):
    me, core, x, y, sib, xn, yn = place()
    n_blk = wd.shape[2] // COLS
    n_buf = wd_buf.shape[0]
    n_exp = h.shape[0]
    half = 32
    first, second = pl.ds(0, half), pl.ds(half, half)

    def load(b):
        slot = (b - 1) % n_buf
        return pltpu.make_async_copy(wd.at[:, :, pl.ds(b * COLS, COLS)], wd_buf.at[slot], w_sem.at[slot])

    load(1).start()
    barrier = pltpu.get_barrier_semaphore()
    for d in range(1, N_DEV):
        pl.semaphore_signal(barrier, inc=1, device_id={"ep": lax.rem(me + d, N_DEV)}, device_id_type=MESH)

    def send_d2d(b):
        return remote(part.at[b, 1 - core], d2d.at[b], ds.at[b], dr.at[b], sib)

    def send_1a(b):
        return remote(part.at[b, core, :, 1 - x, first], h1a.at[b], h1as.at[b], h1ar.at[b], xn)

    def send_1b(b):
        return remote(part.at[b, core, 1 - y, :, second], h1b.at[b], h1bs.at[b], h1br.at[b], yn)

    def send_2a(b):
        return remote(part.at[b, core, 1 - y, x, first], h2a.at[b], h2as.at[b], h2ar.at[b], yn)

    def send_2b(b):
        return remote(part.at[b, core, y, 1 - x, second], h2b.at[b], h2bs.at[b], h2br.at[b], xn)

    def stage_1(b):
        send_d2d(b).start()

    def stage_2(b):
        send_d2d(b).wait_recv()
        part[b, core] += d2d[b]
        send_1a(b).start()
        send_1b(b).start()

    def stage_3(b):
        send_1a(b).wait_recv()
        send_1b(b).wait_recv()
        part[b, core, :, x, first] += h1a[b]
        part[b, core, y, :, second] += h1b[b]
        send_2a(b).start()
        send_2b(b).start()

    def stage_4(b):
        send_2a(b).wait_recv()
        send_2b(b).wait_recv()
        cols = pl.ds(b * COLS, COLS)
        y_out[first, cols] = (part[b, core, y, x, first] + h2a[b]).astype(BF16)
        y_out[second, cols] = (part[b, core, y, x, second] + h2b[b]).astype(BF16)

    def down(b, e, weights):
        out = jnp.dot(h[e], weights[e], preferred_element_type=F32).astype(BF16)
        for i in range(N_DEV):
            o[b % 2, i, pl.ds(e * CAP, CAP), :] = out[i * CAP : (i + 1) * CAP]

    def gather_sum(b):
        for i in range(N_DEV):
            gates = s[i // 2, :, pl.ds((i % 2) * 64, 64), :].reshape(192, 256)
            terms = jnp.dot(gates, o[b % 2, i], preferred_element_type=F32)
            part[b, i % 2, i // 4, (i // 2) % 2] = terms[0:64] + terms[64:128] + terms[128:192]

    def weights_of(b):
        return wd_on if b == 0 else wd_buf.at[(b - 1) % n_buf]

    for b in range(n_blk + LAG_4):
        if b < n_blk:
            if b > 0:
                load(b).wait()
            for e in range(FRONT):
                down(b, e, weights_of(b))
        if 1 <= b < n_blk + 1:
            gather_sum(b - 1)
            if b == 1:
                pl.semaphore_wait(barrier, N_DEV - 1)
            stage_1(b - 1)
        if b < n_blk:
            if b + 2 < n_blk:
                load(b + 2).start()
            for e in range(FRONT, n_exp):
                down(b, e, weights_of(b))
        for k, stage in ((1, stage_2), (LAG_3, stage_3), (LAG_4, stage_4)):
            if k <= b < n_blk + k:
                stage(b - k)

    def drain(b, carry):
        for send in (send_d2d, send_1a, send_1b, send_2a, send_2b):
            send(b).wait_send()
        return carry

    lax.fori_loop(0, n_blk, drain, 0)


def solution(mesh):
    row_spec = P(("dp", "ep"))
    expert_spec = P("ep")
    dma = pltpu.SemaphoreType.DMA

    def local_step(tok, route, gate, wg, wu, wd):
        n_exp, d_model, d_ff = wg.shape
        n_tok = tok.shape[0]
        n_blk = d_model // COLS
        hidden = (n_exp, N_DEV * CAP, d_ff)
        w_on, x_all, codes, h, s, wd_on = pl.pallas_call(
            gather_kernel,
            out_shape=[on_chip((SLOTS, 2, d_model, d_ff), BF16), on_chip((N_DEV * n_tok, d_model), BF16), on_chip((8, 512), F32), on_chip(hidden, BF16), on_chip((4, 3, 128, 256), BF16), on_chip((n_exp, d_ff, COLS), BF16)],
            in_specs=[ANY] * 5,
            out_specs=[VMEM] * 6,
            scratch_shapes=[
                pltpu.VMEM((6, n_tok), jnp.int32),
                pltpu.VMEM((6, n_tok), F32),
                pltpu.VMEM((2, 8, 128), F32),
                pltpu.VMEM((N_DEV, 16, 128), F32),
                pltpu.VMEM((N_DEV, 16, 128), F32),
                dma((SLOTS, 2)),
                dma((3,)),
                dma((7,)),
                dma((7,)),
                dma((6,)),
                dma((6,)),
                dma((N_DEV,)),
                dma((N_DEV,)),
            ],
            compiler_params=pltpu.CompilerParams(collective_id=0, has_side_effects=True, vmem_limit_bytes=LIMIT),
            name="gather",
        )(tok, route.T, gate.T, wg, wu)
        unused, h, wd_on = pl.pallas_call(
            hidden_kernel,
            out_shape=[on_chip(w_on.shape, BF16), on_chip(hidden, BF16), on_chip(wd_on.shape, BF16)],
            in_specs=[VMEM] * 5 + [ANY] * 3,
            out_specs=[VMEM] * 3,
            scratch_shapes=[pltpu.VMEM((256, d_model), BF16), pltpu.SMEM((n_exp,), jnp.int32), dma((SLOTS, 2)), dma],
            input_output_aliases={0: 0, 1: 1, 2: 2},
            compiler_params=pltpu.CompilerParams(vmem_limit_bytes=LIMIT),
            name="hidden",
        )(pin(w_on), pin(h), pin(wd_on), pin(x_all), pin(codes), wg, wu, wd)
        return pl.pallas_call(
            combine_kernel,
            out_shape=jax.ShapeDtypeStruct((n_tok, d_model), BF16),
            in_specs=[VMEM] * 3 + [ANY],
            out_specs=VMEM,
            scratch_shapes=[
                pltpu.VMEM((3, n_exp, d_ff, COLS), BF16),
                pltpu.VMEM((2, N_DEV, 256, COLS), BF16),
                pltpu.VMEM((n_blk, 2, 2, 2, n_tok, COLS), F32),
                pltpu.VMEM((n_blk, 2, 2, n_tok, COLS), F32),
                pltpu.VMEM((n_blk, 2, n_tok // 2, COLS), F32),
                pltpu.VMEM((n_blk, 2, n_tok // 2, COLS), F32),
                pltpu.VMEM((n_blk, n_tok // 2, COLS), F32),
                pltpu.VMEM((n_blk, n_tok // 2, COLS), F32),
                dma((3,)),
            ]
            + [dma((n_blk,))] * 10,
            compiler_params=pltpu.CompilerParams(collective_id=1, has_side_effects=True, vmem_limit_bytes=33 << 20),
            name="combine",
        )(pin(h), pin(s), pin(wd_on), wd)

    return jax.shard_map(local_step, mesh=mesh, in_specs=(row_spec, row_spec, row_spec, expert_spec, expert_spec, expert_spec), out_specs=row_spec, check_vma=False)
```

```python
import jax
import jax.numpy as jnp
from jax import lax
from jax.experimental import pallas as pl
from jax.experimental.pallas import tpu as pltpu
from jax.sharding import PartitionSpec as P

BF16 = jnp.bfloat16
F32 = jnp.float32
MESH = pl.DeviceIdType.MESH
N_DEV = 8
CAP = 32
SLOTS = 4
EARLY = 3
FRONT = 2
LAST = 7
LAG_3 = 3
LAG_4 = 6
LIMIT = 4 << 20
COLS = 256
VMEM = pl.BlockSpec(memory_space=pltpu.VMEM)
ANY = pl.BlockSpec(memory_space=pl.ANY)


def remote(src, dst, send_sem, recv_sem, peer):
    return pltpu.make_async_remote_copy(src_ref=src, dst_ref=dst, send_sem=send_sem, recv_sem=recv_sem, device_id={"ep": peer}, device_id_type=MESH)


def on_chip(shape, dtype):
    return pltpu.VMEM(shape, dtype)


def pin(v):
    return pltpu.with_memory_space_constraint(v, pltpu.VMEM)


def place():
    me = lax.axis_index("ep")
    core = lax.rem(me, 2)
    x = lax.rem(me // 2, 2)
    y = me // 4
    return me, core, x, y, me + 1 - 2 * core, me + 2 - 4 * x, me + 4 - 8 * y


def entry_barrier(me):
    barrier = pltpu.get_barrier_semaphore()
    for d in range(1, N_DEV):
        pl.semaphore_signal(barrier, inc=1, device_id={"ep": lax.rem(me + d, N_DEV)}, device_id_type=MESH)
    pl.semaphore_wait(barrier, N_DEV - 1)


def gather_kernel(tok, route_t, gate_t, wg, wu, w_out, x_out, codes_out, h_out, s_out, wd_out, pad_i, pad_g, pad, sg_loc, sg, w_sem, in_sem, sib_s, sib_r, link_s, link_r, sg_s, sg_r):
    me, core, x, y, sib, xn, yn = place()
    n_tok = tok.shape[0]
    half = n_tok // 2

    def rows(device, part=0, count=half):
        return x_out.at[pl.ds(pl.multiple_of(device * n_tok + part * half, half), count)]

    own = pltpu.make_async_copy(tok, rows(me, 0, n_tok), in_sem.at[0])
    own_route = pltpu.make_async_copy(route_t, pad_i, in_sem.at[1])
    own_gate = pltpu.make_async_copy(gate_t, pad_g, in_sem.at[2])
    own.start()
    own_route.start()
    own_gate.start()
    barrier = pltpu.get_barrier_semaphore()
    for d in range(1, N_DEV):
        pl.semaphore_signal(barrier, inc=1, device_id={"ep": lax.rem(me + d, N_DEV)}, device_id_type=MESH)
    loads = []
    for e in range(EARLY):
        loads.append(pltpu.make_async_copy(wg.at[e], w_out.at[e, 0], w_sem.at[e, 0]))
        loads.append(pltpu.make_async_copy(wu.at[e], w_out.at[e, 1], w_sem.at[e, 1]))
    loads.append(pltpu.make_async_copy(wg.at[EARLY], w_out.at[EARLY, 0], w_sem.at[EARLY, 0]))
    for load in loads:
        load.start()

    pad[...] = jnp.zeros_like(pad)
    own_route.wait()
    pad[0, 0:6, 0:n_tok] = pad_i[...].astype(F32)
    own_gate.wait()
    pad[1, 0:6, 0:n_tok] = pad_g[...]
    routes = pad[0] + pltpu.roll(pad[0], n_tok, 1)
    gates = pad[1] + pltpu.roll(pad[1], n_tok, 1)
    expert = lax.broadcasted_iota(jnp.int32, (64, 128), 0).astype(F32)
    lane = lax.broadcasted_iota(jnp.int32, (64, 128), 1)
    mine = (lane // n_tok) == core
    member = jnp.zeros((64, 128), F32)
    weight = jnp.zeros((64, 128), F32)
    for k in range(6):
        hit = (expert == routes[k : k + 1, :]) & mine
        member = jnp.where(hit, 1.0, member)
        weight = jnp.where(hit, gates[k : k + 1, :], weight)
    row = lax.broadcasted_iota(jnp.int32, (128, 128), 0)
    col = lax.broadcasted_iota(jnp.int32, (128, 128), 1)
    upto = jnp.where((row <= col), 1.0, 0.0).astype(BF16)
    rank = jnp.dot(member.astype(BF16), upto, preferred_element_type=F32)
    code = jnp.where(member > 0.5, rank + (me * CAP).astype(F32), 0.0)
    sg_loc[:, 0:8, :] = code.reshape(8, 8, 128)
    sg_loc[:, 8:16, :] = weight.reshape(8, 8, 128)
    sg[me] = sg_loc[me]
    pl.semaphore_wait(barrier, N_DEV - 1)

    sg_copies = []
    for d in range(1, N_DEV):
        peer = lax.rem(me + d, N_DEV)
        sg_copies.append(remote(sg_loc.at[peer], sg.at[me], sg_s.at[d], sg_r.at[d], peer))
    for copy in sg_copies:
        copy.start()
    to_x_a = remote(rows(me, 0), rows(me, 0), link_s.at[0], link_r.at[0], xn)
    to_x_b = remote(rows(me, 1), rows(me, 1), link_s.at[1], link_r.at[1], xn)
    to_y_b = remote(rows(me, 1), rows(me, 1), link_s.at[2], link_r.at[2], yn)
    to_y_a = remote(rows(me, 0), rows(me, 0), link_s.at[3], link_r.at[3], yn)
    to_sib = remote(rows(me, 0, n_tok), rows(me, 0, n_tok), sib_s.at[0], sib_r.at[0], sib)
    own.wait()
    for copy in (to_x_a, to_y_b, to_x_b, to_y_a, to_sib):
        copy.start()
    dg = lax.rem(xn + 4, N_DEV)
    passed = []

    def pass_on(index, source, part):
        copy = remote(rows(source, part), rows(source, part), sib_s.at[index], sib_r.at[index], sib)
        copy.start()
        passed.append(copy)

    to_x_a.wait_recv()
    via_y = remote(rows(xn, 0), rows(xn, 0), link_s.at[4], link_r.at[4], yn)
    via_y.start()
    pass_on(1, xn, 0)
    to_y_b.wait_recv()
    via_x = remote(rows(yn, 1), rows(yn, 1), link_s.at[5], link_r.at[5], xn)
    via_x.start()
    pass_on(2, yn, 1)
    for copy in sg_copies:
        copy.wait()

    r = lax.broadcasted_iota(jnp.int32, (256, 128), 0)
    lane = lax.broadcasted_iota(jnp.int32, (256, 128), 1)
    for p in range(4):
        target = ((2 * p + lane // 64) * CAP + lax.rem(r, CAP) + 1).astype(F32)
        code = sg[2 * p, 0:8, :] + sg[2 * p + 1, 0:8, :]
        gate = sg[2 * p, 8:16, :] + sg[2 * p + 1, 8:16, :]
        codes_out[:, pl.ds(p * 128, 128)] = code
        code = jnp.broadcast_to(code[:, None, :], (8, CAP, 128)).reshape(256, 128)
        gate = jnp.broadcast_to(gate[:, None, :], (8, CAP, 128)).reshape(256, 128)
        s_t = jnp.where(code == target, gate, 0.0)
        s_f = s_t.T
        hi = jnp.minimum(s_f, 3.3895e38).astype(BF16)
        rest = s_f - hi.astype(F32)
        mid = rest.astype(BF16)
        low = (rest - mid.astype(F32)).astype(BF16)
        s_out[p, 0] = hi
        s_out[p, 1] = mid
        s_out[p, 2] = low

    to_x_b.wait_recv()
    pass_on(3, xn, 1)
    to_y_a.wait_recv()
    pass_on(4, yn, 0)
    via_y.wait_recv()
    pass_on(5, dg, 0)
    via_x.wait_recv()
    pass_on(6, dg, 1)
    for copy in (to_x_a, to_x_b, to_y_b, to_y_a, via_y, via_x):
        copy.wait_send()
    to_sib.wait()
    for copy in passed:
        copy.wait()
    for load in loads:
        load.wait()


def hidden_kernel(w_in, h_in, wd_in, x_all, codes, wg, wu, wd, w_buf, h_out, wd_out, xe, order, w_sem, d_sem):
    n_exp = wg.shape[0]
    d_ff = wg.shape[2]

    def load(n, e, part, src):
        s = lax.rem(n, SLOTS)
        return pltpu.make_async_copy(src.at[e], w_buf.at[s, part], w_sem.at[s, part])

    load(EARLY, EARLY, 1, wu).start()
    down = pltpu.make_async_copy(wd.at[:, :, pl.ds(0, COLS)], wd_out, d_sem)

    def hidden_rows(e, cap, slot):
        m = cap * N_DEV
        r = lax.broadcasted_iota(jnp.int32, (m, 512), 0)
        target = ((r // cap) * CAP + lax.rem(r, cap) + 1).astype(F32)
        pick = (target == codes[pl.ds(e, 1), :]).astype(BF16)
        for c in range(0, x_all.shape[1], 512):
            part = jnp.dot(pick, x_all[:, pl.ds(c, 512)], preferred_element_type=F32)
            xe[pl.ds(0, m), pl.ds(c, 512)] = part.astype(BF16)

        def put(act, c, w):
            if cap == CAP:
                h_out[e, :, pl.ds(c, w)] = act
            else:
                for i in range(N_DEV):
                    h_out[e, pl.ds(i * CAP, cap), pl.ds(c, w)] = act[i * cap : (i + 1) * cap]
                    h_out[e, pl.ds(i * CAP + cap, CAP - cap), pl.ds(c, w)] = jnp.zeros((CAP - cap, w), BF16)

        def act_of(a, b):
            return (a * jax.nn.sigmoid(a) * b).astype(BF16)

        rows = xe[pl.ds(0, m), :]
        for c in range(0, d_ff - 128, 256):
            a = jnp.dot(rows, w_buf[slot, 0, :, pl.ds(c, 256)], preferred_element_type=F32)
            b = jnp.dot(rows, w_buf[slot, 1, :, pl.ds(c, 256)], preferred_element_type=F32)
            put(act_of(a, b), c, 256)
        c = d_ff - 128
        both = jnp.concatenate([w_buf[slot, 0, :, pl.ds(c, 128)], w_buf[slot, 1, :, pl.ds(c, 128)]], axis=1)
        ab = jnp.dot(rows, both, preferred_element_type=F32)
        put(act_of(ab[:, :128], ab[:, 128:]), c, 128)

    block = lax.broadcasted_iota(jnp.int32, (1, 512), 1) // 64

    def few(e):
        return jnp.max(codes[pl.ds(e, 1), :] - (block * CAP).astype(F32)) <= 16.0

    for e in range(SLOTS):
        order[e] = e
    small_of = [few(e).astype(jnp.int32) for e in range(SLOTS, n_exp)]
    n_large = len(small_of) - sum(small_of)
    large_seen, small_seen = jnp.int32(0), n_large
    for e, is_small in enumerate(small_of):
        order[SLOTS + jnp.where(is_small == 1, small_seen, large_seen)] = e + SLOTS
        small_seen = small_seen + is_small
        large_seen = large_seen + 1 - is_small

    def step(n, carry):
        e = order[n]
        slot = lax.rem(n, SLOTS)

        @pl.when(n > EARLY)
        def _():
            load(n, e, 0, wg).wait()

        @pl.when(n >= EARLY)
        def _():
            load(n, e, 1, wu).wait()

        small = few(e)

        @pl.when(small)
        def _():
            hidden_rows(e, CAP // 2, slot)

        @pl.when(jnp.logical_not(small))
        def _():
            hidden_rows(e, CAP, slot)

        @pl.when(n + SLOTS < n_exp)
        def _():
            following = order[jnp.minimum(n + SLOTS, n_exp - 1)]
            load(n + SLOTS, following, 0, wg).start()
            load(n + SLOTS, following, 1, wu).start()

        @pl.when(n + SLOTS == n_exp)
        def _():
            down.start()

        return carry

    lax.fori_loop(0, n_exp, step, 0)
    down.wait()


def combine_kernel(h, s, wd_on, wd, y_out, wd_buf, o, part, d2d, h1a, h1b, h2a, h2b, w_sem, part_sem, ds, dr, h1as, h1ar, h1bs, h1br, h2as, h2ar, h2bs, h2br):
    me, core, x, y, sib, xn, yn = place()
    n_blk = wd.shape[2] // COLS
    n_buf = wd_buf.shape[0]
    n_exp = h.shape[0]
    half = 32
    first, second = pl.ds(0, half), pl.ds(half, half)

    def load(b):
        slot = (b - 1) % n_buf
        return pltpu.make_async_copy(wd.at[:, :, pl.ds(b * COLS, COLS)], wd_buf.at[slot], w_sem.at[slot])

    def part_load(p):
        some = pl.ds(p * 4, 4)
        return pltpu.make_async_copy(wd.at[some, :, pl.ds(COLS, COLS)], wd_buf.at[0, some], part_sem.at[p])

    part_load(0).start()
    part_load(1).start()
    barrier = pltpu.get_barrier_semaphore()
    for d in range(1, N_DEV):
        pl.semaphore_signal(barrier, inc=1, device_id={"ep": lax.rem(me + d, N_DEV)}, device_id_type=MESH)

    def send_d2d(b):
        return remote(part.at[b, 1 - core], d2d.at[b], ds.at[b], dr.at[b], sib)

    def send_1a(b):
        return remote(part.at[b, core, :, 1 - x, first], h1a.at[b], h1as.at[b], h1ar.at[b], xn)

    def send_1b(b):
        return remote(part.at[b, core, 1 - y, :, second], h1b.at[b], h1bs.at[b], h1br.at[b], yn)

    def send_2a(b):
        return remote(part.at[b, core, 1 - y, x, first], h2a.at[b], h2as.at[b], h2ar.at[b], yn)

    def send_2b(b):
        return remote(part.at[b, core, y, 1 - x, second], h2b.at[b], h2bs.at[b], h2br.at[b], xn)

    def stage_1(b):
        send_d2d(b).start()

    def stage_2(b):
        send_d2d(b).wait_recv()
        part[b, core] += d2d[b]
        send_1a(b).start()
        send_1b(b).start()

    def stage_3(b):
        send_1a(b).wait_recv()
        send_1b(b).wait_recv()
        part[b, core, :, x, first] += h1a[b]
        part[b, core, y, :, second] += h1b[b]
        send_2a(b).start()
        send_2b(b).start()

    def stage_4(b):
        send_2a(b).wait_recv()
        send_2b(b).wait_recv()
        cols = pl.ds(b * COLS, COLS)
        y_out[first, cols] = (part[b, core, y, x, first] + h2a[b]).astype(BF16)
        y_out[second, cols] = (part[b, core, y, x, second] + h2b[b]).astype(BF16)

    def down(b, e, weights):
        out = jnp.dot(h[e], weights[e], preferred_element_type=F32).astype(BF16)
        for i in range(N_DEV):
            o[b % 2, i, pl.ds(e * CAP, CAP), :] = out[i * CAP : (i + 1) * CAP]

    def gather_sum(b):
        for i in range(N_DEV):
            gates = s[i // 2, :, pl.ds((i % 2) * 64, 64), :].reshape(192, 256)
            terms = jnp.dot(gates, o[b % 2, i], preferred_element_type=F32)
            part[b, i % 2, i // 4, (i // 2) % 2] = terms[0:64] + terms[64:128] + terms[128:192]

    def weights_of(b):
        return wd_on if b == 0 else wd_buf.at[(b - 1) % n_buf]

    def dots(b, start, stop):
        for e in range(start, stop):
            down(b, e, weights_of(b))

    for b in range(n_blk + LAG_4):
        if b == 1:
            part_load(0).wait()
        elif 1 < b < n_blk:
            load(b).wait()
        if b < n_blk:
            dots(b, 0, FRONT)
        if 2 <= b < n_blk + 1:
            gather_sum(b - 1)
            stage_1(b - 1)
        if b == 1:
            load(2).start()
        if 1 <= b and b + 2 < n_blk:
            load(b + 2).start()
        if b == 1:
            dots(b, FRONT, 4)
            part_load(1).wait()
            dots(b, 4, LAST)
        elif b < n_blk:
            dots(b, FRONT, LAST)
        for k, stage in ((1, stage_2), (LAG_3, stage_3), (LAG_4, stage_4)):
            if k <= b < n_blk + k:
                stage(b - k)
        if b < n_blk:
            dots(b, LAST, n_exp)
        if b == 0:
            gather_sum(0)
            pl.semaphore_wait(barrier, N_DEV - 1)
            stage_1(0)

    def drain(b, carry):
        for send in (send_d2d, send_1a, send_1b, send_2a, send_2b):
            send(b).wait_send()
        return carry

    lax.fori_loop(0, n_blk, drain, 0)


def solution(mesh):
    row_spec = P(("dp", "ep"))
    expert_spec = P("ep")
    dma = pltpu.SemaphoreType.DMA

    def local_step(tok, route, gate, wg, wu, wd):
        n_exp, d_model, d_ff = wg.shape
        n_tok = tok.shape[0]
        n_blk = d_model // COLS
        hidden = (n_exp, N_DEV * CAP, d_ff)
        w_on, x_all, codes, h, s, wd_on = pl.pallas_call(
            gather_kernel,
            out_shape=[on_chip((SLOTS, 2, d_model, d_ff), BF16), on_chip((N_DEV * n_tok, d_model), BF16), on_chip((8, 512), F32), on_chip(hidden, BF16), on_chip((4, 3, 128, 256), BF16), on_chip((n_exp, d_ff, COLS), BF16)],
            in_specs=[ANY] * 5,
            out_specs=[VMEM] * 6,
            scratch_shapes=[
                pltpu.VMEM((6, n_tok), jnp.int32),
                pltpu.VMEM((6, n_tok), F32),
                pltpu.VMEM((2, 8, 128), F32),
                pltpu.VMEM((N_DEV, 16, 128), F32),
                pltpu.VMEM((N_DEV, 16, 128), F32),
                dma((SLOTS, 2)),
                dma((3,)),
                dma((7,)),
                dma((7,)),
                dma((6,)),
                dma((6,)),
                dma((N_DEV,)),
                dma((N_DEV,)),
            ],
            compiler_params=pltpu.CompilerParams(collective_id=0, has_side_effects=True, vmem_limit_bytes=LIMIT),
            name="gather",
        )(tok, route.T, gate.T, wg, wu)
        unused, h, wd_on = pl.pallas_call(
            hidden_kernel,
            out_shape=[on_chip(w_on.shape, BF16), on_chip(hidden, BF16), on_chip(wd_on.shape, BF16)],
            in_specs=[VMEM] * 5 + [ANY] * 3,
            out_specs=[VMEM] * 3,
            scratch_shapes=[pltpu.VMEM((256, d_model), BF16), pltpu.SMEM((n_exp,), jnp.int32), dma((SLOTS, 2)), dma],
            input_output_aliases={0: 0, 1: 1, 2: 2},
            compiler_params=pltpu.CompilerParams(vmem_limit_bytes=LIMIT),
            name="hidden",
        )(pin(w_on), pin(h), pin(wd_on), pin(x_all), pin(codes), wg, wu, wd)
        return pl.pallas_call(
            combine_kernel,
            out_shape=jax.ShapeDtypeStruct((n_tok, d_model), BF16),
            in_specs=[VMEM] * 3 + [ANY],
            out_specs=VMEM,
            scratch_shapes=[
                pltpu.VMEM((3, n_exp, d_ff, COLS), BF16),
                pltpu.VMEM((2, N_DEV, 256, COLS), BF16),
                pltpu.VMEM((n_blk, 2, 2, 2, n_tok, COLS), F32),
                pltpu.VMEM((n_blk, 2, 2, n_tok, COLS), F32),
                pltpu.VMEM((n_blk, 2, n_tok // 2, COLS), F32),
                pltpu.VMEM((n_blk, 2, n_tok // 2, COLS), F32),
                pltpu.VMEM((n_blk, n_tok // 2, COLS), F32),
                pltpu.VMEM((n_blk, n_tok // 2, COLS), F32),
                dma((3,)),
                dma((2,)),
            ]
            + [dma((n_blk,))] * 10,
            compiler_params=pltpu.CompilerParams(collective_id=1, has_side_effects=True, vmem_limit_bytes=33 << 20),
            name="combine",
        )(pin(h), pin(s), pin(wd_on), wd)

    return jax.shard_map(local_step, mesh=mesh, in_specs=(row_spec, row_spec, row_spec, expert_spec, expert_spec, expert_spec), out_specs=row_spec, check_vma=False)
```

```python
import jax
import jax.numpy as jnp
from jax import lax
from jax.experimental import pallas as pl
from jax.experimental.pallas import tpu as pltpu
from jax.sharding import PartitionSpec as P

BF16 = jnp.bfloat16
F32 = jnp.float32
MESH = pl.DeviceIdType.MESH
N_DEV = 8
CAP = 32
SLOTS = 4
EARLY = 3
FRONT = 2
LAG_3 = 3
LAG_4 = 6
LIMIT = 4 << 20
COLS = 256
VMEM = pl.BlockSpec(memory_space=pltpu.VMEM)
ANY = pl.BlockSpec(memory_space=pl.ANY)


def remote(src, dst, send_sem, recv_sem, peer):
    return pltpu.make_async_remote_copy(src_ref=src, dst_ref=dst, send_sem=send_sem, recv_sem=recv_sem, device_id={"ep": peer}, device_id_type=MESH)


def on_chip(shape, dtype):
    return pltpu.VMEM(shape, dtype)


def pin(v):
    return pltpu.with_memory_space_constraint(v, pltpu.VMEM)


def place():
    me = lax.axis_index("ep")
    core = lax.rem(me, 2)
    x = lax.rem(me // 2, 2)
    y = me // 4
    return me, core, x, y, me + 1 - 2 * core, me + 2 - 4 * x, me + 4 - 8 * y


def entry_barrier(me):
    barrier = pltpu.get_barrier_semaphore()
    for d in range(1, N_DEV):
        pl.semaphore_signal(barrier, inc=1, device_id={"ep": lax.rem(me + d, N_DEV)}, device_id_type=MESH)
    pl.semaphore_wait(barrier, N_DEV - 1)


def gather_kernel(tok, route_t, gate_t, wg, wu, w_out, x_out, codes_out, h_out, s_out, wd_out, pad_i, pad_g, pad, sg_loc, sg, w_sem, in_sem, sib_s, sib_r, link_s, link_r, sg_s, sg_r):
    me, core, x, y, sib, xn, yn = place()
    n_tok = tok.shape[0]
    half = n_tok // 2

    def rows(device, part=0, count=half):
        return x_out.at[pl.ds(pl.multiple_of(device * n_tok + part * half, half), count)]

    own = pltpu.make_async_copy(tok, rows(me, 0, n_tok), in_sem.at[0])
    own_route = pltpu.make_async_copy(route_t, pad_i, in_sem.at[1])
    own_gate = pltpu.make_async_copy(gate_t, pad_g, in_sem.at[2])
    own.start()
    own_route.start()
    own_gate.start()
    barrier = pltpu.get_barrier_semaphore()
    for d in range(1, N_DEV):
        pl.semaphore_signal(barrier, inc=1, device_id={"ep": lax.rem(me + d, N_DEV)}, device_id_type=MESH)
    loads = []
    for e in range(EARLY):
        loads.append(pltpu.make_async_copy(wg.at[e], w_out.at[e, 0], w_sem.at[e, 0]))
        loads.append(pltpu.make_async_copy(wu.at[e], w_out.at[e, 1], w_sem.at[e, 1]))
    loads.append(pltpu.make_async_copy(wg.at[EARLY], w_out.at[EARLY, 0], w_sem.at[EARLY, 0]))
    for load in loads:
        load.start()

    pad[...] = jnp.zeros_like(pad)
    own_route.wait()
    pad[0, 0:6, 0:n_tok] = pad_i[...].astype(F32)
    own_gate.wait()
    pad[1, 0:6, 0:n_tok] = pad_g[...]
    routes = pad[0] + pltpu.roll(pad[0], n_tok, 1)
    gates = pad[1] + pltpu.roll(pad[1], n_tok, 1)
    expert = lax.broadcasted_iota(jnp.int32, (64, 128), 0).astype(F32)
    lane = lax.broadcasted_iota(jnp.int32, (64, 128), 1)
    mine = (lane // n_tok) == core
    member = jnp.zeros((64, 128), F32)
    weight = jnp.zeros((64, 128), F32)
    for k in range(6):
        hit = (expert == routes[k : k + 1, :]) & mine
        member = jnp.where(hit, 1.0, member)
        weight = jnp.where(hit, gates[k : k + 1, :], weight)
    row = lax.broadcasted_iota(jnp.int32, (128, 128), 0)
    col = lax.broadcasted_iota(jnp.int32, (128, 128), 1)
    upto = jnp.where((row <= col), 1.0, 0.0).astype(BF16)
    rank = jnp.dot(member.astype(BF16), upto, preferred_element_type=F32)
    code = jnp.where(member > 0.5, rank + (me * CAP).astype(F32), 0.0)
    sg_loc[:, 0:8, :] = code.reshape(8, 8, 128)
    sg_loc[:, 8:16, :] = weight.reshape(8, 8, 128)
    sg[me] = sg_loc[me]
    pl.semaphore_wait(barrier, N_DEV - 1)

    sg_copies = []
    for d in range(1, N_DEV):
        peer = lax.rem(me + d, N_DEV)
        sg_copies.append(remote(sg_loc.at[peer], sg.at[me], sg_s.at[d], sg_r.at[d], peer))
    for copy in sg_copies:
        copy.start()
    to_x_a = remote(rows(me, 0), rows(me, 0), link_s.at[0], link_r.at[0], xn)
    to_x_b = remote(rows(me, 1), rows(me, 1), link_s.at[1], link_r.at[1], xn)
    to_y_b = remote(rows(me, 1), rows(me, 1), link_s.at[2], link_r.at[2], yn)
    to_y_a = remote(rows(me, 0), rows(me, 0), link_s.at[3], link_r.at[3], yn)
    to_sib = remote(rows(me, 0, n_tok), rows(me, 0, n_tok), sib_s.at[0], sib_r.at[0], sib)
    own.wait()
    for copy in (to_x_a, to_y_b, to_x_b, to_y_a, to_sib):
        copy.start()
    dg = lax.rem(xn + 4, N_DEV)
    passed = []

    def pass_on(index, source, part):
        copy = remote(rows(source, part), rows(source, part), sib_s.at[index], sib_r.at[index], sib)
        copy.start()
        passed.append(copy)

    to_x_a.wait_recv()
    via_y = remote(rows(xn, 0), rows(xn, 0), link_s.at[4], link_r.at[4], yn)
    via_y.start()
    pass_on(1, xn, 0)
    to_y_b.wait_recv()
    via_x = remote(rows(yn, 1), rows(yn, 1), link_s.at[5], link_r.at[5], xn)
    via_x.start()
    pass_on(2, yn, 1)
    for copy in sg_copies:
        copy.wait()

    r = lax.broadcasted_iota(jnp.int32, (256, 128), 0)
    lane = lax.broadcasted_iota(jnp.int32, (256, 128), 1)
    for p in range(4):
        target = ((2 * p + lane // 64) * CAP + lax.rem(r, CAP) + 1).astype(F32)
        code = sg[2 * p, 0:8, :] + sg[2 * p + 1, 0:8, :]
        gate = sg[2 * p, 8:16, :] + sg[2 * p + 1, 8:16, :]
        codes_out[:, pl.ds(p * 128, 128)] = code
        code = jnp.broadcast_to(code[:, None, :], (8, CAP, 128)).reshape(256, 128)
        gate = jnp.broadcast_to(gate[:, None, :], (8, CAP, 128)).reshape(256, 128)
        s_t = jnp.where(code == target, gate, 0.0)
        s_f = s_t.T
        hi = jnp.minimum(s_f, 3.3895e38).astype(BF16)
        rest = s_f - hi.astype(F32)
        mid = rest.astype(BF16)
        low = (rest - mid.astype(F32)).astype(BF16)
        s_out[p, 0] = hi
        s_out[p, 1] = mid
        s_out[p, 2] = low

    to_x_b.wait_recv()
    pass_on(3, xn, 1)
    to_y_a.wait_recv()
    pass_on(4, yn, 0)
    via_y.wait_recv()
    pass_on(5, dg, 0)
    via_x.wait_recv()
    pass_on(6, dg, 1)
    for copy in (to_x_a, to_x_b, to_y_b, to_y_a, via_y, via_x):
        copy.wait_send()
    to_sib.wait()
    for copy in passed:
        copy.wait()
    for load in loads:
        load.wait()


def hidden_kernel(w_in, h_in, wd_in, x_all, codes, wg, wu, wd, w_buf, h_out, wd_out, xe, order, w_sem, d_sem):
    n_exp = wg.shape[0]
    d_ff = wg.shape[2]

    def load(n, e, part, src):
        s = lax.rem(n, SLOTS)
        return pltpu.make_async_copy(src.at[e], w_buf.at[s, part], w_sem.at[s, part])

    load(EARLY, EARLY, 1, wu).start()
    down = pltpu.make_async_copy(wd.at[:, :, pl.ds(0, COLS)], wd_out, d_sem)

    def hidden_rows(e, cap, slot):
        m = cap * N_DEV
        r = lax.broadcasted_iota(jnp.int32, (m, 512), 0)
        target = ((r // cap) * CAP + lax.rem(r, cap) + 1).astype(F32)
        pick = (target == codes[pl.ds(e, 1), :]).astype(BF16)
        for c in range(0, x_all.shape[1], 512):
            part = jnp.dot(pick, x_all[:, pl.ds(c, 512)], preferred_element_type=F32)
            xe[pl.ds(0, m), pl.ds(c, 512)] = part.astype(BF16)

        def put(act, c, w):
            if cap == CAP:
                h_out[e, :, pl.ds(c, w)] = act
            else:
                for i in range(N_DEV):
                    h_out[e, pl.ds(i * CAP, cap), pl.ds(c, w)] = act[i * cap : (i + 1) * cap]
                    h_out[e, pl.ds(i * CAP + cap, CAP - cap), pl.ds(c, w)] = jnp.zeros((CAP - cap, w), BF16)

        def act_of(a, b):
            return (a * jax.nn.sigmoid(a) * b).astype(BF16)

        rows = xe[pl.ds(0, m), :]
        for c in range(0, d_ff - 128, 256):
            a = jnp.dot(rows, w_buf[slot, 0, :, pl.ds(c, 256)], preferred_element_type=F32)
            b = jnp.dot(rows, w_buf[slot, 1, :, pl.ds(c, 256)], preferred_element_type=F32)
            put(act_of(a, b), c, 256)
        c = d_ff - 128
        both = jnp.concatenate([w_buf[slot, 0, :, pl.ds(c, 128)], w_buf[slot, 1, :, pl.ds(c, 128)]], axis=1)
        ab = jnp.dot(rows, both, preferred_element_type=F32)
        put(act_of(ab[:, :128], ab[:, 128:]), c, 128)

    block = lax.broadcasted_iota(jnp.int32, (1, 512), 1) // 64

    def few(e):
        return jnp.max(codes[pl.ds(e, 1), :] - (block * CAP).astype(F32)) <= 16.0

    for e in range(SLOTS):
        order[e] = e
    small_of = [few(e).astype(jnp.int32) for e in range(SLOTS, n_exp)]
    n_large = len(small_of) - sum(small_of)
    large_seen, small_seen = jnp.int32(0), n_large
    for e, is_small in enumerate(small_of):
        order[SLOTS + jnp.where(is_small == 1, small_seen, large_seen)] = e + SLOTS
        small_seen = small_seen + is_small
        large_seen = large_seen + 1 - is_small

    def step(n, carry):
        e = order[n]
        slot = lax.rem(n, SLOTS)

        @pl.when(n > EARLY)
        def _():
            load(n, e, 0, wg).wait()

        @pl.when(n >= EARLY)
        def _():
            load(n, e, 1, wu).wait()

        small = few(e)

        @pl.when(small)
        def _():
            hidden_rows(e, CAP // 2, slot)

        @pl.when(jnp.logical_not(small))
        def _():
            hidden_rows(e, CAP, slot)

        @pl.when(n + SLOTS < n_exp)
        def _():
            following = order[jnp.minimum(n + SLOTS, n_exp - 1)]
            load(n + SLOTS, following, 0, wg).start()
            load(n + SLOTS, following, 1, wu).start()

        @pl.when(n + SLOTS == n_exp)
        def _():
            down.start()

        return carry

    lax.fori_loop(0, n_exp, step, 0)
    down.wait()


def combine_kernel(h, s, wd_on, wd, y_out, wd_buf, o, part, d2d, h1a, h1b, h2a, h2b, w_sem, ds, dr, h1as, h1ar, h1bs, h1br, h2as, h2ar, h2bs, h2br):
    me, core, x, y, sib, xn, yn = place()
    n_blk = wd.shape[2] // COLS
    n_buf = wd_buf.shape[0]
    n_exp = h.shape[0]
    half = 32
    first, second = pl.ds(0, half), pl.ds(half, half)

    def load(b):
        slot = (b - 1) % n_buf
        return pltpu.make_async_copy(wd.at[:, :, pl.ds(b * COLS, COLS)], wd_buf.at[slot], w_sem.at[slot])

    for b in range(1, n_buf + 1):
        load(b).start()
    barrier = pltpu.get_barrier_semaphore()
    for d in range(1, N_DEV):
        pl.semaphore_signal(barrier, inc=1, device_id={"ep": lax.rem(me + d, N_DEV)}, device_id_type=MESH)

    def send_d2d(b):
        return remote(part.at[b, 1 - core], d2d.at[b], ds.at[b], dr.at[b], sib)

    def send_1a(b):
        return remote(part.at[b, core, :, 1 - x, first], h1a.at[b], h1as.at[b], h1ar.at[b], xn)

    def send_1b(b):
        return remote(part.at[b, core, 1 - y, :, second], h1b.at[b], h1bs.at[b], h1br.at[b], yn)

    def send_2a(b):
        return remote(part.at[b, core, 1 - y, x, first], h2a.at[b], h2as.at[b], h2ar.at[b], yn)

    def send_2b(b):
        return remote(part.at[b, core, y, 1 - x, second], h2b.at[b], h2bs.at[b], h2br.at[b], xn)

    def stage_1(b):
        send_d2d(b).start()

    def stage_2(b):
        send_d2d(b).wait_recv()
        part[b, core] += d2d[b]
        send_1a(b).start()
        send_1b(b).start()

    def stage_3(b):
        send_1a(b).wait_recv()
        send_1b(b).wait_recv()
        part[b, core, :, x, first] += h1a[b]
        part[b, core, y, :, second] += h1b[b]
        send_2a(b).start()
        send_2b(b).start()

    def stage_4(b):
        send_2a(b).wait_recv()
        send_2b(b).wait_recv()
        cols = pl.ds(b * COLS, COLS)
        y_out[first, cols] = (part[b, core, y, x, first] + h2a[b]).astype(BF16)
        y_out[second, cols] = (part[b, core, y, x, second] + h2b[b]).astype(BF16)

    def down(b, e, weights):
        out = jnp.dot(h[e], weights[e], preferred_element_type=F32).astype(BF16)
        for i in range(N_DEV):
            o[b % 2, i, pl.ds(e * CAP, CAP), :] = out[i * CAP : (i + 1) * CAP]

    def gather_sum(b):
        for i in range(N_DEV):
            gates = s[i // 2, :, pl.ds((i % 2) * 64, 64), :].reshape(192, 256)
            terms = jnp.dot(gates, o[b % 2, i], preferred_element_type=F32)
            part[b, i % 2, i // 4, (i // 2) % 2] = terms[0:64] + terms[64:128] + terms[128:192]

    def weights_of(b):
        return wd_on if b == 0 else wd_buf.at[(b - 1) % n_buf]

    for b in range(n_blk + LAG_4):
        if b < n_blk:
            if b > 0:
                load(b).wait()
            for e in range(FRONT):
                down(b, e, weights_of(b))
        if 1 <= b < n_blk + 1:
            gather_sum(b - 1)
            if b == 1:
                pl.semaphore_wait(barrier, N_DEV - 1)
            stage_1(b - 1)
        if b < n_blk:
            for e in range(FRONT, n_exp):
                down(b, e, weights_of(b))
            if 1 <= b and b + n_buf < n_blk:
                load(b + n_buf).start()
        for k, stage in ((1, stage_2), (LAG_3, stage_3), (LAG_4, stage_4)):
            if k <= b < n_blk + k:
                stage(b - k)

    def drain(b, carry):
        for send in (send_d2d, send_1a, send_1b, send_2a, send_2b):
            send(b).wait_send()
        return carry

    lax.fori_loop(0, n_blk, drain, 0)


def solution(mesh):
    row_spec = P(("dp", "ep"))
    expert_spec = P("ep")
    dma = pltpu.SemaphoreType.DMA

    def local_step(tok, route, gate, wg, wu, wd):
        n_exp, d_model, d_ff = wg.shape
        n_tok = tok.shape[0]
        n_blk = d_model // COLS
        hidden = (n_exp, N_DEV * CAP, d_ff)
        w_on, x_all, codes, h, s, wd_on = pl.pallas_call(
            gather_kernel,
            out_shape=[on_chip((SLOTS, 2, d_model, d_ff), BF16), on_chip((N_DEV * n_tok, d_model), BF16), on_chip((8, 512), F32), on_chip(hidden, BF16), on_chip((4, 3, 128, 256), BF16), on_chip((n_exp, d_ff, COLS), BF16)],
            in_specs=[ANY] * 5,
            out_specs=[VMEM] * 6,
            scratch_shapes=[
                pltpu.VMEM((6, n_tok), jnp.int32),
                pltpu.VMEM((6, n_tok), F32),
                pltpu.VMEM((2, 8, 128), F32),
                pltpu.VMEM((N_DEV, 16, 128), F32),
                pltpu.VMEM((N_DEV, 16, 128), F32),
                dma((SLOTS, 2)),
                dma((3,)),
                dma((7,)),
                dma((7,)),
                dma((6,)),
                dma((6,)),
                dma((N_DEV,)),
                dma((N_DEV,)),
            ],
            compiler_params=pltpu.CompilerParams(collective_id=0, has_side_effects=True, vmem_limit_bytes=LIMIT),
            name="gather",
        )(tok, route.T, gate.T, wg, wu)
        unused, h, wd_on = pl.pallas_call(
            hidden_kernel,
            out_shape=[on_chip(w_on.shape, BF16), on_chip(hidden, BF16), on_chip(wd_on.shape, BF16)],
            in_specs=[VMEM] * 5 + [ANY] * 3,
            out_specs=[VMEM] * 3,
            scratch_shapes=[pltpu.VMEM((256, d_model), BF16), pltpu.SMEM((n_exp,), jnp.int32), dma((SLOTS, 2)), dma],
            input_output_aliases={0: 0, 1: 1, 2: 2},
            compiler_params=pltpu.CompilerParams(vmem_limit_bytes=LIMIT),
            name="hidden",
        )(pin(w_on), pin(h), pin(wd_on), pin(x_all), pin(codes), wg, wu, wd)
        return pl.pallas_call(
            combine_kernel,
            out_shape=jax.ShapeDtypeStruct((n_tok, d_model), BF16),
            in_specs=[VMEM] * 3 + [ANY],
            out_specs=VMEM,
            scratch_shapes=[
                pltpu.VMEM((3, n_exp, d_ff, COLS), BF16),
                pltpu.VMEM((2, N_DEV, 256, COLS), BF16),
                pltpu.VMEM((n_blk, 2, 2, 2, n_tok, COLS), F32),
                pltpu.VMEM((n_blk, 2, 2, n_tok, COLS), F32),
                pltpu.VMEM((n_blk, 2, n_tok // 2, COLS), F32),
                pltpu.VMEM((n_blk, 2, n_tok // 2, COLS), F32),
                pltpu.VMEM((n_blk, n_tok // 2, COLS), F32),
                pltpu.VMEM((n_blk, n_tok // 2, COLS), F32),
                dma((3,)),
            ]
            + [dma((n_blk,))] * 10,
            compiler_params=pltpu.CompilerParams(collective_id=1, has_side_effects=True, vmem_limit_bytes=33 << 20),
            name="combine",
        )(pin(h), pin(s), pin(wd_on), wd)

    return jax.shard_map(local_step, mesh=mesh, in_specs=(row_spec, row_spec, row_spec, expert_spec, expert_spec, expert_spec), out_specs=row_spec, check_vma=False)
```
